512 devices in a mesh: dp: 32 (over z, y_lo), pipe: 8 (over x, core), tensor: 2 (over y_hi).
Axes of the slice: x: 4, y: 4 (y_hi: 2, y_lo: 2; y = y_hi * 2 + y_lo), z: 16, core: 2. Of those that a mesh axis runs over, the one named last changes fastest.
Arguments:
- hidden: bfloat16 [8, 4096, 3584], P('pipe', 'dp', 'tensor'), may hold values from -6 to 6
- frozen_weight: bfloat16 [3584, 3584], P('dp', 'tensor'), may hold values from -1 to 1
- final_norm_gain: float32 [3584], P('tensor'), may hold values from 0.1 to 1.9
- adapter_down_maps: bfloat16 [8, 32, 3584], P(None, None, 'tensor'), may hold values from -0.09375 to 0.09375
- adapter_up_maps: bfloat16 [8, 32, 3584], P(None, None, 'tensor'), may hold values from -1 to 1
- tenant: int32 [8, 256], P('pipe'), may hold values from 0 to 7, as said below
- adapter: int32 [8], P('pipe'), may hold values from 0 to 7
Outputs:
- upstream_grad: bfloat16 [8, 4096, 3584], P('pipe', 'dp', 'tensor')
- grad_up: float32 [8, 32, 3584], P('pipe', None, 'tensor')
- grad_down: float32 [8, 32, 3584], P('pipe', None, 'tensor')
- row_loss: float32 [8, 256], P('pipe', 'dp')
The draws below stay inside these ranges and needn't reach their ends.
Inputs may be any that keep to these rules, and one draw needn't show every extreme that they name: Rows 2i and 2i + 1 of a micro-batch have the same tenant.
All inputs are finite; a program needn't handle non-finite values.
Results may differ from the reference program's by a relative error of at most 0.024.
Values may be sent and summed in bfloat16 or wider, within the bound.
A program may use at most 64 MiB of HBM per device.

```python
import jax
import jax.numpy as jnp
from jax import lax

MODEL_WIDTH = 3584
ADAPTER_RANK = 32
ADAPTER_COUNT = 8
SEQ = 16
TENANTS = 8
ROWS_DEV = 8
ROWS = 256
TOKENS = 4096
MICRO = 8
N_DP = 32
N_TENSOR = 2


def draw_tenant(key, part):
    first_key, second_key = jax.random.split(jax.random.fold_in(key, 71))
    first = jax.random.randint(first_key, (MICRO, ROWS // 2), 0, TENANTS)
    second = jax.random.randint(second_key, (MICRO, ROWS // 2), 0, TENANTS)
    paired = jnp.minimum(first, second)
    return jnp.repeat(paired, 2, axis=1).astype(jnp.int32)


def draw_frozen_weight(key, part):
    entry_key, rough_key = jax.random.split(jax.random.fold_in(key, 53))
    level = jnp.arange(MODEL_WIDTH, dtype=jnp.float32) / (MODEL_WIDTH - 1)
    rough = jnp.exp(jax.random.uniform(rough_key, (MODEL_WIDTH,), jnp.float32, -0.4, 0.4))
    column_scale = 10.0 ** level * rough / 4.64
    entries = jax.random.normal(entry_key, (MODEL_WIDTH, MODEL_WIDTH), jnp.float32)
    entries = jnp.clip(entries, -6.0, 6.0) / jnp.sqrt(jnp.float32(MODEL_WIDTH))
    values = jnp.clip(entries * column_scale[None, :], -1.0, 1.0)
    return values.astype(jnp.bfloat16)


def plant(drawn, own_key, smallest, largest):
    index_at = [jax.random.randint(jax.random.fold_in(own_key, axis), (), 0, length) for axis, length in enumerate(drawn.shape)]
    widest = drawn.shape.index(max(drawn.shape))
    next_to = index_at[:widest] + [(index_at[widest] + 1) % drawn.shape[widest]] + index_at[widest + 1:]
    return drawn.at[tuple(index_at)].set(smallest).at[tuple(next_to)].set(largest)


def steps_of(rng, shape, cuts, smallest, top_value):
    loudness = 1.0
    for axis_at, shards_of in cuts:
        steps = jax.random.uniform(jax.random.fold_in(jax.random.fold_in(rng, 6), axis_at), (shards_of,), jnp.float32, smallest / len(cuts), top_value / len(cuts))
        loudness = loudness * jnp.repeat(jnp.exp(steps), shape[axis_at] // shards_of).reshape((-1,) + (1,) * (len(shape) - 1 - axis_at))
    return loudness


def gaussian(own_key, dims, deviation, limit, cuts=(), kind=jnp.bfloat16):
    values = jax.random.normal(own_key, dims, jnp.float32) * deviation
    if len(cuts) > 0:
        values = steps_of(own_key, dims, cuts, -0.22, 0.18) * values
    return jnp.clip(values, min=-limit, max=limit).astype(kind)


def setup_inputs(seed: int = 0) -> dict:
    arg_keys = jax.random.split(jax.random.key(seed), 8)
    hidden = gaussian(arg_keys[0], (MICRO, TOKENS, MODEL_WIDTH), 1.0, 6.0, ((0, 8), (1, 32), (2, 2)))
    frozen_weight = draw_frozen_weight(jax.random.fold_in(arg_keys[7], 71), 0)
    final_norm_gain = jnp.clip(1.0 + 0.18 * jax.random.normal(arg_keys[2], (MODEL_WIDTH,), jnp.float32), 0.1, 1.9)
    adapter_down_maps = gaussian(arg_keys[3], (ADAPTER_COUNT, ADAPTER_RANK, MODEL_WIDTH), MODEL_WIDTH ** -0.5, 0.09375, ((2, 2),))
    adapter_up_maps = gaussian(arg_keys[4], (ADAPTER_COUNT, ADAPTER_RANK, MODEL_WIDTH), ADAPTER_RANK ** -0.5, 1.0, ((2, 2),))
    tenant = draw_tenant(jax.random.fold_in(arg_keys[7], 71), 0)
    adapter = plant(jax.random.randint(arg_keys[6], (MICRO,), 0, ADAPTER_COUNT), jax.random.fold_in(arg_keys[6], 1), 0, ADAPTER_COUNT - 1).astype(jnp.int32)
    return {"hidden": hidden, "frozen_weight": frozen_weight, "final_norm_gain": final_norm_gain, "adapter_down_maps": adapter_down_maps, "adapter_up_maps": adapter_up_maps, "tenant": tenant, "adapter": adapter}


logit_divisor = 0.05
loss_scale = 256.0
adapter_scale = 0.5
epsilon = 1e-06

def micro_batch_step(tokens, tenants, down_matrix, up_matrix, frozen_weight, final_norm_gain):
    frozen_output = jnp.dot(tokens, frozen_weight, preferred_element_type=jnp.float32)
    low_rank_hidden = jnp.dot(tokens, down_matrix.T, preferred_element_type=jnp.float32).astype(jnp.bfloat16)
    output_rows = frozen_output + adapter_scale * jnp.dot(low_rank_hidden, up_matrix, preferred_element_type=jnp.float32)
    token_inv = lax.rsqrt(lax.optimization_barrier(jnp.sum(output_rows * output_rows, axis=1)) / MODEL_WIDTH + epsilon)
    normed = output_rows * token_inv[:, None] * final_norm_gain[None, :]
    pooled = lax.optimization_barrier(jnp.mean(normed.reshape(ROWS, SEQ, MODEL_WIDTH), axis=1))
    inverse = lax.rsqrt(lax.optimization_barrier(jnp.sum(pooled * pooled, axis=1)) + epsilon)
    unit_rows = pooled * inverse[:, None]
    encoded_vectors = unit_rows.astype(jnp.bfloat16)
    cosine_logits = jnp.dot(encoded_vectors, encoded_vectors.T, preferred_element_type=jnp.float32) / logit_divisor
    row_ids = jnp.arange(ROWS, dtype=jnp.int32)
    allowed = (tenants[:, None] == tenants[None, :]) & (row_ids[:, None] != row_ids[None, :])
    partner = row_ids[None, :] == (row_ids ^ 1)[:, None]
    exps = jnp.where(allowed, jnp.exp(cosine_logits), 0.0)
    log_total = jnp.log(lax.optimization_barrier(jnp.sum(exps, axis=1)))
    positive = lax.optimization_barrier(jnp.sum(jnp.where(partner, cosine_logits, 0.0), axis=1))
    row_loss = log_total - positive
    probs = jnp.where(allowed, jnp.exp(cosine_logits - log_total[:, None]), 0.0)
    weights = (loss_scale * (probs - partner.astype(jnp.float32))).astype(jnp.bfloat16)
    matching_logits = jnp.dot(weights, encoded_vectors, preferred_element_type=jnp.float32)
    block_weights = weights.reshape(N_DP, ROWS_DEV, ROWS).astype(jnp.float32)
    block_rows = encoded_vectors.reshape(N_DP, ROWS_DEV, MODEL_WIDTH).astype(jnp.float32)
    far_terms = jnp.einsum('kij,kid->kjd', block_weights, block_rows).astype(jnp.bfloat16)
    far_terms = lax.optimization_barrier(far_terms)
    distractor_logits = lax.optimization_barrier(jnp.sum(far_terms.astype(jnp.float32), axis=0))
    encoded_vector_derivative = (matching_logits + distractor_logits) / logit_divisor
    along = lax.optimization_barrier(jnp.sum(unit_rows * encoded_vector_derivative, axis=1))
    grad_pool = inverse[:, None] * (encoded_vector_derivative - unit_rows * along[:, None])
    spread = jnp.broadcast_to((grad_pool * final_norm_gain[None, :])[:, None, :] / SEQ, (ROWS, SEQ, MODEL_WIDTH)).reshape(TOKENS, MODEL_WIDTH)
    inner = lax.optimization_barrier(jnp.sum(spread * output_rows, axis=1))
    grad_norm_in = token_inv[:, None] * (spread - output_rows * (inner * token_inv * token_inv / MODEL_WIDTH)[:, None])
    output_gradient = grad_norm_in.astype(jnp.bfloat16)
    low_rank_gradient = (adapter_scale * jnp.dot(output_gradient, up_matrix.T, preferred_element_type=jnp.float32)).astype(jnp.bfloat16)
    width = MODEL_WIDTH // N_TENSOR
    base_sum = jnp.zeros((TOKENS, MODEL_WIDTH), jnp.float32)
    for block in range(N_TENSOR):
        lower = block * width
        part_sum = jnp.dot(output_gradient[:, lower:lower + width], frozen_weight[:, lower:lower + width].T, preferred_element_type=jnp.float32).astype(jnp.bfloat16)
        part_sum = lax.optimization_barrier(part_sum)
        base_sum = base_sum + part_sum.astype(jnp.float32)
    grad_in = (base_sum + jnp.dot(low_rank_gradient, down_matrix, preferred_element_type=jnp.float32)).astype(jnp.bfloat16)
    up_map_gradient = adapter_scale * jnp.dot(low_rank_hidden.T, output_gradient, preferred_element_type=jnp.float32)
    grad_downward = jnp.dot(low_rank_gradient.T, tokens, preferred_element_type=jnp.float32)
    return (grad_in, up_map_gradient, grad_downward, row_loss)

def reference(hidden, frozen_weight, final_norm_gain, adapter_down_maps, adapter_up_maps, tenant, adapter):
    step_results = []
    for batch_position in range(MICRO):
        picked_adapter = adapter[batch_position]
        step_results.append(micro_batch_step(hidden[batch_position], tenant[batch_position], adapter_down_maps[picked_adapter], adapter_up_maps[picked_adapter], frozen_weight, final_norm_gain))
    grad_in = jnp.stack([item[0] for item in step_results])
    upstream_grad = jnp.roll(grad_in, -1, axis=0)
    grad_up = jnp.stack([item[1] for item in step_results])
    grad_down = jnp.stack([item[2] for item in step_results])
    row_loss = jnp.stack([item[3] for item in step_results])
    return (upstream_grad, grad_up, grad_down, row_loss)
```

```python
import jax
import jax.numpy as jnp
from jax import lax
from jax.experimental import pallas as pl
from jax.experimental.pallas import tpu as pltpu
from jax.sharding import PartitionSpec as P

MESH = pl.DeviceIdType.MESH
F32, BF16 = jnp.float32, jnp.bfloat16

WIDTH = 3584
HALF = 1792
CORE = 896
SHARD = 112
PLANE = 224
CUT_A, CUT_B = 48, 96
NZ = 16
SEQ = 16
ROWS = 8
ALL = 256
TOK = 128
RANK = 32
OWNERS = 14
TILE = 256
TILES = 7

logit_divisor = 0.05
loss_scale = 256.0
adapter_scale = 0.5
epsilon = 1e-06


def nt(a, b):
    return lax.dot_general(a, b, (((1,), (1,)), ((), ())), preferred_element_type=F32)


def tn(a, b):
    return lax.dot_general(a, b, (((0,), (0,)), ((), ())), preferred_element_type=F32)


def nn(a, b):
    return jnp.dot(a, b, preferred_element_type=F32)


def per_token(rows):
    width = rows.shape[1]
    return jnp.broadcast_to(rows[:, None, :], (ROWS, SEQ, width)).reshape(TOK, width)


def as_lanes(columns):
    lane = lax.broadcasted_iota(jnp.int32, (TOK, TOK), 1)
    packed = jnp.zeros((TOK, TOK), F32)
    for number, column in enumerate(columns):
        packed = jnp.where(lane == number, jnp.broadcast_to(column, (TOK, TOK)), packed)
    return jnp.transpose(packed)[0:8, :]


def as_columns(lanes):
    return jnp.transpose(lanes)


def kernel(
    x_hbm,
    w_hbm,
    gain_ref,
    down_hbm,
    up_hbm,
    tenant_ref,
    adapter_ref,
    gin_ref,
    gup_ref,
    gdown_ref,
    loss_ref,
    wbuf,
    acc,
    x_own,
    x3,
    downs,
    ups,
    low_snd,
    low_rcv,
    lowt,
    tok_snd,
    tok_rcv,
    pooled_ref,
    e3,
    e2,
    s_snd,
    s_rcv,
    mask_ref,
    sum_snd,
    sum_rcv,
    go,
    gl_snd,
    gl_rcv,
    glt,
    part_snd,
    part_rcv,
    gin_snd,
    rs_up,
    rs_down,
    rs_rcv,
    ag,
    in_sem,
    z_sem,
    xy_sem,
    d2d_sem,
    w_send,
    x_sem,
    small_sem,
    ez_sem,
    ey_sem,
    e_send,
    part_sem,
    gin_sem,
    rs_sem,
    ag_sem,
):
    dp = lax.axis_index("dp")
    pipe = lax.axis_index("pipe")
    tensor = lax.axis_index("tensor")
    z = dp // 2
    y = dp % 2
    x = pipe // 2
    core = pipe % 2
    own_q = (x + y) % 2
    dp_right = (dp + 2) % 32
    dp_left = (dp + 30) % 32
    dp_y = dp + 1 - 2 * y
    x_right = (pipe + 2) % 8
    x_left = (pipe + 6) % 8
    partner = pipe + 1 - 2 * core
    peer = 1 - tensor
    before = (pipe + 7) % 8
    after = (pipe + 1) % 8

    def fetch(src, dst, number):
        return pltpu.make_async_copy(src, dst, in_sem.at[number])

    x_copy = fetch(x_hbm, x_own, 0)
    down_copy = fetch(down_hbm, downs, 1)
    up_copy = fetch(up_hbm, ups, 2)
    x_copy.start()
    down_copy.start()
    up_copy.start()

    barrier = pltpu.get_barrier_semaphore()
    for where in (
        {"dp": dp_right},
        {"dp": dp_left},
        {"dp": dp_y},
        {"pipe": x_right},
        {"pipe": x_left},
        {"pipe": before},
        {"pipe": after},
        {"tensor": peer},
    ):
        pl.semaphore_signal(barrier, inc=1, device_id=where, device_id_type=MESH)
    pl.semaphore_wait(barrier, 8)

    def remote(src, dst, send, recv, where):
        copy = pltpu.make_async_remote_copy(
            src_ref=src, dst_ref=dst, send_sem=send, recv_sem=recv, device_id=where, device_id_type=MESH
        )
        copy.start()

    def arrived(ref, sem):
        pltpu.make_async_copy(ref, ref, sem).wait()

    columns = pl.ds(pl.multiple_of(core * CORE, 128), CORE)

    def piece(zz, q, first, count):
        return wbuf.at[pl.ds(pl.multiple_of((zz * 2 + q) * SHARD + first, 16), count), columns]

    chunks = ((0, CUT_A), (CUT_A, SHARD - CUT_A))

    @pl.when(x % 2 == 0)
    def _():
        for number, (first, count) in enumerate(chunks):
            pltpu.make_async_copy(
                w_hbm.at[pl.ds(first, count), columns], piece(z, own_q, first, count), z_sem.at[0, number]
            ).start()

    @pl.when(x % 2 == 1)
    def _():
        for number, (first, count) in enumerate(chunks):
            remote(
                w_hbm.at[pl.ds(first, count), columns],
                piece(z, y, first, count),
                w_send.at[6],
                z_sem.at[0, number],
                {"dp": dp_y},
            )

    def got(zz, rel, number):
        first, count = chunks[number]
        arrived(piece(zz, own_q, first, count), z_sem.at[rel, number])

    def forward(zz, rel, number, right):
        first, count = chunks[number]
        part = piece(zz, own_q, first, count)
        there = (rel + 15) % NZ if right else (rel + 1) % NZ
        remote(
            part, part, w_send.at[0 if right else 1], z_sem.at[there, number],
            {"dp": dp_right if right else dp_left},
        )

    def share(zz, rel, number):
        if number == 0:
            part = piece(zz, own_q, 0, CUT_A)
            remote(part, part, w_send.at[2], xy_sem.at[rel], {"pipe": x_right})
        else:
            part = piece(zz, own_q, CUT_A, CUT_B - CUT_A)
            remote(part, part, w_send.at[3], xy_sem.at[rel], {"pipe": x_left})
            part = piece(zz, own_q, CUT_B, SHARD - CUT_B)
            remote(part, part, w_send.at[4], xy_sem.at[rel], {"dp": dp_y})
            part = piece(zz, own_q, 0, SHARD)
            remote(part, part, w_send.at[5], d2d_sem.at[0, rel], {"pipe": partner})

    def complement(zz, rel):
        part = piece(zz, 1 - own_q, 0, SHARD)
        arrived(part, xy_sem.at[rel])
        remote(part, part, w_send.at[5], d2d_sem.at[1, rel], {"pipe": partner})

    other = pl.ds(pl.multiple_of((1 - core) * CORE, 128), CORE)

    def compute(zz, rel):
        for number in range(2):
            q = own_q if number == 0 else 1 - own_q
            rows = pl.ds(pl.multiple_of((zz * 2 + q) * SHARD, 16), SHARD)
            arrived(wbuf.at[rows, other], d2d_sem.at[number, rel])
        lhs = x3[zz]
        rows = pl.ds(pl.multiple_of(zz * PLANE, 16), PLANE)
        for n in range(TILES):
            at = slice(n * TILE, (n + 1) * TILE)
            acc[:, at] += nn(lhs, wbuf[rows, at])

    def right_z(k):
        return (z + NZ - k) % NZ

    def left_z(k):
        return (z + k) % NZ

    def prepare():
        x_copy.wait()
        down_copy.wait()
        up_copy.wait()
        for number in range(8):
            x3[tensor * 8 + number] = x_own[:, number * PLANE : (number + 1) * PLANE]
        mine = x3.at[pl.ds(tensor * 8, 8)]
        remote(mine, mine, x_sem.at[0], x_sem.at[1], {"tensor": peer})
        picked = adapter_ref[0]
        low_snd[...] = nt(downs[picked], x_own[...])
        remote(low_snd, low_rcv, small_sem.at[0], small_sem.at[1], {"tensor": peer})
        tenants = jnp.broadcast_to(tenant_ref[...], (ALL, ALL)).astype(F32)
        own = jnp.transpose(tenants)
        row = lax.broadcasted_iota(jnp.int32, (ALL, ALL), 0)
        column = lax.broadcasted_iota(jnp.int32, (ALL, ALL), 1)
        mask_ref[...] = jnp.where((tenants == own) & (row != column), 1.0, 0.0)

    def first_terms():
        arrived(x3.at[pl.ds(peer * 8, 8)], x_sem.at[1])
        arrived(low_rcv, small_sem.at[1])
        picked = adapter_ref[0]
        lowt[...] = (low_snd[...] + low_rcv[...]).astype(BF16)
        for n in range(TILES):
            at = slice(n * TILE, (n + 1) * TILE)
            acc[:, at] = adapter_scale * tn(lowt[...], ups[picked, :, at])

    def step(k, carry):
        rel = (NZ - k) % NZ
        zr = right_z(k)
        zl = left_z(k)

        @pl.when(k <= 8)
        def _():
            got(zr, rel, 0)

        @pl.when(k <= 7)
        def _():
            forward(zr, rel, 0, True)

        @pl.when(k == 0)
        def _():
            forward(z, 0, 0, False)

        @pl.when((k >= 1) & (k <= 7))
        def _():
            got(zl, k, 0)

        @pl.when((k >= 1) & (k <= 6))
        def _():
            forward(zl, k, 0, False)

        @pl.when(k <= 8)
        def _():
            share(zr, rel, 0)

        @pl.when((k >= 1) & (k <= 7))
        def _():
            share(zl, k, 0)

        @pl.when(k <= 8)
        def _():
            got(zr, rel, 1)

        @pl.when(k <= 7)
        def _():
            forward(zr, rel, 1, True)

        @pl.when(k == 0)
        def _():
            forward(z, 0, 1, False)

        @pl.when((k >= 1) & (k <= 7))
        def _():
            got(zl, k, 1)

        @pl.when((k >= 1) & (k <= 6))
        def _():
            forward(zl, k, 1, False)

        @pl.when(k <= 8)
        def _():
            share(zr, rel, 1)

        @pl.when((k >= 1) & (k <= 7))
        def _():
            share(zl, k, 1)

        @pl.when(k == 0)
        def _():
            prepare()

        @pl.when((k >= 1) & (k <= 9))
        def _():
            complement(right_z(k - 1), (NZ + 1 - k) % NZ)

        @pl.when((k >= 2) & (k <= 8))
        def _():
            complement(left_z(k - 1), k - 1)

        @pl.when(k == 2)
        def _():
            first_terms()

        @pl.when(k >= 2)
        def _():
            compute(right_z(k - 2), (NZ + 2 - k) % NZ)

        @pl.when((k >= 3) & (k <= 9))
        def _():
            compute(left_z(k - 2), k - 2)

        return carry

    lax.fori_loop(0, 11, step, 0)

    picked = adapter_ref[0]

    out = acc[...]
    tok_snd[...] = as_lanes((jnp.sum(out * out, axis=1, keepdims=True),))
    remote(tok_snd, tok_rcv, small_sem.at[2], small_sem.at[3], {"tensor": peer})
    arrived(tok_rcv, small_sem.at[3])
    squares = as_columns(tok_snd[...] + tok_rcv[...])[:, 0:1]
    token_inv = lax.rsqrt(squares / WIDTH + epsilon)
    gained = acc[...] * gain_ref[...]
    pooled = jnp.sum((gained * token_inv).reshape(ROWS, SEQ, HALF), axis=1) * (1.0 / SEQ)
    pooled_ref[...] = pooled
    e3[dp] = pooled.astype(BF16)

    def row_of(zz, yy):
        return e3.at[zz * 2 + yy]

    def e_forward(zz, rel, right):
        there = (rel + 15) % NZ if right else (rel + 1) % NZ
        part = row_of(zz, y)
        remote(
            part, part, e_send.at[0 if right else 1], ez_sem.at[there],
            {"dp": dp_right if right else dp_left},
        )

    def e_share(zz, rel):
        part = row_of(zz, y)
        remote(part, part, e_send.at[2], ey_sem.at[rel], {"dp": dp_y})

    e_forward(z, 0, True)
    e_forward(z, 0, False)
    e_share(z, 0)
    second = jnp.sum(acc[...] * gain_ref[...] * per_token(pooled_ref[...]), axis=1, keepdims=True)

    def e_step(k, carry):
        rel = (NZ - k) % NZ
        arrived(row_of(right_z(k), y), ez_sem.at[rel])

        @pl.when(k <= 7)
        def _():
            e_forward(right_z(k), rel, True)

        @pl.when(k <= 7)
        def _():
            arrived(row_of(left_z(k), y), ez_sem.at[k])

        @pl.when(k <= 6)
        def _():
            e_forward(left_z(k), k, False)

        e_share(right_z(k), rel)

        @pl.when(k <= 7)
        def _():
            e_share(left_z(k), k)

        return carry

    lax.fori_loop(1, 9, e_step, 0)

    def e_last(rel, carry):
        arrived(row_of((z + rel) % NZ, 1 - y), ey_sem.at[rel])
        return carry

    lax.fori_loop(0, NZ, e_last, 0)
    e2[...] = e3[...].astype(F32).reshape(ALL, HALF).astype(BF16)

    s_snd[...] = nt(e2[...], e2[...])
    remote(s_snd, s_rcv, small_sem.at[4], small_sem.at[5], {"tensor": peer})
    arrived(s_rcv, small_sem.at[5])
    row = lax.broadcasted_iota(jnp.int32, (ALL, ALL), 0)
    column = lax.broadcasted_iota(jnp.int32, (ALL, ALL), 1)
    raw = s_snd[...] + s_rcv[...]
    diagonal = jnp.where(row == column, raw, 0.0)
    inverse_row = lax.rsqrt(jnp.sum(diagonal, axis=0, keepdims=True) + epsilon)
    inverse_column = lax.rsqrt(jnp.sum(diagonal, axis=1, keepdims=True) + epsilon)
    scores = raw * inverse_column * inverse_row / logit_divisor
    exps = jnp.where(mask_ref[...] > 0.0, jnp.exp(scores), 0.0)
    total_row = jnp.log(jnp.sum(exps, axis=0, keepdims=True))
    s_snd_rows = pl.ds(pl.multiple_of(dp * ROWS, ROWS), ROWS)
    own_raw = s_snd[s_snd_rows, :] + s_rcv[s_snd_rows, :]
    own_mask = mask_ref[s_snd_rows, :]
    own_row = lax.broadcasted_iota(jnp.int32, (ROWS, ALL), 0) + dp * ROWS
    own_column = lax.broadcasted_iota(jnp.int32, (ROWS, ALL), 1)
    inverse = lax.rsqrt(
        jnp.sum(jnp.where(own_row == own_column, own_raw, 0.0), axis=1, keepdims=True) + epsilon
    )
    own_scores = own_raw * inverse * inverse_row / logit_divisor
    mated = own_column == own_row + 1 - 2 * (own_row % 2)
    allowed = own_mask > 0.0
    total = jnp.log(jnp.sum(jnp.where(allowed, jnp.exp(own_scores), 0.0), axis=1, keepdims=True))
    positive = jnp.sum(jnp.where(mated, own_scores, 0.0), axis=1, keepdims=True)
    loss = jnp.broadcast_to(total - positive, (ROWS, TOK))
    loss_ref[...] = jnp.transpose(loss)[0:1, :]
    both = jnp.where(allowed, jnp.exp(own_scores - total) + jnp.exp(own_scores - total_row), 0.0)
    weights = loss_scale * (both - jnp.where(mated, 2.0, 0.0))
    grad_emb = nn((weights * inverse_row).astype(BF16), e2[...]) / logit_divisor

    unit = pooled_ref[...] * inverse
    along_part = jnp.sum(unit * grad_emb, axis=1, keepdims=True)
    gained = acc[...] * gain_ref[...]
    first = jnp.sum(gained * per_token(grad_emb), axis=1, keepdims=True)
    along_tokens = per_token(jnp.broadcast_to(along_part, (ROWS, TOK)))[:, 0:1]
    sum_snd[...] = as_lanes((first, second, along_tokens))
    remote(sum_snd, sum_rcv, small_sem.at[6], small_sem.at[7], {"tensor": peer})
    arrived(sum_rcv, small_sem.at[7])
    sums = as_columns(sum_snd[...] + sum_rcv[...])
    first_sum, second_sum, along = sums[:, 0:1], sums[:, 1:2], sums[:, 2:3]
    inverse_tokens = per_token(jnp.broadcast_to(inverse, (ROWS, TOK)))[:, 0:1]
    inner = inverse_tokens * (first_sum - along * inverse_tokens * second_sum) * (1.0 / SEQ)
    spread = (
        inverse_tokens
        * (per_token(grad_emb) - per_token(unit) * along)
        * gain_ref[...]
        * (1.0 / SEQ)
    )
    pull = inner * token_inv * token_inv * (1.0 / WIDTH)
    go[...] = (token_inv * (spread - acc[...] * pull)).astype(BF16)

    gl_snd[...] = adapter_scale * nt(ups[picked], go[...])
    remote(gl_snd, gl_rcv, small_sem.at[8], small_sem.at[9], {"tensor": peer})

    owner = z < OWNERS

    def scatter(buffer, values, kind):
        for number in range(OWNERS):
            buffer[number] = values[:, number * 128 : (number + 1) * 128].astype(BF16)

        @pl.when((y == kind) & owner)
        def _():
            rs_rcv[dp] = buffer[jnp.minimum(z, OWNERS - 1)]

        def one(off, carry):
            zz = (z + off) % NZ
            there = zz * 2 + kind

            @pl.when((zz < OWNERS) & (there != dp))
            def _():
                remote(
                    buffer.at[zz], rs_rcv.at[dp], rs_sem.at[kind], rs_sem.at[2], {"dp": there}
                )

            return carry

        lax.fori_loop(0, NZ, one, 0)

    scatter(rs_up, adapter_scale * nn(lowt[...], go[...]), 0)

    def part_step(j, carry):
        rows = pl.ds(pl.multiple_of(peer * HALF + j * TILE, TILE), TILE)
        part_snd[j] = nt(go[...], wbuf[rows, :]).astype(BF16)
        remote(part_snd.at[j], part_rcv.at[j], part_sem.at[TILES], part_sem.at[j], {"tensor": peer})
        return carry

    lax.fori_loop(0, TILES, part_step, 0)

    arrived(gl_rcv, small_sem.at[9])
    glt[...] = (gl_snd[...] + gl_rcv[...]).astype(BF16)
    scatter(rs_down, nn(glt[...], x_own[...]), 1)

    def gin_step(j, carry):
        rows = pl.ds(pl.multiple_of(tensor * HALF + j * TILE, TILE), TILE)
        at = pl.ds(pl.multiple_of(j * TILE, TILE), TILE)
        mine = nt(go[...], wbuf[rows, :]) + tn(glt[...], downs[picked, :, at])
        arrived(part_rcv.at[j], part_sem.at[j])
        gin_snd[j] = (mine + part_rcv[j].astype(F32)).astype(BF16)
        remote(gin_snd.at[j], gin_ref.at[:, at], gin_sem.at[TILES], gin_sem.at[j], {"pipe": before})
        return carry

    lax.fori_loop(0, TILES, gin_step, 0)

    @pl.when(owner)
    def _():
        arrived(rs_rcv.at[pl.ds(0, 31)], rs_sem.at[2])
        mine = ag.at[y * OWNERS + jnp.minimum(z, OWNERS - 1)]
        mine[...] = jnp.sum(rs_rcv[...].astype(F32), axis=0).astype(BF16)

        def one(off, carry):
            remote(mine, mine, ag_sem.at[0], ag_sem.at[1], {"dp": (dp + off) % 32})
            return carry

        lax.fori_loop(1, 32, one, 0)
        arrived(ag.at[pl.ds(0, 2 * OWNERS - 1)], ag_sem.at[1])

    @pl.when(z >= OWNERS)
    def _():
        arrived(ag, ag_sem.at[1])

    for number in range(OWNERS):
        at = slice(number * 128, (number + 1) * 128)
        gup_ref[:, at] = ag[number].astype(F32)
        gdown_ref[:, at] = ag[OWNERS + number].astype(F32)

    for number, rows in enumerate((8 * SHARD, 7 * SHARD, NZ * 48, NZ * 48, NZ * 16, 2 * NZ * SHARD)):
        arrived(wbuf.at[pl.ds(0, rows), pl.ds(0, CORE)], w_send.at[number])

    @pl.when(x % 2 == 1)
    def _():
        arrived(wbuf.at[pl.ds(0, SHARD), pl.ds(0, CORE)], w_send.at[6])

    arrived(x3.at[pl.ds(0, 8)], x_sem.at[0])
    arrived(low_snd, small_sem.at[0])
    arrived(tok_snd, small_sem.at[2])
    arrived(e3.at[pl.ds(0, 8)], e_send.at[0])
    arrived(e3.at[pl.ds(0, 7)], e_send.at[1])
    arrived(e3.at[pl.ds(0, 16)], e_send.at[2])
    arrived(s_snd, small_sem.at[4])
    arrived(sum_snd, small_sem.at[6])
    arrived(gl_snd, small_sem.at[8])
    arrived(part_snd, part_sem.at[TILES])
    arrived(gin_snd, gin_sem.at[TILES])
    for kind in range(2):

        @pl.when((y == kind) & owner)
        def _():
            arrived(rs_up.at[pl.ds(0, OWNERS - 1)], rs_sem.at[kind])

        @pl.when((y != kind) | (z >= OWNERS))
        def _():
            arrived(rs_up, rs_sem.at[kind])

    @pl.when(owner)
    def _():
        arrived(rs_rcv.at[pl.ds(0, 31)], ag_sem.at[0])

    def gin_last(j, carry):
        at = pl.ds(pl.multiple_of(j * TILE, TILE), TILE)
        arrived(gin_ref.at[:, at], gin_sem.at[j])
        return carry

    lax.fori_loop(0, TILES, gin_last, 0)


def body(hidden, frozen_weight, final_norm_gain, down_maps, up_maps, tenant, adapter):
    vmem = pl.BlockSpec(memory_space=pltpu.VMEM)
    anywhere = pl.BlockSpec(memory_space=pl.ANY)
    dma = pltpu.SemaphoreType.DMA
    gin, gup, gdown, loss = pl.pallas_call(
        kernel,
        name="whole_step",
        out_shape=(
            jax.ShapeDtypeStruct((TOK, HALF), BF16),
            jax.ShapeDtypeStruct((RANK, HALF), F32),
            jax.ShapeDtypeStruct((RANK, HALF), F32),
            jax.ShapeDtypeStruct((1, ROWS), F32),
        ),
        in_specs=[
            anywhere,
            anywhere,
            vmem,
            anywhere,
            anywhere,
            vmem,
            pl.BlockSpec(memory_space=pltpu.SMEM),
        ],
        out_specs=(anywhere, vmem, vmem, vmem),
        scratch_shapes=[
            pltpu.VMEM((WIDTH, HALF), BF16),
            pltpu.VMEM((TOK, HALF), F32),
            pltpu.VMEM((TOK, HALF), BF16),
            pltpu.VMEM((NZ, TOK, PLANE), BF16),
            pltpu.VMEM((8, RANK, HALF), BF16),
            pltpu.VMEM((8, RANK, HALF), BF16),
            pltpu.VMEM((RANK, TOK), F32),
            pltpu.VMEM((RANK, TOK), F32),
            pltpu.VMEM((RANK, TOK), BF16),
            pltpu.VMEM((8, TOK), F32),
            pltpu.VMEM((8, TOK), F32),
            pltpu.VMEM((ROWS, HALF), F32),
            pltpu.VMEM((32, ROWS, HALF), BF16),
            pltpu.VMEM((ALL, HALF), BF16),
            pltpu.VMEM((ALL, ALL), F32),
            pltpu.VMEM((ALL, ALL), F32),
            pltpu.VMEM((ALL, ALL), F32),
            pltpu.VMEM((8, TOK), F32),
            pltpu.VMEM((8, TOK), F32),
            pltpu.VMEM((TOK, HALF), BF16),
            pltpu.VMEM((RANK, TOK), F32),
            pltpu.VMEM((RANK, TOK), F32),
            pltpu.VMEM((RANK, TOK), BF16),
            pltpu.VMEM((TILES, TOK, TILE), BF16),
            pltpu.VMEM((TILES, TOK, TILE), BF16),
            pltpu.VMEM((TILES, TOK, TILE), BF16),
            pltpu.VMEM((OWNERS, RANK, 128), BF16),
            pltpu.VMEM((OWNERS, RANK, 128), BF16),
            pltpu.VMEM((32, RANK, 128), BF16),
            pltpu.VMEM((2 * OWNERS, RANK, 128), BF16),
            dma((3,)),
            dma((NZ, 2)),
            dma((NZ,)),
            dma((2, NZ)),
            dma((7,)),
            dma((2,)),
            dma((10,)),
            dma((NZ,)),
            dma((NZ,)),
            dma((3,)),
            dma((TILES + 1,)),
            dma((TILES + 1,)),
            dma((3,)),
            dma((2,)),
        ],
        compiler_params=pltpu.CompilerParams(
            collective_id=0, has_side_effects=True, vmem_limit_bytes=56 * 1024 * 1024
        ),
    )(hidden[0], frozen_weight, final_norm_gain[None, :], down_maps, up_maps, tenant, adapter)
    return gin[None], gup[None], gdown[None], loss


def solution(mesh):
    return jax.shard_map(
        body,
        mesh=mesh,
        in_specs=(
            P("pipe", "dp", "tensor"),
            P("dp", "tensor"),
            P("tensor"),
            P(None, None, "tensor"),
            P(None, None, "tensor"),
            P("pipe", None),
            P("pipe"),
        ),
        out_specs=(
            P("pipe", "dp", "tensor"),
            P("pipe", None, "tensor"),
            P("pipe", None, "tensor"),
            P("pipe", "dp"),
        ),
        check_vma=False,
    )
```

```python
import jax
import jax.numpy as jnp
from jax import lax
from jax.experimental import pallas as pl
from jax.experimental.pallas import tpu as pltpu
from jax.sharding import PartitionSpec as P

MESH = pl.DeviceIdType.MESH
F32, BF16 = jnp.float32, jnp.bfloat16

WIDTH = 3584
HALF = 1792
CORE = 896
SHARD = 112
PLANE = 224
CUT_A, CUT_B = 48, 96
NZ = 16
SEQ = 16
ROWS = 8
ALL = 256
TOK = 128
RANK = 32
OWNERS = 14
TILE = 256
TILES = 7

logit_divisor = 0.05
loss_scale = 256.0
adapter_scale = 0.5
epsilon = 1e-06


def nt(a, b):
    return lax.dot_general(a, b, (((1,), (1,)), ((), ())), preferred_element_type=F32)


def tn(a, b):
    return lax.dot_general(a, b, (((0,), (0,)), ((), ())), preferred_element_type=F32)


def nn(a, b):
    return jnp.dot(a, b, preferred_element_type=F32)


def per_token(rows):
    width = rows.shape[1]
    return jnp.broadcast_to(rows[:, None, :], (ROWS, SEQ, width)).reshape(TOK, width)


def as_lanes(columns):
    lane = lax.broadcasted_iota(jnp.int32, (TOK, TOK), 1)
    packed = jnp.zeros((TOK, TOK), F32)
    for number, column in enumerate(columns):
        packed = jnp.where(lane == number, jnp.broadcast_to(column, (TOK, TOK)), packed)
    return jnp.transpose(packed)[0:8, :]


def as_columns(lanes):
    return jnp.transpose(lanes)


def kernel(
    x_hbm,
    w_hbm,
    gain_hbm,
    down_hbm,
    up_hbm,
    tenant_ref,
    adapter_ref,
    gin_ref,
    gup_ref,
    gdown_ref,
    loss_ref,
    gain_ref,
    wbuf,
    acc,
    x_own,
    x3,
    downs,
    ups,
    low_snd,
    low_rcv,
    lowt,
    tok_snd,
    tok_rcv,
    pooled_ref,
    e3,
    e2,
    s_snd,
    s_rcv,
    s_all,
    mask_ref,
    sum_snd,
    sum_rcv,
    go,
    gl_snd,
    gl_rcv,
    glt,
    part_snd,
    part_rcv,
    own_part,
    gin_snd,
    rs_up,
    rs_down,
    rs_rcv,
    ag,
    in_sem,
    z_sem,
    xy_sem,
    d2d_sem,
    w_send,
    x_sem,
    small_sem,
    ez_sem,
    ey_sem,
    e_send,
    part_sem,
    gin_sem,
    rs_sem,
    ag_sem,
):
    dp = lax.axis_index("dp")
    pipe = lax.axis_index("pipe")
    tensor = lax.axis_index("tensor")
    z = dp // 2
    y = dp % 2
    x = pipe // 2
    core = pipe % 2
    own_q = (x + y) % 2
    dp_right = (dp + 2) % 32
    dp_left = (dp + 30) % 32
    dp_y = dp + 1 - 2 * y
    x_right = (pipe + 2) % 8
    x_left = (pipe + 6) % 8
    partner = pipe + 1 - 2 * core
    peer = 1 - tensor
    before = (pipe + 7) % 8
    after = (pipe + 1) % 8

    def fetch(src, dst, number):
        return pltpu.make_async_copy(src, dst, in_sem.at[number])

    x_copy = fetch(x_hbm, x_own, 0)
    down_copy = fetch(down_hbm, downs, 1)
    up_copy = fetch(up_hbm, ups, 2)
    x_copy.start()
    down_copy.start()
    up_copy.start()
    gain_copy = fetch(gain_hbm, gain_ref.at[0], 3)
    gain_copy.start()

    barrier = pltpu.get_barrier_semaphore()
    for where in (
        {"dp": dp_right},
        {"dp": dp_left},
        {"dp": dp_y},
        {"pipe": x_right},
        {"pipe": x_left},
        {"pipe": before},
        {"pipe": after},
        {"tensor": peer},
    ):
        pl.semaphore_signal(barrier, inc=1, device_id=where, device_id_type=MESH)
    pl.semaphore_wait(barrier, 8)

    def remote(src, dst, send, recv, where):
        copy = pltpu.make_async_remote_copy(
            src_ref=src, dst_ref=dst, send_sem=send, recv_sem=recv, device_id=where, device_id_type=MESH
        )
        copy.start()

    def arrived(ref, sem):
        pltpu.make_async_copy(ref, ref, sem).wait()

    columns = pl.ds(pl.multiple_of(core * CORE, 128), CORE)

    def piece(zz, q, first, count):
        return wbuf.at[pl.ds(pl.multiple_of((zz * 2 + q) * SHARD + first, 16), count), columns]

    chunks = ((0, CUT_A), (CUT_A, SHARD - CUT_A))

    @pl.when(x % 2 == 0)
    def _():
        for number, (first, count) in enumerate(chunks):
            pltpu.make_async_copy(
                w_hbm.at[pl.ds(first, count), columns], piece(z, own_q, first, count), z_sem.at[0, number]
            ).start()

    @pl.when(x % 2 == 1)
    def _():
        for number, (first, count) in enumerate(chunks):
            remote(
                w_hbm.at[pl.ds(first, count), columns],
                piece(z, y, first, count),
                w_send.at[6],
                z_sem.at[0, number],
                {"dp": dp_y},
            )

    def got(zz, rel, number):
        first, count = chunks[number]
        arrived(piece(zz, own_q, first, count), z_sem.at[rel, number])

    def forward(zz, rel, number, right):
        first, count = chunks[number]
        part = piece(zz, own_q, first, count)
        there = (rel + 15) % NZ if right else (rel + 1) % NZ
        remote(
            part, part, w_send.at[0 if right else 1], z_sem.at[there, number],
            {"dp": dp_right if right else dp_left},
        )

    def share(zz, rel, number):
        if number == 0:
            part = piece(zz, own_q, 0, CUT_A)
            remote(part, part, w_send.at[2], xy_sem.at[rel], {"pipe": x_right})
        else:
            part = piece(zz, own_q, CUT_A, CUT_B - CUT_A)
            remote(part, part, w_send.at[3], xy_sem.at[rel], {"pipe": x_left})
            part = piece(zz, own_q, CUT_B, SHARD - CUT_B)
            remote(part, part, w_send.at[4], xy_sem.at[rel], {"dp": dp_y})
            part = piece(zz, own_q, 0, SHARD)
            remote(part, part, w_send.at[5], d2d_sem.at[0, rel], {"pipe": partner})

    def complement(zz, rel):
        part = piece(zz, 1 - own_q, 0, SHARD)
        arrived(part, xy_sem.at[rel])
        remote(part, part, w_send.at[5], d2d_sem.at[1, rel], {"pipe": partner})

    other = pl.ds(pl.multiple_of((1 - core) * CORE, 128), CORE)

    def compute(zz, rel):
        for number in range(2):
            q = own_q if number == 0 else 1 - own_q
            rows = pl.ds(pl.multiple_of((zz * 2 + q) * SHARD, 16), SHARD)
            arrived(wbuf.at[rows, other], d2d_sem.at[number, rel])
        lhs = x3[zz]
        rows = pl.ds(pl.multiple_of(zz * PLANE, 16), PLANE)
        for n in range(TILES):
            at = slice(n * TILE, (n + 1) * TILE)
            acc[:, at] += nn(lhs, wbuf[rows, at])

    def right_z(k):
        return (z + NZ - k) % NZ

    def left_z(k):
        return (z + k) % NZ

    def prepare():
        x_copy.wait()
        down_copy.wait()
        up_copy.wait()
        gain_copy.wait()
        for number in range(8):
            x3[tensor * 8 + number] = x_own[:, number * PLANE : (number + 1) * PLANE]
        mine = x3.at[pl.ds(tensor * 8, 8)]
        remote(mine, mine, x_sem.at[0], x_sem.at[1], {"tensor": peer})
        picked = adapter_ref[0]
        low_snd[...] = nt(downs[picked], x_own[...])
        remote(low_snd, low_rcv, small_sem.at[0], small_sem.at[1], {"tensor": peer})
        tenants = jnp.broadcast_to(tenant_ref[...], (ALL, ALL)).astype(F32)
        own = jnp.transpose(tenants)
        row = lax.broadcasted_iota(jnp.int32, (ALL, ALL), 0)
        column = lax.broadcasted_iota(jnp.int32, (ALL, ALL), 1)
        mask_ref[...] = jnp.where((tenants == own) & (row != column), 1.0, 0.0)

    def first_terms():
        arrived(x3.at[pl.ds(peer * 8, 8)], x_sem.at[1])
        arrived(low_rcv, small_sem.at[1])
        picked = adapter_ref[0]
        lowt[...] = (low_snd[...] + low_rcv[...]).astype(BF16)
        for n in range(TILES):
            at = slice(n * TILE, (n + 1) * TILE)
            acc[:, at] = adapter_scale * tn(lowt[...], ups[picked, :, at])

    def step(k, carry):
        rel = (NZ - k) % NZ
        zr = right_z(k)
        zl = left_z(k)

        for number in range(2):

            @pl.when(k <= 8)
            def _():
                got(zr, rel, number)

            @pl.when(k <= 7 - number)
            def _():
                forward(zr, rel, number, True)

            @pl.when(k == 0)
            def _():
                forward(z, 0, number, False)

            @pl.when((k >= 1) & (k <= 7))
            def _():
                got(zl, k, number)

            @pl.when((k >= 1) & (k <= 6 + number))
            def _():
                forward(zl, k, number, False)

            @pl.when(k <= 8)
            def _():
                share(zr, rel, number)

            @pl.when((k >= 1) & (k <= 7))
            def _():
                share(zl, k, number)

        @pl.when(k == 0)
        def _():
            prepare()

        @pl.when((k >= 1) & (k <= 9))
        def _():
            complement(right_z(k - 1), (NZ + 1 - k) % NZ)

        @pl.when((k >= 2) & (k <= 8))
        def _():
            complement(left_z(k - 1), k - 1)

        @pl.when(k == 2)
        def _():
            first_terms()

        @pl.when(k >= 2)
        def _():
            compute(right_z(k - 2), (NZ + 2 - k) % NZ)

        @pl.when((k >= 3) & (k <= 9))
        def _():
            compute(left_z(k - 2), k - 2)

        return carry

    lax.fori_loop(0, 11, step, 0)

    picked = adapter_ref[0]

    out = acc[...]
    tok_snd[...] = as_lanes((jnp.sum(out * out, axis=1, keepdims=True),))
    remote(tok_snd, tok_rcv, small_sem.at[2], small_sem.at[3], {"tensor": peer})
    arrived(tok_rcv, small_sem.at[3])
    squares = as_columns(tok_snd[...] + tok_rcv[...])[:, 0:1]
    token_inv = lax.rsqrt(squares / WIDTH + epsilon)
    gained = acc[...] * gain_ref[...]
    pooled = jnp.sum((gained * token_inv).reshape(ROWS, SEQ, HALF), axis=1) * (1.0 / SEQ)
    pooled_ref[...] = pooled
    e3[dp] = pooled.astype(BF16)

    def row_of(rel, yy):
        return e3.at[((z + rel) % NZ) * 2 + yy]

    def e_send_z(rel, hops, half=None):
        part = row_of(rel, y)
        if half is not None:
            part = part.at[:, pl.ds(half * CORE, CORE)]
        remote(
            part, part, e_send.at[0], ez_sem.at[(rel - hops) % NZ], {"dp": (dp + 32 + 2 * hops) % 32}
        )

    def e_send_y(rel):
        part = row_of(rel, y)
        remote(part, part, e_send.at[1], ey_sem.at[rel], {"dp": dp_y})

    for hops in (4, -4, 1, -1, 2, -2):
        e_send_z(0, hops)
    e_send_y(0)
    second = jnp.sum(acc[...] * gain_ref[...] * per_token(pooled_ref[...]), axis=1, keepdims=True)
    for rel in (15, 1, 14, 2, 12, 4, 11, 3, 13, 5, 10, 6, 8, 7, 9):
        arrived(row_of(rel, y), ez_sem.at[rel])
        if rel == 12:
            e_send_z(12, 4, 0)
        if rel == 4:
            e_send_z(4, -4, 1)
        if rel % 4 == 0:
            e_send_z(rel, 1)
            e_send_z(rel, -1)
        if rel == 12:
            e_send_z(12, 2)
        if rel == 4:
            e_send_z(4, -2)
        e_send_y(rel)

    def e_last(rel, carry):
        arrived(e3.at[((z + rel) % NZ) * 2 + 1 - y], ey_sem.at[rel])
        return carry

    lax.fori_loop(0, NZ, e_last, 0)
    e2[...] = e3[...].astype(F32).reshape(ALL, HALF).astype(BF16)

    row = lax.broadcasted_iota(jnp.int32, (TOK, TOK), 0)
    column = lax.broadcasted_iota(jnp.int32, (TOK, TOK), 1)
    upper, lower = e2[0:TOK, :], e2[TOK:ALL, :]
    corner = nt(lower, lower)
    s_snd[0:TOK, :] = nt(upper, lower)
    s_snd[TOK:ALL, :] = jnp.where(row >= column, nt(upper, upper), corner)
    s_snd[ALL:, :] = jnp.broadcast_to(
        jnp.sum(jnp.where(row == column, corner, 0.0), axis=0, keepdims=True), (8, TOK)
    )
    remote(s_snd, s_rcv, small_sem.at[4], small_sem.at[5], {"tensor": peer})
    arrived(s_rcv, small_sem.at[5])
    block = s_snd[0:TOK, :] + s_rcv[0:TOK, :]
    both = s_snd[TOK:ALL, :] + s_rcv[TOK:ALL, :]
    below = jnp.where(row > column, both, 0.0)
    above = jnp.where(row < column, both, 0.0)
    corner = jnp.broadcast_to(s_snd[ALL : ALL + 1, :] + s_rcv[ALL : ALL + 1, :], (TOK, TOK))
    s_all[0:TOK, 0:TOK] = jnp.where(row >= column, both, 0.0) + jnp.transpose(below)
    s_all[0:TOK, TOK:ALL] = block
    s_all[TOK:ALL, 0:TOK] = jnp.transpose(block)
    s_all[TOK:ALL, TOK:ALL] = above + jnp.transpose(above) + jnp.where(row == column, corner, 0.0)
    row = lax.broadcasted_iota(jnp.int32, (ALL, ALL), 0)
    column = lax.broadcasted_iota(jnp.int32, (ALL, ALL), 1)
    raw = s_all[...]
    diagonal = jnp.where(row == column, raw, 0.0)
    inverse_row = lax.rsqrt(jnp.sum(diagonal, axis=0, keepdims=True) + epsilon)
    inverse_column = lax.rsqrt(jnp.sum(diagonal, axis=1, keepdims=True) + epsilon)
    scores = raw * inverse_column * inverse_row / logit_divisor
    exps = jnp.where(mask_ref[...] > 0.0, jnp.exp(scores), 0.0)
    total_row = jnp.log(jnp.sum(exps, axis=0, keepdims=True))
    own_rows = pl.ds(pl.multiple_of(dp * ROWS, ROWS), ROWS)
    own_raw = s_all[own_rows, :]
    own_mask = mask_ref[own_rows, :]
    own_row = lax.broadcasted_iota(jnp.int32, (ROWS, ALL), 0) + dp * ROWS
    own_column = lax.broadcasted_iota(jnp.int32, (ROWS, ALL), 1)
    inverse = lax.rsqrt(
        jnp.sum(jnp.where(own_row == own_column, own_raw, 0.0), axis=1, keepdims=True) + epsilon
    )
    own_scores = own_raw * inverse * inverse_row / logit_divisor
    mated = own_column == own_row + 1 - 2 * (own_row % 2)
    allowed = own_mask > 0.0
    total = jnp.log(jnp.sum(jnp.where(allowed, jnp.exp(own_scores), 0.0), axis=1, keepdims=True))
    positive = jnp.sum(jnp.where(mated, own_scores, 0.0), axis=1, keepdims=True)
    loss = jnp.broadcast_to(total - positive, (ROWS, TOK))
    loss_ref[...] = jnp.transpose(loss)[0:1, :]
    both = jnp.where(allowed, jnp.exp(own_scores - total) + jnp.exp(own_scores - total_row), 0.0)
    weights = loss_scale * (both - jnp.where(mated, 2.0, 0.0))
    grad_emb = nn((weights * inverse_row).astype(BF16), e2[...]) / logit_divisor

    unit = pooled_ref[...] * inverse
    along_part = jnp.sum(unit * grad_emb, axis=1, keepdims=True)
    gained = acc[...] * gain_ref[...]
    first = jnp.sum(gained * per_token(grad_emb), axis=1, keepdims=True)
    along_tokens = per_token(jnp.broadcast_to(along_part, (ROWS, TOK)))[:, 0:1]
    sum_snd[...] = as_lanes((first, second, along_tokens))
    remote(sum_snd, sum_rcv, small_sem.at[6], small_sem.at[7], {"tensor": peer})
    arrived(sum_rcv, small_sem.at[7])
    sums = as_columns(sum_snd[...] + sum_rcv[...])
    first_sum, second_sum, along = sums[:, 0:1], sums[:, 1:2], sums[:, 2:3]
    inverse_tokens = per_token(jnp.broadcast_to(inverse, (ROWS, TOK)))[:, 0:1]
    inner = inverse_tokens * (first_sum - along * inverse_tokens * second_sum) * (1.0 / SEQ)
    spread = (
        inverse_tokens
        * (per_token(grad_emb) - per_token(unit) * along)
        * gain_ref[...]
        * (1.0 / SEQ)
    )
    pull = inner * token_inv * token_inv * (1.0 / WIDTH)
    go[...] = (token_inv * (spread - acc[...] * pull)).astype(BF16)

    gl_snd[...] = adapter_scale * nt(ups[picked], go[...])
    remote(gl_snd, gl_rcv, small_sem.at[8], small_sem.at[9], {"tensor": peer})

    owner = z < OWNERS

    def scatter(buffer, values, kind):
        for number in range(OWNERS):
            buffer[number] = values[:, number * 128 : (number + 1) * 128].astype(BF16)

        @pl.when((y == kind) & owner)
        def _():
            rs_rcv[dp] = buffer[jnp.minimum(z, OWNERS - 1)]

        def one(off, carry):
            zz = (z + off) % NZ
            there = zz * 2 + kind

            @pl.when((zz < OWNERS) & (there != dp))
            def _():
                remote(
                    buffer.at[zz], rs_rcv.at[dp], rs_sem.at[kind], rs_sem.at[2], {"dp": there}
                )

            return carry

        lax.fori_loop(0, NZ, one, 0)

    scatter(rs_up, adapter_scale * nn(lowt[...], go[...]), 0)

    def part_step(j, carry):
        rows = pl.ds(pl.multiple_of(peer * HALF + j * TILE, TILE), TILE)
        part_snd[j] = nt(go[...], wbuf[rows, :]).astype(BF16)
        remote(part_snd.at[j], part_rcv.at[j], part_sem.at[TILES], part_sem.at[j], {"tensor": peer})
        return carry

    lax.fori_loop(0, 3, part_step, 0)

    arrived(gl_rcv, small_sem.at[9])
    glt[...] = (gl_snd[...] + gl_rcv[...]).astype(BF16)
    scatter(rs_down, nn(glt[...], x_own[...]), 1)

    lax.fori_loop(3, TILES, part_step, 0)

    def own_step(j, carry):
        rows = pl.ds(pl.multiple_of(tensor * HALF + j * TILE, TILE), TILE)
        at = pl.ds(pl.multiple_of(j * TILE, TILE), TILE)
        own_part[j] = nt(go[...], wbuf[rows, :]) + tn(glt[...], downs[picked, :, at])
        return carry

    lax.fori_loop(0, TILES, own_step, 0)

    @pl.when(owner)
    def _():
        arrived(rs_rcv.at[pl.ds(0, 31)], rs_sem.at[2])
        mine = ag.at[y * OWNERS + jnp.minimum(z, OWNERS - 1)]
        mine[...] = jnp.sum(rs_rcv[...].astype(F32), axis=0).astype(BF16)

        def one(off, carry):
            remote(mine, mine, ag_sem.at[0], ag_sem.at[1], {"dp": (dp + off) % 32})
            return carry

        lax.fori_loop(1, 32, one, 0)

    def gin_step(j, carry):
        at = pl.ds(pl.multiple_of(j * TILE, TILE), TILE)
        arrived(part_rcv.at[j], part_sem.at[j])
        gin_snd[j] = (own_part[j] + part_rcv[j].astype(F32)).astype(BF16)
        remote(gin_snd.at[j], gin_ref.at[:, at], gin_sem.at[TILES], gin_sem.at[j], {"pipe": before})
        return carry

    lax.fori_loop(0, TILES, gin_step, 0)

    @pl.when(owner)
    def _():
        arrived(ag.at[pl.ds(0, 2 * OWNERS - 1)], ag_sem.at[1])

    @pl.when(z >= OWNERS)
    def _():
        arrived(ag, ag_sem.at[1])

    for number in range(OWNERS):
        at = slice(number * 128, (number + 1) * 128)
        gup_ref[:, at] = ag[number].astype(F32)
        gdown_ref[:, at] = ag[OWNERS + number].astype(F32)

    for number, rows in enumerate((7 * SHARD + CUT_A, 8 * SHARD - CUT_A, NZ * 48, NZ * 48, NZ * 16, 2 * NZ * SHARD)):
        arrived(wbuf.at[pl.ds(0, rows), pl.ds(0, CORE)], w_send.at[number])

    @pl.when(x % 2 == 1)
    def _():
        arrived(wbuf.at[pl.ds(0, SHARD), pl.ds(0, CORE)], w_send.at[6])

    arrived(x3.at[pl.ds(0, 8)], x_sem.at[0])
    arrived(low_snd, small_sem.at[0])
    arrived(tok_snd, small_sem.at[2])
    arrived(e3.at[pl.ds(0, 15)], e_send.at[0])
    arrived(e3.at[pl.ds(0, 16)], e_send.at[1])
    arrived(s_snd, small_sem.at[4])
    arrived(sum_snd, small_sem.at[6])
    arrived(gl_snd, small_sem.at[8])
    arrived(part_snd, part_sem.at[TILES])
    arrived(gin_snd, gin_sem.at[TILES])
    for kind in range(2):

        @pl.when((y == kind) & owner)
        def _():
            arrived(rs_up.at[pl.ds(0, OWNERS - 1)], rs_sem.at[kind])

        @pl.when((y != kind) | (z >= OWNERS))
        def _():
            arrived(rs_up, rs_sem.at[kind])

    @pl.when(owner)
    def _():
        arrived(rs_rcv.at[pl.ds(0, 31)], ag_sem.at[0])

    def gin_last(j, carry):
        at = pl.ds(pl.multiple_of(j * TILE, TILE), TILE)
        arrived(gin_ref.at[:, at], gin_sem.at[j])
        return carry

    lax.fori_loop(0, TILES, gin_last, 0)


def body(hidden, frozen_weight, final_norm_gain, down_maps, up_maps, tenant, adapter):
    vmem = pl.BlockSpec(memory_space=pltpu.VMEM)
    anywhere = pl.BlockSpec(memory_space=pl.ANY)
    dma = pltpu.SemaphoreType.DMA
    gin, gup, gdown, loss = pl.pallas_call(
        kernel,
        name="whole_step",
        out_shape=(
            pltpu.VMEM((TOK, HALF), BF16),
            pltpu.VMEM((RANK, HALF), F32),
            pltpu.VMEM((RANK, HALF), F32),
            pltpu.VMEM((1, ROWS), F32),
        ),
        in_specs=[
            anywhere,
            anywhere,
            anywhere,
            anywhere,
            anywhere,
            vmem,
            pl.BlockSpec(memory_space=pltpu.SMEM),
        ],
        out_specs=(anywhere, vmem, vmem, vmem),
        scratch_shapes=[
            pltpu.VMEM((1, HALF), F32),
            pltpu.VMEM((WIDTH, HALF), BF16),
            pltpu.VMEM((TOK, HALF), F32),
            pltpu.VMEM((TOK, HALF), BF16),
            pltpu.VMEM((NZ, TOK, PLANE), BF16),
            pltpu.VMEM((8, RANK, HALF), BF16),
            pltpu.VMEM((8, RANK, HALF), BF16),
            pltpu.VMEM((RANK, TOK), F32),
            pltpu.VMEM((RANK, TOK), F32),
            pltpu.VMEM((RANK, TOK), BF16),
            pltpu.VMEM((8, TOK), F32),
            pltpu.VMEM((8, TOK), F32),
            pltpu.VMEM((ROWS, HALF), F32),
            pltpu.VMEM((32, ROWS, HALF), BF16),
            pltpu.VMEM((ALL, HALF), BF16),
            pltpu.VMEM((ALL + 8, TOK), F32),
            pltpu.VMEM((ALL + 8, TOK), F32),
            pltpu.VMEM((ALL, ALL), F32),
            pltpu.VMEM((ALL, ALL), F32),
            pltpu.VMEM((8, TOK), F32),
            pltpu.VMEM((8, TOK), F32),
            pltpu.VMEM((TOK, HALF), BF16),
            pltpu.VMEM((RANK, TOK), F32),
            pltpu.VMEM((RANK, TOK), F32),
            pltpu.VMEM((RANK, TOK), BF16),
            pltpu.VMEM((TILES, TOK, TILE), BF16),
            pltpu.VMEM((TILES, TOK, TILE), BF16),
            pltpu.VMEM((TILES, TOK, TILE), F32),
            pltpu.VMEM((TILES, TOK, TILE), BF16),
            pltpu.VMEM((OWNERS, RANK, 128), BF16),
            pltpu.VMEM((OWNERS, RANK, 128), BF16),
            pltpu.VMEM((32, RANK, 128), BF16),
            pltpu.VMEM((2 * OWNERS, RANK, 128), BF16),
            dma((4,)),
            dma((NZ, 2)),
            dma((NZ,)),
            dma((2, NZ)),
            dma((7,)),
            dma((2,)),
            dma((10,)),
            dma((NZ,)),
            dma((NZ,)),
            dma((2,)),
            dma((TILES + 1,)),
            dma((TILES + 1,)),
            dma((3,)),
            dma((2,)),
        ],
        compiler_params=pltpu.CompilerParams(
            collective_id=0, has_side_effects=True, vmem_limit_bytes=56 * 1024 * 1024
        ),
    )(hidden[0], frozen_weight, final_norm_gain, down_maps, up_maps, tenant, adapter)
    return gin[None], gup[None], gdown[None], loss


def solution(mesh):
    return jax.shard_map(
        body,
        mesh=mesh,
        in_specs=(
            P("pipe", "dp", "tensor"),
            P("dp", "tensor"),
            P("tensor"),
            P(None, None, "tensor"),
            P(None, None, "tensor"),
            P("pipe", None),
            P("pipe"),
        ),
        out_specs=(
            P("pipe", "dp", "tensor"),
            P("pipe", None, "tensor"),
            P("pipe", None, "tensor"),
            P("pipe", "dp"),
        ),
        check_vma=False,
    )
```

```python
import jax
import jax.numpy as jnp
from jax import lax
from jax.experimental import pallas as pl
from jax.experimental.pallas import tpu as pltpu
from jax.sharding import PartitionSpec as P

MESH = pl.DeviceIdType.MESH
F32, BF16 = jnp.float32, jnp.bfloat16

WIDTH = 3584
HALF = 1792
CORE = 896
SHARD = 112
PLANE = 224
CUT_A, CUT_B = 48, 96
NZ = 16
SEQ = 16
ROWS = 8
ALL = 256
TOK = 128
RANK = 32
OWNERS = 14
TILE = 256
TILES = 7
LAG = 4

logit_divisor = 0.05
loss_scale = 256.0
adapter_scale = 0.5
epsilon = 1e-06


def nt(a, b):
    return lax.dot_general(a, b, (((1,), (1,)), ((), ())), preferred_element_type=F32)


def tn(a, b):
    return lax.dot_general(a, b, (((0,), (0,)), ((), ())), preferred_element_type=F32)


def nn(a, b):
    return jnp.dot(a, b, preferred_element_type=F32)


def per_token(rows):
    width = rows.shape[1]
    return jnp.broadcast_to(rows[:, None, :], (ROWS, SEQ, width)).reshape(TOK, width)


def as_lanes(columns):
    lane = lax.broadcasted_iota(jnp.int32, (TOK, TOK), 1)
    packed = jnp.zeros((TOK, TOK), F32)
    for number, column in enumerate(columns):
        packed = jnp.where(lane == number, jnp.broadcast_to(column, (TOK, TOK)), packed)
    return jnp.transpose(packed)[0:8, :]


def as_columns(lanes):
    return jnp.transpose(lanes)


def kernel(
    x_hbm,
    w_hbm,
    gain_hbm,
    down_hbm,
    up_hbm,
    tenant_ref,
    adapter_ref,
    gin_ref,
    gup_ref,
    gdown_ref,
    loss_ref,
    gain_ref,
    wbuf,
    acc,
    x_own,
    x3,
    x_pass,
    downs,
    ups,
    low_snd,
    low_rcv,
    lowt,
    tok_snd,
    tok_rcv,
    pooled_ref,
    e3,
    e2,
    s_snd,
    s_rcv,
    s_all,
    mask_ref,
    gained_ref,
    t_snd,
    t_rcv,
    go,
    gl_snd,
    gl_rcv,
    glt,
    part_snd,
    part_rcv,
    own_part,
    gin_snd,
    rs_up,
    rs_down,
    rs_rcv,
    ag,
    in_sem,
    z_sem,
    xy_sem,
    d2d_sem,
    w_send,
    x_sem,
    small_sem,
    ez_sem,
    ey_sem,
    e_send,
    part_sem,
    gin_sem,
    rs_sem,
    ag_sem,
    agz_sem,
):
    dp = lax.axis_index("dp")
    pipe = lax.axis_index("pipe")
    tensor = lax.axis_index("tensor")
    z = dp // 2
    y = dp % 2
    x = pipe // 2
    core = pipe % 2
    own_q = (x + y) % 2
    dp_right = (dp + 2) % 32
    dp_left = (dp + 30) % 32
    dp_y = dp + 1 - 2 * y
    x_right = (pipe + 2) % 8
    x_left = (pipe + 6) % 8
    partner = pipe + 1 - 2 * core
    peer = 1 - tensor
    plus = {"dp": dp_y, "tensor": (tensor + y) % 2}
    minus = {"dp": dp_y, "tensor": (tensor + 1 - y) % 2}
    before = (pipe + 7) % 8
    after = (pipe + 1) % 8

    def fetch(src, dst, number):
        return pltpu.make_async_copy(src, dst, in_sem.at[number])

    x_copy = fetch(x_hbm, x_own, 0)
    down_copy = fetch(down_hbm, downs, 1)
    up_copy = fetch(up_hbm, ups, 2)
    x_copy.start()
    down_copy.start()
    up_copy.start()
    gain_copy = fetch(gain_hbm, gain_ref.at[0], 3)
    gain_copy.start()

    barrier = pltpu.get_barrier_semaphore()
    for where in (
        {"dp": dp_right},
        {"dp": dp_left},
        {"dp": dp_y},
        {"pipe": x_right},
        {"pipe": x_left},
        {"pipe": before},
        {"pipe": after},
        {"tensor": peer},
        {"dp": dp_y, "tensor": peer},
    ):
        pl.semaphore_signal(barrier, inc=1, device_id=where, device_id_type=MESH)
    pl.semaphore_wait(barrier, 9)

    def remote(src, dst, send, recv, where):
        copy = pltpu.make_async_remote_copy(
            src_ref=src, dst_ref=dst, send_sem=send, recv_sem=recv, device_id=where, device_id_type=MESH
        )
        copy.start()

    def arrived(ref, sem):
        pltpu.make_async_copy(ref, ref, sem).wait()

    columns = pl.ds(pl.multiple_of(core * CORE, 128), CORE)

    def piece(zz, q, first, count):
        return wbuf.at[pl.ds(pl.multiple_of((zz * 2 + q) * SHARD + first, 16), count), columns]

    chunks = ((CUT_B, SHARD - CUT_B), (0, CUT_A), (CUT_A, CUT_B - CUT_A))

    @pl.when(x % 2 == 0)
    def _():
        for number, (first, count) in enumerate(chunks):
            pltpu.make_async_copy(
                w_hbm.at[pl.ds(first, count), columns], piece(z, own_q, first, count), z_sem.at[0, number]
            ).start()

    @pl.when(x % 2 == 1)
    def _():
        for number, (first, count) in enumerate(chunks):
            remote(
                w_hbm.at[pl.ds(first, count), columns],
                piece(z, y, first, count),
                w_send.at[6],
                z_sem.at[0, number],
                {"dp": dp_y},
            )

    def got(zz, rel, number):
        first, count = chunks[number]
        arrived(piece(zz, own_q, first, count), z_sem.at[rel, number])

    def forward(zz, rel, number, right):
        first, count = chunks[number]
        part = piece(zz, own_q, first, count)
        there = (rel + 15) % NZ if right else (rel + 1) % NZ
        remote(
            part, part, w_send.at[0 if right else 1], z_sem.at[there, number],
            {"dp": dp_right if right else dp_left},
        )

    def share(zz, rel, number):
        first, count = chunks[number]
        part = piece(zz, own_q, first, count)
        where = ({"dp": dp_y}, {"pipe": x_right}, {"pipe": x_left})[number]
        remote(part, part, w_send.at[2 + number], xy_sem.at[rel], where)
        if number == 2:
            part = piece(zz, own_q, 0, SHARD)
            remote(part, part, w_send.at[5], d2d_sem.at[0, rel], {"pipe": partner})

    def complement(zz, rel):
        part = piece(zz, 1 - own_q, 0, SHARD)
        arrived(part, xy_sem.at[rel])
        remote(part, part, w_send.at[5], d2d_sem.at[1, rel], {"pipe": partner})

    other = pl.ds(pl.multiple_of((1 - core) * CORE, 128), CORE)

    def compute(zz, rel):
        for number in range(2):
            q = own_q if number == 0 else 1 - own_q
            rows = pl.ds(pl.multiple_of((zz * 2 + q) * SHARD, 16), SHARD)
            arrived(wbuf.at[rows, other], d2d_sem.at[number, rel])
        lhs = x3[zz]
        rows = pl.ds(pl.multiple_of(zz * PLANE, 16), PLANE)
        for n in range(TILES):
            at = slice(n * TILE, (n + 1) * TILE)
            acc[:, at] += nn(lhs, wbuf[rows, at])

    def right_z(k):
        return (z + NZ - k) % NZ

    def left_z(k):
        return (z + k) % NZ

    def prepare():
        x_copy.wait()
        down_copy.wait()
        up_copy.wait()
        gain_copy.wait()
        for number in range(8):
            x3[tensor * 8 + number] = x_own[:, number * PLANE : (number + 1) * PLANE]
        remote(x3.at[pl.ds(tensor * 8, 4)], x_pass.at[0], x_sem.at[0], x_sem.at[1], plus)
        remote(x3.at[pl.ds(tensor * 8 + 4, 4)], x_pass.at[1], x_sem.at[0], x_sem.at[2], minus)
        picked = adapter_ref[0]
        low_snd[...] = nt(downs[picked], x_own[...])
        remote(low_snd, low_rcv, small_sem.at[0], small_sem.at[1], {"tensor": peer})
        tenants = jnp.broadcast_to(tenant_ref[...], (ALL, ALL)).astype(F32)
        own = jnp.transpose(tenants)
        row = lax.broadcasted_iota(jnp.int32, (ALL, ALL), 0)
        column = lax.broadcasted_iota(jnp.int32, (ALL, ALL), 1)
        mask_ref[...] = jnp.where((tenants == own) & (row != column), 1.0, 0.0)

    def pass_on():
        arrived(x_pass.at[0], x_sem.at[1])
        half = (tensor + 1 - y) % 2
        remote(x_pass.at[0], x3.at[pl.ds(half * 8, 4)], x_sem.at[3], x_sem.at[4], plus)
        arrived(x_pass.at[1], x_sem.at[2])
        half = (tensor + y) % 2
        remote(x_pass.at[1], x3.at[pl.ds(half * 8 + 4, 4)], x_sem.at[3], x_sem.at[5], minus)

    def first_terms():
        arrived(x3.at[pl.ds(peer * 8, 4)], x_sem.at[4])
        arrived(x3.at[pl.ds(peer * 8 + 4, 4)], x_sem.at[5])
        arrived(low_rcv, small_sem.at[1])
        picked = adapter_ref[0]
        lowt[...] = (low_snd[...] + low_rcv[...]).astype(BF16)
        for n in range(TILES):
            at = slice(n * TILE, (n + 1) * TILE)
            acc[:, at] = adapter_scale * tn(lowt[...], ups[picked, :, at])

    def step(k, carry):
        rel = (NZ - k) % NZ
        zr = right_z(k)
        zl = left_z(k)

        for number in range(3):

            @pl.when(k <= 8)
            def _():
                got(zr, rel, number)

            @pl.when(k <= (7 if number < 2 else 6))
            def _():
                forward(zr, rel, number, True)

            @pl.when(k == 0)
            def _():
                forward(z, 0, number, False)

            @pl.when((k >= 1) & (k <= 7))
            def _():
                got(zl, k, number)

            @pl.when((k >= 1) & (k <= (6 if number < 2 else 7)))
            def _():
                forward(zl, k, number, False)

            @pl.when(k <= 8)
            def _():
                share(zr, rel, number)

            @pl.when((k >= 1) & (k <= 7))
            def _():
                share(zl, k, number)

        @pl.when(k == 0)
        def _():
            prepare()

        @pl.when(k == 2)
        def _():
            pass_on()

        @pl.when(k == LAG)
        def _():
            first_terms()

        @pl.when(k >= LAG)
        def _():
            compute(right_z(k - LAG), (NZ + LAG - k) % NZ)

        @pl.when((k >= LAG + 1) & (k <= LAG + 7))
        def _():
            compute(left_z(k - LAG), k - LAG)

        @pl.when((k >= 2) & (k <= 10))
        def _():
            complement(right_z(k - 2), (NZ + 2 - k) % NZ)

        @pl.when((k >= 3) & (k <= 9))
        def _():
            complement(left_z(k - 2), k - 2)

        return carry

    lax.fori_loop(0, LAG + 9, step, 0)

    picked = adapter_ref[0]

    out = acc[...]
    tok_snd[...] = as_lanes((jnp.sum(out * out, axis=1, keepdims=True),))
    remote(tok_snd, tok_rcv, small_sem.at[2], small_sem.at[3], {"tensor": peer})
    arrived(tok_rcv, small_sem.at[3])
    squares = as_columns(tok_snd[...] + tok_rcv[...])[:, 0:1]
    token_inv = lax.rsqrt(squares / WIDTH + epsilon)
    gained = acc[...] * gain_ref[...]
    pooled = jnp.sum((gained * token_inv).reshape(ROWS, SEQ, HALF), axis=1) * (1.0 / SEQ)
    pooled_ref[...] = pooled
    e3[dp] = pooled.astype(BF16)

    def row_of(rel, yy):
        return e3.at[((z + rel) % NZ) * 2 + yy]

    def e_send_z(rel, hops, half=None):
        part = row_of(rel, y)
        if half is not None:
            part = part.at[:, pl.ds(half * CORE, CORE)]
        remote(
            part, part, e_send.at[0], ez_sem.at[(rel - hops) % NZ], {"dp": (dp + 32 + 2 * hops) % 32}
        )

    def e_send_y(rel):
        part = row_of(rel, y)
        remote(part, part, e_send.at[1], ey_sem.at[rel], {"dp": dp_y})

    def e_send_diagonal(hops):
        part = row_of(8, y)
        remote(
            part, part, e_send.at[0], ey_sem.at[8 - hops], {"dp": (dp_y + 32 + 2 * hops) % 32}
        )

    for hops in (4, -4, 1, -1, 2, -2):
        e_send_z(0, hops)
    e_send_y(0)
    gained_ref[...] = (acc[...] * gain_ref[...]).astype(BF16)
    for rel in (15, 1, 14, 2, 12, 4, 11, 3, 13, 5, 10, 6, 8, 7, 9):
        arrived(row_of(rel, y), ez_sem.at[rel])
        if rel == 12:
            e_send_z(12, 4, 0)
        if rel == 4:
            e_send_z(4, -4, 1)
        if rel % 4 == 0:
            e_send_z(rel, 1)
            e_send_z(rel, -1)
        if rel == 12:
            e_send_z(12, 2)
        if rel == 4:
            e_send_z(4, -2)
        if rel == 8:
            e_send_diagonal(1)
            e_send_diagonal(-1)
        if rel not in (7, 9):
            e_send_y(rel)

    def e_last(rel, carry):
        arrived(e3.at[((z + rel) % NZ) * 2 + 1 - y], ey_sem.at[rel])
        return carry

    lax.fori_loop(0, NZ, e_last, 0)
    e2[...] = e3[...].astype(F32).reshape(ALL, HALF).astype(BF16)

    row = lax.broadcasted_iota(jnp.int32, (TOK, TOK), 0)
    column = lax.broadcasted_iota(jnp.int32, (TOK, TOK), 1)
    upper, lower = e2[0:TOK, :], e2[TOK:ALL, :]
    corner = nt(lower, lower)
    s_snd[0:TOK, :] = nt(upper, lower)
    s_snd[TOK:ALL, :] = jnp.where(row >= column, nt(upper, upper), corner)
    s_snd[ALL:, :] = jnp.broadcast_to(
        jnp.sum(jnp.where(row == column, corner, 0.0), axis=0, keepdims=True), (8, TOK)
    )
    remote(s_snd, s_rcv, small_sem.at[4], small_sem.at[5], {"tensor": peer})
    t_snd[...] = nt(gained_ref[...], e2[...]).astype(BF16)
    remote(t_snd, t_rcv, small_sem.at[6], small_sem.at[7], {"tensor": peer})
    arrived(s_rcv, small_sem.at[5])
    block = s_snd[0:TOK, :] + s_rcv[0:TOK, :]
    both = s_snd[TOK:ALL, :] + s_rcv[TOK:ALL, :]
    below = jnp.where(row > column, both, 0.0)
    above = jnp.where(row < column, both, 0.0)
    corner = jnp.broadcast_to(s_snd[ALL : ALL + 1, :] + s_rcv[ALL : ALL + 1, :], (TOK, TOK))
    s_all[0:TOK, 0:TOK] = jnp.where(row >= column, both, 0.0) + jnp.transpose(below)
    s_all[0:TOK, TOK:ALL] = block
    s_all[TOK:ALL, 0:TOK] = jnp.transpose(block)
    s_all[TOK:ALL, TOK:ALL] = above + jnp.transpose(above) + jnp.where(row == column, corner, 0.0)
    row = lax.broadcasted_iota(jnp.int32, (ALL, ALL), 0)
    column = lax.broadcasted_iota(jnp.int32, (ALL, ALL), 1)
    raw = s_all[...]
    diagonal = jnp.where(row == column, raw, 0.0)
    inverse_row = lax.rsqrt(jnp.sum(diagonal, axis=0, keepdims=True) + epsilon)
    inverse_column = lax.rsqrt(jnp.sum(diagonal, axis=1, keepdims=True) + epsilon)
    scores = raw * inverse_column * inverse_row / logit_divisor
    exps = jnp.where(mask_ref[...] > 0.0, jnp.exp(scores), 0.0)
    total_row = jnp.log(jnp.sum(exps, axis=0, keepdims=True))
    own_rows = pl.ds(pl.multiple_of(dp * ROWS, ROWS), ROWS)
    own_raw = s_all[own_rows, :]
    own_mask = mask_ref[own_rows, :]
    own_row = lax.broadcasted_iota(jnp.int32, (ROWS, ALL), 0) + dp * ROWS
    own_column = lax.broadcasted_iota(jnp.int32, (ROWS, ALL), 1)
    inverse = lax.rsqrt(
        jnp.sum(jnp.where(own_row == own_column, own_raw, 0.0), axis=1, keepdims=True) + epsilon
    )
    own_scores = own_raw * inverse * inverse_row / logit_divisor
    mated = own_column == own_row + 1 - 2 * (own_row % 2)
    allowed = own_mask > 0.0
    total = jnp.log(jnp.sum(jnp.where(allowed, jnp.exp(own_scores), 0.0), axis=1, keepdims=True))
    positive = jnp.sum(jnp.where(mated, own_scores, 0.0), axis=1, keepdims=True)
    loss = jnp.broadcast_to(total - positive, (ROWS, TOK))
    loss_ref[...] = jnp.transpose(loss)[0:1, :]
    both = jnp.where(allowed, jnp.exp(own_scores - total) + jnp.exp(own_scores - total_row), 0.0)
    weights = loss_scale * (both - jnp.where(mated, 2.0, 0.0))
    rounded = (weights * inverse_row).astype(BF16)
    grad_emb = nn(rounded, e2[...]) / logit_divisor
    rounded = rounded.astype(F32) / logit_divisor
    unit = pooled_ref[...] * inverse
    along = inverse * jnp.sum(rounded * own_raw, axis=1, keepdims=True)
    factors = rounded - jnp.where(own_row == own_column, along * inverse, 0.0)
    arrived(t_rcv, small_sem.at[7])
    meets = t_snd[...].astype(F32) + t_rcv[...].astype(F32)
    inverse_tokens = per_token(jnp.broadcast_to(inverse, (ROWS, TOK)))[:, 0:1]
    inner = inverse_tokens * jnp.sum(per_token(factors) * meets, axis=1, keepdims=True) * (1.0 / SEQ)
    spread = per_token(inverse * (grad_emb - unit * along) * gain_ref[...] * (1.0 / SEQ))
    pull = inner * token_inv * token_inv * (1.0 / WIDTH)
    go[...] = (token_inv * (spread - acc[...] * pull)).astype(BF16)

    gl_snd[...] = adapter_scale * nt(ups[picked], go[...])
    remote(gl_snd, gl_rcv, small_sem.at[8], small_sem.at[9], {"tensor": peer})

    owner = z < OWNERS

    def far_first(number):
        away = 8 - (number + 1) // 2
        return (number % 2) * away + (1 - number % 2) * (NZ - away)

    def scatter(buffer, values, kind):
        for number in range(OWNERS):
            buffer[number] = values[:, number * 128 : (number + 1) * 128].astype(BF16)

        @pl.when((y == kind) & owner)
        def _():
            rs_rcv[dp] = buffer[jnp.minimum(z, OWNERS - 1)]

        def one(number, carry):
            zz = (z + far_first(number)) % NZ
            there = zz * 2 + kind

            @pl.when((zz < OWNERS) & (there != dp))
            def _():
                remote(
                    buffer.at[zz], rs_rcv.at[dp], rs_sem.at[kind], rs_sem.at[2], {"dp": there}
                )

            return carry

        lax.fori_loop(0, NZ, one, 0)

    scatter(rs_up, adapter_scale * nn(lowt[...], go[...]), 0)

    def part_step(j, carry):
        rows = pl.ds(pl.multiple_of(peer * HALF + j * TILE, TILE), TILE)
        part_snd[j] = nt(go[...], wbuf[rows, :]).astype(BF16)
        remote(part_snd.at[j], part_rcv.at[j], part_sem.at[TILES], part_sem.at[j], {"tensor": peer})
        return carry

    arrived(gl_rcv, small_sem.at[9])
    glt[...] = (gl_snd[...] + gl_rcv[...]).astype(BF16)
    scatter(rs_down, nn(glt[...], x_own[...]), 1)

    lax.fori_loop(0, TILES, part_step, 0)

    def own_step(j, carry):
        rows = pl.ds(pl.multiple_of(tensor * HALF + j * TILE, TILE), TILE)
        at = pl.ds(pl.multiple_of(j * TILE, TILE), TILE)
        own_part[j] = nt(go[...], wbuf[rows, :]) + tn(glt[...], downs[picked, :, at])
        return carry

    lax.fori_loop(0, TILES, own_step, 0)

    @pl.when(owner)
    def _():
        arrived(rs_rcv.at[pl.ds(0, 31)], rs_sem.at[2])
        mine = ag.at[y * OWNERS + jnp.minimum(z, OWNERS - 1)]
        mine[...] = jnp.sum(rs_rcv[...].astype(F32), axis=0).astype(BF16)

        def one(number, carry):
            off = far_first(number)
            remote(
                mine, mine, ag_sem.at[0], agz_sem.at[NZ - off], {"dp": ((z + off) % NZ) * 2 + y}
            )
            return carry

        remote(mine, mine, ag_sem.at[1], ag_sem.at[2], {"dp": dp_y})
        lax.fori_loop(0, NZ - 1, one, 0)

    def gin_step(j, carry):
        at = pl.ds(pl.multiple_of(j * TILE, TILE), TILE)
        arrived(part_rcv.at[j], part_sem.at[j])
        gin_snd[j] = (own_part[j] + part_rcv[j].astype(F32)).astype(BF16)
        remote(gin_snd.at[j], gin_ref.at[:, at], gin_sem.at[TILES], gin_sem.at[j], {"pipe": before})
        return carry

    lax.fori_loop(0, TILES, gin_step, 0)

    def ag_step(number, carry):
        rel = far_first(NZ - 2 - number)
        zz = (z + rel) % NZ

        @pl.when(zz < OWNERS)
        def _():
            part = ag.at[y * OWNERS + zz]
            arrived(part, agz_sem.at[rel])
            remote(part, part, ag_sem.at[1], ag_sem.at[2], {"dp": dp_y})

        return carry

    lax.fori_loop(0, NZ - 1, ag_step, 0)
    arrived(ag.at[pl.ds((1 - y) * OWNERS, OWNERS)], ag_sem.at[2])

    for number in range(OWNERS):
        at = slice(number * 128, (number + 1) * 128)
        gup_ref[:, at] = ag[number].astype(F32)
        gdown_ref[:, at] = ag[OWNERS + number].astype(F32)

    for number, rows in enumerate((7 * SHARD + 64, 7 * SHARD + 48, NZ * 16, NZ * 48, NZ * 48, 2 * NZ * SHARD)):
        arrived(wbuf.at[pl.ds(0, rows), pl.ds(0, CORE)], w_send.at[number])

    @pl.when(x % 2 == 1)
    def _():
        arrived(wbuf.at[pl.ds(0, SHARD), pl.ds(0, CORE)], w_send.at[6])

    arrived(x3.at[pl.ds(0, 8)], x_sem.at[0])
    arrived(x3.at[pl.ds(0, 8)], x_sem.at[3])
    arrived(low_snd, small_sem.at[0])
    arrived(tok_snd, small_sem.at[2])
    arrived(e3.at[pl.ds(0, 17)], e_send.at[0])
    arrived(e3.at[pl.ds(0, 14)], e_send.at[1])
    arrived(s_snd, small_sem.at[4])
    arrived(t_snd, small_sem.at[6])
    arrived(gl_snd, small_sem.at[8])
    arrived(part_snd, part_sem.at[TILES])
    arrived(gin_snd, gin_sem.at[TILES])
    for kind in range(2):

        @pl.when((y == kind) & owner)
        def _():
            arrived(rs_up.at[pl.ds(0, OWNERS - 1)], rs_sem.at[kind])

        @pl.when((y != kind) | (z >= OWNERS))
        def _():
            arrived(rs_up, rs_sem.at[kind])

    @pl.when(owner)
    def _():
        arrived(rs_rcv.at[pl.ds(0, NZ - 1)], ag_sem.at[0])

    arrived(rs_up, ag_sem.at[1])

    def gin_last(j, carry):
        at = pl.ds(pl.multiple_of(j * TILE, TILE), TILE)
        arrived(gin_ref.at[:, at], gin_sem.at[j])
        return carry

    lax.fori_loop(0, TILES, gin_last, 0)


def body(hidden, frozen_weight, final_norm_gain, down_maps, up_maps, tenant, adapter):
    vmem = pl.BlockSpec(memory_space=pltpu.VMEM)
    anywhere = pl.BlockSpec(memory_space=pl.ANY)
    dma = pltpu.SemaphoreType.DMA
    gin, gup, gdown, loss = pl.pallas_call(
        kernel,
        name="whole_step",
        out_shape=(
            pltpu.VMEM((TOK, HALF), BF16),
            pltpu.VMEM((RANK, HALF), F32),
            pltpu.VMEM((RANK, HALF), F32),
            pltpu.VMEM((1, ROWS), F32),
        ),
        in_specs=[
            anywhere,
            anywhere,
            anywhere,
            anywhere,
            anywhere,
            vmem,
            pl.BlockSpec(memory_space=pltpu.SMEM),
        ],
        out_specs=(anywhere, vmem, vmem, vmem),
        scratch_shapes=[
            pltpu.VMEM((1, HALF), F32),
            pltpu.VMEM((WIDTH, HALF), BF16),
            pltpu.VMEM((TOK, HALF), F32),
            pltpu.VMEM((TOK, HALF), BF16),
            pltpu.VMEM((NZ, TOK, PLANE), BF16),
            pltpu.VMEM((2, 4, TOK, PLANE), BF16),
            pltpu.VMEM((8, RANK, HALF), BF16),
            pltpu.VMEM((8, RANK, HALF), BF16),
            pltpu.VMEM((RANK, TOK), F32),
            pltpu.VMEM((RANK, TOK), F32),
            pltpu.VMEM((RANK, TOK), BF16),
            pltpu.VMEM((8, TOK), F32),
            pltpu.VMEM((8, TOK), F32),
            pltpu.VMEM((ROWS, HALF), F32),
            pltpu.VMEM((32, ROWS, HALF), BF16),
            pltpu.VMEM((ALL, HALF), BF16),
            pltpu.VMEM((ALL + 8, TOK), F32),
            pltpu.VMEM((ALL + 8, TOK), F32),
            pltpu.VMEM((ALL, ALL), F32),
            pltpu.VMEM((ALL, ALL), F32),
            pltpu.VMEM((TOK, HALF), BF16),
            pltpu.VMEM((TOK, ALL), BF16),
            pltpu.VMEM((TOK, ALL), BF16),
            pltpu.VMEM((TOK, HALF), BF16),
            pltpu.VMEM((RANK, TOK), F32),
            pltpu.VMEM((RANK, TOK), F32),
            pltpu.VMEM((RANK, TOK), BF16),
            pltpu.VMEM((TILES, TOK, TILE), BF16),
            pltpu.VMEM((TILES, TOK, TILE), BF16),
            pltpu.VMEM((TILES, TOK, TILE), F32),
            pltpu.VMEM((TILES, TOK, TILE), BF16),
            pltpu.VMEM((OWNERS, RANK, 128), BF16),
            pltpu.VMEM((OWNERS, RANK, 128), BF16),
            pltpu.VMEM((32, RANK, 128), BF16),
            pltpu.VMEM((2 * OWNERS, RANK, 128), BF16),
            dma((4,)),
            dma((NZ, 3)),
            dma((NZ,)),
            dma((2, NZ)),
            dma((7,)),
            dma((6,)),
            dma((10,)),
            dma((NZ,)),
            dma((NZ,)),
            dma((2,)),
            dma((TILES + 1,)),
            dma((TILES + 1,)),
            dma((3,)),
            dma((3,)),
            dma((NZ,)),
        ],
        compiler_params=pltpu.CompilerParams(
            collective_id=0, has_side_effects=True, vmem_limit_bytes=56 * 1024 * 1024
        ),
    )(hidden[0], frozen_weight, final_norm_gain, down_maps, up_maps, tenant, adapter)
    return gin[None], gup[None], gdown[None], loss


def solution(mesh):
    return jax.shard_map(
        body,
        mesh=mesh,
        in_specs=(
            P("pipe", "dp", "tensor"),
            P("dp", "tensor"),
            P("tensor"),
            P(None, None, "tensor"),
            P(None, None, "tensor"),
            P("pipe", None),
            P("pipe"),
        ),
        out_specs=(
            P("pipe", "dp", "tensor"),
            P("pipe", None, "tensor"),
            P("pipe", None, "tensor"),
            P("pipe", "dp"),
        ),
        check_vma=False,
    )
```

```python
import jax
import jax.numpy as jnp
from jax import lax
from jax.experimental import pallas as pl
from jax.experimental.pallas import tpu as pltpu
from jax.sharding import PartitionSpec as P

MESH = pl.DeviceIdType.MESH
F32, BF16 = jnp.float32, jnp.bfloat16

WIDTH = 3584
HALF = 1792
CORE = 896
SHARD = 112
PLANE = 224
CUT_A, CUT_B = 48, 96
NZ = 16
SEQ = 16
ROWS = 8
ALL = 256
TOK = 128
RANK = 32
OWNERS = 14
TILE = 256
TILES = 7
LAG = 4

logit_divisor = 0.05
loss_scale = 256.0
adapter_scale = 0.5
epsilon = 1e-06


def nt(a, b):
    return lax.dot_general(a, b, (((1,), (1,)), ((), ())), preferred_element_type=F32)


def tn(a, b):
    return lax.dot_general(a, b, (((0,), (0,)), ((), ())), preferred_element_type=F32)


def nn(a, b):
    return jnp.dot(a, b, preferred_element_type=F32)


def per_token(rows):
    width = rows.shape[1]
    return jnp.broadcast_to(rows[:, None, :], (ROWS, SEQ, width)).reshape(TOK, width)


def as_lanes(columns):
    lane = lax.broadcasted_iota(jnp.int32, (TOK, TOK), 1)
    packed = jnp.zeros((TOK, TOK), F32)
    for number, column in enumerate(columns):
        packed = jnp.where(lane == number, jnp.broadcast_to(column, (TOK, TOK)), packed)
    return jnp.transpose(packed)[0:8, :]


def as_columns(lanes):
    return jnp.transpose(lanes)


def kernel(
    x_hbm,
    w_hbm,
    gain_hbm,
    down_hbm,
    up_hbm,
    tenant_ref,
    adapter_ref,
    gin_ref,
    gup_ref,
    gdown_ref,
    loss_ref,
    gain_ref,
    wbuf,
    acc,
    x_own,
    x3,
    x_pass,
    downs,
    ups,
    low_snd,
    low_rcv,
    lowt,
    tok_snd,
    tok_rcv,
    pooled_ref,
    e3,
    e2,
    s_snd,
    s_rcv,
    s_all,
    mask_ref,
    gained_ref,
    t_snd,
    t_rcv,
    go,
    gl_snd,
    gl_rcv,
    glt,
    part_snd,
    part_rcv,
    own_part,
    gin_snd,
    rs_up,
    rs_down,
    rs_rcv,
    ag,
    in_sem,
    z_sem,
    xy_sem,
    d2d_sem,
    w_send,
    x_sem,
    small_sem,
    ez_sem,
    ey_sem,
    e_send,
    part_sem,
    gin_sem,
    rs_sem,
    ag_sem,
    agz_sem,
):
    dp = lax.axis_index("dp")
    pipe = lax.axis_index("pipe")
    tensor = lax.axis_index("tensor")
    z = dp // 2
    y = dp % 2
    x = pipe // 2
    core = pipe % 2
    own_q = (x + y) % 2
    dp_right = (dp + 2) % 32
    dp_left = (dp + 30) % 32
    dp_y = dp + 1 - 2 * y
    x_right = (pipe + 2) % 8
    x_left = (pipe + 6) % 8
    partner = pipe + 1 - 2 * core
    peer = 1 - tensor
    plus = {"dp": dp_y, "tensor": (tensor + y) % 2}
    minus = {"dp": dp_y, "tensor": (tensor + 1 - y) % 2}
    before = (pipe + 7) % 8
    after = (pipe + 1) % 8

    def fetch(src, dst, number):
        return pltpu.make_async_copy(src, dst, in_sem.at[number])

    x_copy = fetch(x_hbm, x_own, 0)
    down_copy = fetch(down_hbm, downs, 1)
    up_copy = fetch(up_hbm, ups, 2)
    x_copy.start()
    down_copy.start()
    up_copy.start()
    gain_copy = fetch(gain_hbm, gain_ref.at[0], 3)
    gain_copy.start()

    barrier = pltpu.get_barrier_semaphore()
    for where in (
        {"dp": dp_right},
        {"dp": dp_left},
        {"dp": dp_y},
        {"pipe": x_right},
        {"pipe": x_left},
        {"pipe": before},
        {"pipe": after},
        {"tensor": peer},
        {"dp": dp_y, "tensor": peer},
    ):
        pl.semaphore_signal(barrier, inc=1, device_id=where, device_id_type=MESH)
    pl.semaphore_wait(barrier, 9)

    def remote(src, dst, send, recv, where):
        copy = pltpu.make_async_remote_copy(
            src_ref=src, dst_ref=dst, send_sem=send, recv_sem=recv, device_id=where, device_id_type=MESH
        )
        copy.start()

    def arrived(ref, sem):
        pltpu.make_async_copy(ref, ref, sem).wait()

    columns = pl.ds(pl.multiple_of(core * CORE, 128), CORE)

    def piece(zz, q, first, count):
        return wbuf.at[pl.ds(pl.multiple_of((zz * 2 + q) * SHARD + first, 16), count), columns]

    chunks = ((CUT_B, SHARD - CUT_B), (0, CUT_A), (CUT_A, CUT_B - CUT_A))

    @pl.when(x % 2 == 0)
    def _():
        for number, (first, count) in enumerate(chunks):
            pltpu.make_async_copy(
                w_hbm.at[pl.ds(first, count), columns], piece(z, own_q, first, count), z_sem.at[0, number]
            ).start()

    @pl.when(x % 2 == 1)
    def _():
        for number, (first, count) in enumerate(chunks):
            remote(
                w_hbm.at[pl.ds(first, count), columns],
                piece(z, y, first, count),
                w_send.at[6],
                z_sem.at[0, number],
                {"dp": dp_y},
            )

    def got(zz, rel, number):
        first, count = chunks[number]
        arrived(piece(zz, own_q, first, count), z_sem.at[rel, number])

    def forward(zz, rel, number, right):
        first, count = chunks[number]
        part = piece(zz, own_q, first, count)
        there = (rel + 15) % NZ if right else (rel + 1) % NZ
        remote(
            part, part, w_send.at[0 if right else 1], z_sem.at[there, number],
            {"dp": dp_right if right else dp_left},
        )

    def share(zz, rel, number):
        first, count = chunks[number]
        part = piece(zz, own_q, first, count)
        where = ({"dp": dp_y}, {"pipe": x_right}, {"pipe": x_left})[number]
        remote(part, part, w_send.at[2 + number], xy_sem.at[rel], where)
        if number == 2:
            part = piece(zz, own_q, 0, SHARD)
            remote(part, part, w_send.at[5], d2d_sem.at[0, rel], {"pipe": partner})

    def complement(zz, rel):
        part = piece(zz, 1 - own_q, 0, SHARD)
        arrived(part, xy_sem.at[rel])
        remote(part, part, w_send.at[5], d2d_sem.at[1, rel], {"pipe": partner})

    other = pl.ds(pl.multiple_of((1 - core) * CORE, 128), CORE)

    def compute(zz, rel):
        for number in range(2):
            q = own_q if number == 0 else 1 - own_q
            rows = pl.ds(pl.multiple_of((zz * 2 + q) * SHARD, 16), SHARD)
            arrived(wbuf.at[rows, other], d2d_sem.at[number, rel])
        lhs = x3[zz]
        rows = pl.ds(pl.multiple_of(zz * PLANE, 16), PLANE)
        for n in range(TILES):
            at = slice(n * TILE, (n + 1) * TILE)
            acc[:, at] += nn(lhs, wbuf[rows, at])

    def right_z(k):
        return (z + NZ - k) % NZ

    def left_z(k):
        return (z + k) % NZ

    def prepare():
        x_copy.wait()
        down_copy.wait()
        up_copy.wait()
        gain_copy.wait()
        for number in range(8):
            x3[tensor * 8 + number] = x_own[:, number * PLANE : (number + 1) * PLANE]
        remote(x3.at[pl.ds(tensor * 8, 4)], x_pass.at[0], x_sem.at[0], x_sem.at[1], plus)
        remote(x3.at[pl.ds(tensor * 8 + 4, 4)], x_pass.at[1], x_sem.at[0], x_sem.at[2], minus)
        picked = adapter_ref[0]
        low_snd[...] = nt(downs[picked], x_own[...])
        remote(low_snd, low_rcv, small_sem.at[0], small_sem.at[1], {"tensor": peer})
        tenants = jnp.broadcast_to(tenant_ref[...], (ALL, ALL)).astype(F32)
        own = jnp.transpose(tenants)
        row = lax.broadcasted_iota(jnp.int32, (ALL, ALL), 0)
        column = lax.broadcasted_iota(jnp.int32, (ALL, ALL), 1)
        mask_ref[...] = jnp.where((tenants == own) & (row != column), 1.0, 0.0)

    def pass_on():
        arrived(x_pass.at[0], x_sem.at[1])
        half = (tensor + 1 - y) % 2
        remote(x_pass.at[0], x3.at[pl.ds(half * 8, 4)], x_sem.at[3], x_sem.at[4], plus)
        arrived(x_pass.at[1], x_sem.at[2])
        half = (tensor + y) % 2
        remote(x_pass.at[1], x3.at[pl.ds(half * 8 + 4, 4)], x_sem.at[3], x_sem.at[5], minus)

    def first_terms():
        arrived(x3.at[pl.ds(peer * 8, 4)], x_sem.at[4])
        arrived(x3.at[pl.ds(peer * 8 + 4, 4)], x_sem.at[5])
        arrived(low_rcv, small_sem.at[1])
        picked = adapter_ref[0]
        lowt[...] = (low_snd[...] + low_rcv[...]).astype(BF16)
        for n in range(TILES):
            at = slice(n * TILE, (n + 1) * TILE)
            acc[:, at] = adapter_scale * tn(lowt[...], ups[picked, :, at])

    def step(k, carry):
        rel = (NZ - k) % NZ
        zr = right_z(k)
        zl = left_z(k)

        for number in range(3):

            @pl.when(k <= 8)
            def _():
                got(zr, rel, number)

            @pl.when(k <= (7 if number < 2 else 6))
            def _():
                forward(zr, rel, number, True)

            @pl.when(k == 0)
            def _():
                forward(z, 0, number, False)

            @pl.when((k >= 1) & (k <= 7))
            def _():
                got(zl, k, number)

            @pl.when((k >= 1) & (k <= (6 if number < 2 else 7)))
            def _():
                forward(zl, k, number, False)

            @pl.when(k <= 8)
            def _():
                share(zr, rel, number)

            @pl.when((k >= 1) & (k <= 7))
            def _():
                share(zl, k, number)

        @pl.when(k == 0)
        def _():
            prepare()

        @pl.when(k == 2)
        def _():
            pass_on()

        @pl.when(k == LAG)
        def _():
            first_terms()

        @pl.when(k >= LAG)
        def _():
            compute(right_z(k - LAG), (NZ + LAG - k) % NZ)

        @pl.when((k >= LAG + 1) & (k <= LAG + 7))
        def _():
            compute(left_z(k - LAG), k - LAG)

        @pl.when((k >= 2) & (k <= 10))
        def _():
            complement(right_z(k - 2), (NZ + 2 - k) % NZ)

        @pl.when((k >= 3) & (k <= 9))
        def _():
            complement(left_z(k - 2), k - 2)

        return carry

    lax.fori_loop(0, LAG + 9, step, 0)

    picked = adapter_ref[0]

    out = acc[...]
    tok_snd[...] = as_lanes((jnp.sum(out * out, axis=1, keepdims=True),))
    remote(tok_snd, tok_rcv, small_sem.at[2], small_sem.at[3], {"tensor": peer})
    arrived(tok_rcv, small_sem.at[3])
    squares = as_columns(tok_snd[...] + tok_rcv[...])[:, 0:1]
    token_inv = lax.rsqrt(squares / WIDTH + epsilon)
    gained = acc[...] * gain_ref[...]
    pooled = jnp.sum((gained * token_inv).reshape(ROWS, SEQ, HALF), axis=1) * (1.0 / SEQ)
    pooled_ref[...] = pooled
    e3[dp] = pooled.astype(BF16)

    def row_of(rel, yy):
        return e3.at[((z + rel) % NZ) * 2 + yy]

    def e_send_z(rel, hops, half=None, across=False):
        part = row_of(rel, y)
        if half is not None:
            part = part.at[:, pl.ds(half * CORE, CORE)]
        there = (rel - hops) % NZ
        to = dp_y if across else dp
        remote(
            part,
            part,
            e_send.at[0],
            ey_sem.at[there] if across else ez_sem.at[there],
            {"dp": (to + 32 + 2 * hops) % 32},
        )

    def e_send_y(rel):
        part = row_of(rel, y)
        remote(part, part, e_send.at[1], ey_sem.at[rel], {"dp": dp_y})

    for hops in (6, -6, 3, -3, 1, -1):
        e_send_z(0, hops)
    e_send_y(0)
    gained_ref[...] = (acc[...] * gain_ref[...]).astype(BF16)
    for rel in (15, 1, 13, 3, 10, 6, 14, 2, 12, 4, 11, 5, 9, 7, 8):
        arrived(row_of(rel, y), ez_sem.at[rel])
        if rel in (3, 13):
            for hops in (1, -1):
                e_send_z(rel, hops)
        if rel in (6, 10):
            for across in (True, False):
                for hops in (1, -1):
                    e_send_z(rel, hops, across=across)
                if rel == 6:
                    e_send_z(6, -2, 0, across)
                else:
                    e_send_z(10, 2, 1, across)
        if rel not in (5, 7, 8, 9, 11):
            e_send_y(rel)

    def e_last(rel, carry):
        arrived(e3.at[((z + rel) % NZ) * 2 + 1 - y], ey_sem.at[rel])
        return carry

    lax.fori_loop(0, NZ, e_last, 0)
    e2[...] = e3[...].astype(F32).reshape(ALL, HALF).astype(BF16)

    row = lax.broadcasted_iota(jnp.int32, (TOK, TOK), 0)
    column = lax.broadcasted_iota(jnp.int32, (TOK, TOK), 1)
    upper, lower = e2[0:TOK, :], e2[TOK:ALL, :]
    corner = nt(lower, lower)
    s_snd[0:TOK, :] = nt(upper, lower)
    s_snd[TOK:ALL, :] = jnp.where(row >= column, nt(upper, upper), corner)
    s_snd[ALL:, :] = jnp.broadcast_to(
        jnp.sum(jnp.where(row == column, corner, 0.0), axis=0, keepdims=True), (8, TOK)
    )
    remote(s_snd, s_rcv, small_sem.at[4], small_sem.at[5], {"tensor": peer})
    t_snd[...] = nt(gained_ref[...], e2[...]).astype(BF16)
    remote(t_snd, t_rcv, small_sem.at[6], small_sem.at[7], {"tensor": peer})
    arrived(s_rcv, small_sem.at[5])
    block = s_snd[0:TOK, :] + s_rcv[0:TOK, :]
    both = s_snd[TOK:ALL, :] + s_rcv[TOK:ALL, :]
    below = jnp.where(row > column, both, 0.0)
    above = jnp.where(row < column, both, 0.0)
    corner = jnp.broadcast_to(s_snd[ALL : ALL + 1, :] + s_rcv[ALL : ALL + 1, :], (TOK, TOK))
    s_all[0:TOK, 0:TOK] = jnp.where(row >= column, both, 0.0) + jnp.transpose(below)
    s_all[0:TOK, TOK:ALL] = block
    s_all[TOK:ALL, 0:TOK] = jnp.transpose(block)
    s_all[TOK:ALL, TOK:ALL] = above + jnp.transpose(above) + jnp.where(row == column, corner, 0.0)
    row = lax.broadcasted_iota(jnp.int32, (ALL, ALL), 0)
    column = lax.broadcasted_iota(jnp.int32, (ALL, ALL), 1)
    raw = s_all[...]
    diagonal = jnp.where(row == column, raw, 0.0)
    inverse_row = lax.rsqrt(jnp.sum(diagonal, axis=0, keepdims=True) + epsilon)
    inverse_column = lax.rsqrt(jnp.sum(diagonal, axis=1, keepdims=True) + epsilon)
    scores = raw * inverse_column * inverse_row / logit_divisor
    exps = jnp.where(mask_ref[...] > 0.0, jnp.exp(scores), 0.0)
    total_row = jnp.log(jnp.sum(exps, axis=0, keepdims=True))
    own_rows = pl.ds(pl.multiple_of(dp * ROWS, ROWS), ROWS)
    own_raw = s_all[own_rows, :]
    own_mask = mask_ref[own_rows, :]
    own_row = lax.broadcasted_iota(jnp.int32, (ROWS, ALL), 0) + dp * ROWS
    own_column = lax.broadcasted_iota(jnp.int32, (ROWS, ALL), 1)
    inverse = lax.rsqrt(
        jnp.sum(jnp.where(own_row == own_column, own_raw, 0.0), axis=1, keepdims=True) + epsilon
    )
    own_scores = own_raw * inverse * inverse_row / logit_divisor
    mated = own_column == own_row + 1 - 2 * (own_row % 2)
    allowed = own_mask > 0.0
    total = jnp.log(jnp.sum(jnp.where(allowed, jnp.exp(own_scores), 0.0), axis=1, keepdims=True))
    positive = jnp.sum(jnp.where(mated, own_scores, 0.0), axis=1, keepdims=True)
    loss = jnp.broadcast_to(total - positive, (ROWS, TOK))
    loss_ref[...] = jnp.transpose(loss)[0:1, :]
    both = jnp.where(allowed, jnp.exp(own_scores - total) + jnp.exp(own_scores - total_row), 0.0)
    weights = loss_scale * (both - jnp.where(mated, 2.0, 0.0))
    rounded = (weights * inverse_row).astype(BF16)
    grad_emb = nn(rounded, e2[...]) / logit_divisor
    rounded = rounded.astype(F32) / logit_divisor
    unit = pooled_ref[...] * inverse
    along = inverse * jnp.sum(rounded * own_raw, axis=1, keepdims=True)
    factors = rounded - jnp.where(own_row == own_column, along * inverse, 0.0)
    arrived(t_rcv, small_sem.at[7])
    meets = t_snd[...].astype(F32) + t_rcv[...].astype(F32)
    inverse_tokens = per_token(jnp.broadcast_to(inverse, (ROWS, TOK)))[:, 0:1]
    inner = inverse_tokens * jnp.sum(per_token(factors) * meets, axis=1, keepdims=True) * (1.0 / SEQ)
    spread = per_token(inverse * (grad_emb - unit * along) * gain_ref[...] * (1.0 / SEQ))
    pull = inner * token_inv * token_inv * (1.0 / WIDTH)
    go[...] = (token_inv * (spread - acc[...] * pull)).astype(BF16)

    gl_snd[...] = adapter_scale * nt(ups[picked], go[...])
    remote(gl_snd, gl_rcv, small_sem.at[8], small_sem.at[9], {"tensor": peer})

    owner = z < OWNERS

    def far_first(number):
        away = 8 - (number + 1) // 2
        return (number % 2) * away + (1 - number % 2) * (NZ - away)

    def scatter(buffer, values, kind):
        for number in range(OWNERS):
            buffer[number] = values[:, number * 128 : (number + 1) * 128].astype(BF16)

        @pl.when((y == kind) & owner)
        def _():
            rs_rcv[dp] = buffer[jnp.minimum(z, OWNERS - 1)]

        def one(number, carry):
            zz = (z + far_first(number)) % NZ
            there = zz * 2 + kind

            @pl.when((zz < OWNERS) & (there != dp))
            def _():
                remote(
                    buffer.at[zz], rs_rcv.at[dp], rs_sem.at[kind], rs_sem.at[2], {"dp": there}
                )

            return carry

        lax.fori_loop(0, NZ, one, 0)

    scatter(rs_up, adapter_scale * nn(lowt[...], go[...]), 0)

    def part_step(j, carry):
        rows = pl.ds(pl.multiple_of(peer * HALF + j * TILE, TILE), TILE)
        part_snd[j] = nt(go[...], wbuf[rows, :]).astype(BF16)
        remote(part_snd.at[j], part_rcv.at[j], part_sem.at[TILES], part_sem.at[j], {"tensor": peer})
        return carry

    lax.fori_loop(0, 2, part_step, 0)

    arrived(gl_rcv, small_sem.at[9])
    glt[...] = (gl_snd[...] + gl_rcv[...]).astype(BF16)
    scatter(rs_down, nn(glt[...], x_own[...]), 1)

    lax.fori_loop(2, TILES, part_step, 0)

    def own_step(j, carry):
        rows = pl.ds(pl.multiple_of(tensor * HALF + j * TILE, TILE), TILE)
        at = pl.ds(pl.multiple_of(j * TILE, TILE), TILE)
        own_part[j] = nt(go[...], wbuf[rows, :]) + tn(glt[...], downs[picked, :, at])
        return carry

    lax.fori_loop(0, TILES, own_step, 0)

    @pl.when(owner)
    def _():
        arrived(rs_rcv.at[pl.ds(0, 31)], rs_sem.at[2])
        mine = ag.at[y * OWNERS + jnp.minimum(z, OWNERS - 1)]
        mine[...] = jnp.sum(rs_rcv[...].astype(F32), axis=0).astype(BF16)

        def one(number, carry):
            off = far_first(number)
            remote(
                mine, mine, ag_sem.at[0], agz_sem.at[NZ - off], {"dp": ((z + off) % NZ) * 2 + y}
            )
            return carry

        remote(mine, mine, ag_sem.at[1], ag_sem.at[2], {"dp": dp_y})
        lax.fori_loop(0, NZ - 1, one, 0)

    def gin_step(j, carry):
        at = pl.ds(pl.multiple_of(j * TILE, TILE), TILE)
        arrived(part_rcv.at[j], part_sem.at[j])
        gin_snd[j] = (own_part[j] + part_rcv[j].astype(F32)).astype(BF16)
        remote(gin_snd.at[j], gin_ref.at[:, at], gin_sem.at[TILES], gin_sem.at[j], {"pipe": before})
        return carry

    lax.fori_loop(0, TILES, gin_step, 0)

    def ag_step(number, carry):
        rel = far_first(NZ - 2 - number)
        zz = (z + rel) % NZ

        @pl.when(zz < OWNERS)
        def _():
            part = ag.at[y * OWNERS + zz]
            arrived(part, agz_sem.at[rel])
            remote(part, part, ag_sem.at[1], ag_sem.at[2], {"dp": dp_y})

        return carry

    lax.fori_loop(0, NZ - 1, ag_step, 0)
    arrived(ag.at[pl.ds((1 - y) * OWNERS, OWNERS)], ag_sem.at[2])

    for number in range(OWNERS):
        at = slice(number * 128, (number + 1) * 128)
        gup_ref[:, at] = ag[number].astype(F32)
        gdown_ref[:, at] = ag[OWNERS + number].astype(F32)

    for number, rows in enumerate((7 * SHARD + 64, 7 * SHARD + 48, NZ * 16, NZ * 48, NZ * 48, 2 * NZ * SHARD)):
        arrived(wbuf.at[pl.ds(0, rows), pl.ds(0, CORE)], w_send.at[number])

    @pl.when(x % 2 == 1)
    def _():
        arrived(wbuf.at[pl.ds(0, SHARD), pl.ds(0, CORE)], w_send.at[6])

    arrived(x3.at[pl.ds(0, 8)], x_sem.at[0])
    arrived(x3.at[pl.ds(0, 8)], x_sem.at[3])
    arrived(low_snd, small_sem.at[0])
    arrived(tok_snd, small_sem.at[2])
    arrived(e3.at[pl.ds(0, 20)], e_send.at[0])
    arrived(e3.at[pl.ds(0, 11)], e_send.at[1])
    arrived(s_snd, small_sem.at[4])
    arrived(t_snd, small_sem.at[6])
    arrived(gl_snd, small_sem.at[8])
    arrived(part_snd, part_sem.at[TILES])
    arrived(gin_snd, gin_sem.at[TILES])
    for kind in range(2):

        @pl.when((y == kind) & owner)
        def _():
            arrived(rs_up.at[pl.ds(0, OWNERS - 1)], rs_sem.at[kind])

        @pl.when((y != kind) | (z >= OWNERS))
        def _():
            arrived(rs_up, rs_sem.at[kind])

    @pl.when(owner)
    def _():
        arrived(rs_rcv.at[pl.ds(0, NZ - 1)], ag_sem.at[0])

    arrived(rs_up, ag_sem.at[1])

    def gin_last(j, carry):
        at = pl.ds(pl.multiple_of(j * TILE, TILE), TILE)
        arrived(gin_ref.at[:, at], gin_sem.at[j])
        return carry

    lax.fori_loop(0, TILES, gin_last, 0)


def put_out(gin, gup, gdown, loss, gin_hbm, gup_hbm, gdown_hbm, loss_hbm, sems):
    copies = [
        pltpu.make_async_copy(src, dst, sems.at[number])
        for number, (src, dst) in enumerate(
            ((gin, gin_hbm), (gup, gup_hbm), (gdown, gdown_hbm), (loss, loss_hbm))
        )
    ]
    for copy in copies:
        copy.start()
    for copy in copies:
        copy.wait()


def body(hidden, frozen_weight, final_norm_gain, down_maps, up_maps, tenant, adapter):
    vmem = pl.BlockSpec(memory_space=pltpu.VMEM)
    anywhere = pl.BlockSpec(memory_space=pl.ANY)
    dma = pltpu.SemaphoreType.DMA
    gin, gup, gdown, loss = pl.pallas_call(
        kernel,
        name="whole_step",
        out_shape=(
            pltpu.VMEM((TOK, HALF), BF16),
            pltpu.VMEM((RANK, HALF), F32),
            pltpu.VMEM((RANK, HALF), F32),
            pltpu.VMEM((1, ROWS), F32),
        ),
        in_specs=[
            anywhere,
            anywhere,
            anywhere,
            anywhere,
            anywhere,
            vmem,
            pl.BlockSpec(memory_space=pltpu.SMEM),
        ],
        out_specs=(anywhere, vmem, vmem, vmem),
        scratch_shapes=[
            pltpu.VMEM((1, HALF), F32),
            pltpu.VMEM((WIDTH, HALF), BF16),
            pltpu.VMEM((TOK, HALF), F32),
            pltpu.VMEM((TOK, HALF), BF16),
            pltpu.VMEM((NZ, TOK, PLANE), BF16),
            pltpu.VMEM((2, 4, TOK, PLANE), BF16),
            pltpu.VMEM((8, RANK, HALF), BF16),
            pltpu.VMEM((8, RANK, HALF), BF16),
            pltpu.VMEM((RANK, TOK), F32),
            pltpu.VMEM((RANK, TOK), F32),
            pltpu.VMEM((RANK, TOK), BF16),
            pltpu.VMEM((8, TOK), F32),
            pltpu.VMEM((8, TOK), F32),
            pltpu.VMEM((ROWS, HALF), F32),
            pltpu.VMEM((32, ROWS, HALF), BF16),
            pltpu.VMEM((ALL, HALF), BF16),
            pltpu.VMEM((ALL + 8, TOK), F32),
            pltpu.VMEM((ALL + 8, TOK), F32),
            pltpu.VMEM((ALL, ALL), F32),
            pltpu.VMEM((ALL, ALL), F32),
            pltpu.VMEM((TOK, HALF), BF16),
            pltpu.VMEM((TOK, ALL), BF16),
            pltpu.VMEM((TOK, ALL), BF16),
            pltpu.VMEM((TOK, HALF), BF16),
            pltpu.VMEM((RANK, TOK), F32),
            pltpu.VMEM((RANK, TOK), F32),
            pltpu.VMEM((RANK, TOK), BF16),
            pltpu.VMEM((TILES, TOK, TILE), BF16),
            pltpu.VMEM((TILES, TOK, TILE), BF16),
            pltpu.VMEM((TILES, TOK, TILE), F32),
            pltpu.VMEM((TILES, TOK, TILE), BF16),
            pltpu.VMEM((OWNERS, RANK, 128), BF16),
            pltpu.VMEM((OWNERS, RANK, 128), BF16),
            pltpu.VMEM((32, RANK, 128), BF16),
            pltpu.VMEM((2 * OWNERS, RANK, 128), BF16),
            dma((4,)),
            dma((NZ, 3)),
            dma((NZ,)),
            dma((2, NZ)),
            dma((7,)),
            dma((6,)),
            dma((10,)),
            dma((NZ,)),
            dma((NZ,)),
            dma((2,)),
            dma((TILES + 1,)),
            dma((TILES + 1,)),
            dma((3,)),
            dma((3,)),
            dma((NZ,)),
        ],
        compiler_params=pltpu.CompilerParams(
            collective_id=0, has_side_effects=True, vmem_limit_bytes=56 * 1024 * 1024
        ),
    )(hidden[0], frozen_weight, final_norm_gain, down_maps, up_maps, tenant, adapter)
    gin, gup, gdown, loss = pl.pallas_call(
        put_out,
        name="put_out",
        out_shape=(
            jax.ShapeDtypeStruct((TOK, HALF), BF16),
            jax.ShapeDtypeStruct((RANK, HALF), F32),
            jax.ShapeDtypeStruct((RANK, HALF), F32),
            jax.ShapeDtypeStruct((1, ROWS), F32),
        ),
        in_specs=[vmem] * 4,
        out_specs=(anywhere,) * 4,
        scratch_shapes=[dma((4,))],
        compiler_params=pltpu.CompilerParams(vmem_limit_bytes=4 * 1024 * 1024),
    )(gin, gup, gdown, loss)
    return gin[None], gup[None], gdown[None], loss


def solution(mesh):
    return jax.shard_map(
        body,
        mesh=mesh,
        in_specs=(
            P("pipe", "dp", "tensor"),
            P("dp", "tensor"),
            P("tensor"),
            P(None, None, "tensor"),
            P(None, None, "tensor"),
            P("pipe", None),
            P("pipe"),
        ),
        out_specs=(
            P("pipe", "dp", "tensor"),
            P("pipe", None, "tensor"),
            P("pipe", None, "tensor"),
            P("pipe", "dp"),
        ),
        check_vma=False,
    )
```

```python
import jax
import jax.numpy as jnp
from jax import lax
from jax.experimental import pallas as pl
from jax.experimental.pallas import tpu as pltpu
from jax.sharding import PartitionSpec as P

MESH = pl.DeviceIdType.MESH
F32, BF16 = jnp.float32, jnp.bfloat16

WIDTH = 3584
HALF = 1792
CORE = 896
SHARD = 112
PLANE = 224
CUT_A, CUT_B = 48, 96
NZ = 16
SEQ = 16
ROWS = 8
ALL = 256
TOK = 128
RANK = 32
OWNERS = 14
TILE = 256
TILES = 7
FAR = 7
LAG = 4

logit_divisor = 0.05
loss_scale = 256.0
adapter_scale = 0.5
epsilon = 1e-06


def nt(a, b):
    return lax.dot_general(a, b, (((1,), (1,)), ((), ())), preferred_element_type=F32)


def tn(a, b):
    return lax.dot_general(a, b, (((0,), (0,)), ((), ())), preferred_element_type=F32)


def nn(a, b):
    return jnp.dot(a, b, preferred_element_type=F32)


def per_token(rows):
    width = rows.shape[1]
    return jnp.broadcast_to(rows[:, None, :], (ROWS, SEQ, width)).reshape(TOK, width)


def as_lanes(columns):
    lane = lax.broadcasted_iota(jnp.int32, (TOK, TOK), 1)
    packed = jnp.zeros((TOK, TOK), F32)
    for number, column in enumerate(columns):
        packed = jnp.where(lane == number, jnp.broadcast_to(column, (TOK, TOK)), packed)
    return jnp.transpose(packed)[0:8, :]


def as_columns(lanes):
    return jnp.transpose(lanes)


def kernel(
    x_hbm,
    w_hbm,
    gain_hbm,
    down_hbm,
    up_hbm,
    tenant_ref,
    adapter_ref,
    gin_ref,
    gup_ref,
    gdown_ref,
    loss_ref,
    gain_ref,
    wbuf,
    acc,
    x_own,
    x3,
    x_pass,
    downs,
    ups,
    low_snd,
    low_rcv,
    lowt,
    tok_snd,
    tok_rcv,
    pooled_ref,
    e3,
    e2,
    s_snd,
    s_rcv,
    s_all,
    mask_ref,
    gained_ref,
    t_snd,
    t_rcv,
    go,
    gl_snd,
    gl_rcv,
    glt,
    part_snd,
    part_rcv,
    own_part,
    gin_snd,
    rs_up,
    rs_down,
    rs_rcv,
    ag,
    in_sem,
    z_sem,
    xy_sem,
    d2d_sem,
    w_send,
    x_sem,
    small_sem,
    ez_sem,
    ey_sem,
    e_send,
    part_sem,
    gin_sem,
    rs_sem,
    ag_sem,
    agz_sem,
    ags_sem,
):
    dp = lax.axis_index("dp")
    pipe = lax.axis_index("pipe")
    tensor = lax.axis_index("tensor")
    z = dp // 2
    y = dp % 2
    x = pipe // 2
    core = pipe % 2
    own_q = (x + y) % 2
    dp_right = (dp + 2) % 32
    dp_left = (dp + 30) % 32
    dp_y = dp + 1 - 2 * y
    x_right = (pipe + 2) % 8
    x_left = (pipe + 6) % 8
    partner = pipe + 1 - 2 * core
    peer = 1 - tensor
    plus = {"dp": dp_y, "tensor": (tensor + y) % 2}
    minus = {"dp": dp_y, "tensor": (tensor + 1 - y) % 2}
    before = (pipe + 7) % 8
    after = (pipe + 1) % 8

    def fetch(src, dst, number):
        return pltpu.make_async_copy(src, dst, in_sem.at[number])

    x_copy = fetch(x_hbm, x_own, 0)
    down_copy = fetch(down_hbm, downs, 1)
    up_copy = fetch(up_hbm, ups, 2)
    x_copy.start()
    down_copy.start()
    up_copy.start()
    gain_copy = fetch(gain_hbm, gain_ref.at[0], 3)
    gain_copy.start()

    barrier = pltpu.get_barrier_semaphore()
    for where in (
        {"dp": dp_right},
        {"dp": dp_left},
        {"dp": dp_y},
        {"pipe": x_right},
        {"pipe": x_left},
        {"pipe": before},
        {"pipe": after},
        {"tensor": peer},
        {"dp": dp_y, "tensor": peer},
    ):
        pl.semaphore_signal(barrier, inc=1, device_id=where, device_id_type=MESH)
    pl.semaphore_wait(barrier, 9)

    def remote(src, dst, send, recv, where):
        copy = pltpu.make_async_remote_copy(
            src_ref=src, dst_ref=dst, send_sem=send, recv_sem=recv, device_id=where, device_id_type=MESH
        )
        copy.start()

    def arrived(ref, sem):
        pltpu.make_async_copy(ref, ref, sem).wait()

    columns = pl.ds(pl.multiple_of(core * CORE, 128), CORE)

    def piece(zz, q, first, count):
        return wbuf.at[pl.ds(pl.multiple_of((zz * 2 + q) * SHARD + first, 16), count), columns]

    chunks = ((CUT_B, SHARD - CUT_B), (0, CUT_A), (CUT_A, CUT_B - CUT_A))

    @pl.when(x % 2 == 0)
    def _():
        for number, (first, count) in enumerate(chunks):
            pltpu.make_async_copy(
                w_hbm.at[pl.ds(first, count), columns], piece(z, own_q, first, count), z_sem.at[0, number]
            ).start()

    @pl.when(x % 2 == 1)
    def _():
        for number, (first, count) in enumerate(chunks):
            remote(
                w_hbm.at[pl.ds(first, count), columns],
                piece(z, y, first, count),
                w_send.at[6],
                z_sem.at[0, number],
                {"dp": dp_y},
            )

    def got(zz, rel, number):
        first, count = chunks[number]
        arrived(piece(zz, own_q, first, count), z_sem.at[rel, number])

    def forward(zz, rel, number, right):
        first, count = chunks[number]
        part = piece(zz, own_q, first, count)
        there = (rel + 15) % NZ if right else (rel + 1) % NZ
        remote(
            part, part, w_send.at[0 if right else 1], z_sem.at[there, number],
            {"dp": dp_right if right else dp_left},
        )

    def share(zz, rel, number):
        first, count = chunks[number]
        part = piece(zz, own_q, first, count)
        where = ({"dp": dp_y}, {"pipe": x_right}, {"pipe": x_left})[number]
        remote(part, part, w_send.at[2 + number], xy_sem.at[rel], where)
        if number == 2:
            part = piece(zz, own_q, 0, SHARD)
            remote(part, part, w_send.at[5], d2d_sem.at[0, rel], {"pipe": partner})

    def complement(zz, rel):
        part = piece(zz, 1 - own_q, 0, SHARD)
        arrived(part, xy_sem.at[rel])
        remote(part, part, w_send.at[5], d2d_sem.at[1, rel], {"pipe": partner})

    other = pl.ds(pl.multiple_of((1 - core) * CORE, 128), CORE)

    def compute(zz, rel):
        for number in range(2):
            q = own_q if number == 0 else 1 - own_q
            rows = pl.ds(pl.multiple_of((zz * 2 + q) * SHARD, 16), SHARD)
            arrived(wbuf.at[rows, other], d2d_sem.at[number, rel])
        lhs = x3[zz]
        rows = pl.ds(pl.multiple_of(zz * PLANE, 16), PLANE)
        for n in range(TILES):
            at = slice(n * TILE, (n + 1) * TILE)
            acc[:, at] += nn(lhs, wbuf[rows, at])

    def right_z(k):
        return (z + NZ - k) % NZ

    def left_z(k):
        return (z + k) % NZ

    def prepare():
        x_copy.wait()
        down_copy.wait()
        up_copy.wait()
        gain_copy.wait()
        for number in range(8):
            x3[tensor * 8 + number] = x_own[:, number * PLANE : (number + 1) * PLANE]
        remote(x3.at[pl.ds(tensor * 8, 4)], x_pass.at[0], x_sem.at[0], x_sem.at[1], plus)
        remote(x3.at[pl.ds(tensor * 8 + 4, 4)], x_pass.at[1], x_sem.at[0], x_sem.at[2], minus)
        picked = adapter_ref[0]
        low_snd[...] = nt(downs[picked], x_own[...])
        remote(low_snd, low_rcv, small_sem.at[0], small_sem.at[1], {"tensor": peer})
        tenants = jnp.broadcast_to(tenant_ref[...], (ALL, ALL)).astype(F32)
        own = jnp.transpose(tenants)
        row = lax.broadcasted_iota(jnp.int32, (ALL, ALL), 0)
        column = lax.broadcasted_iota(jnp.int32, (ALL, ALL), 1)
        mask_ref[...] = jnp.where((tenants == own) & (row != column), 1.0, 0.0)

    def pass_on():
        arrived(x_pass.at[0], x_sem.at[1])
        half = (tensor + 1 - y) % 2
        remote(x_pass.at[0], x3.at[pl.ds(half * 8, 4)], x_sem.at[3], x_sem.at[4], plus)
        arrived(x_pass.at[1], x_sem.at[2])
        half = (tensor + y) % 2
        remote(x_pass.at[1], x3.at[pl.ds(half * 8 + 4, 4)], x_sem.at[3], x_sem.at[5], minus)

    def first_terms():
        arrived(x3.at[pl.ds(peer * 8, 4)], x_sem.at[4])
        arrived(x3.at[pl.ds(peer * 8 + 4, 4)], x_sem.at[5])
        arrived(low_rcv, small_sem.at[1])
        picked = adapter_ref[0]
        lowt[...] = (low_snd[...] + low_rcv[...]).astype(BF16)
        for n in range(TILES):
            at = slice(n * TILE, (n + 1) * TILE)
            acc[:, at] = adapter_scale * tn(lowt[...], ups[picked, :, at])

    def step(k, carry):
        rel = (NZ - k) % NZ
        zr = right_z(k)
        zl = left_z(k)

        for number in range(3):

            @pl.when(k <= 8)
            def _():
                got(zr, rel, number)

            @pl.when(k <= (7 if number < 2 else 6))
            def _():
                forward(zr, rel, number, True)

            @pl.when(k == 0)
            def _():
                forward(z, 0, number, False)

            @pl.when((k >= 1) & (k <= 7))
            def _():
                got(zl, k, number)

            @pl.when((k >= 1) & (k <= (6 if number < 2 else 7)))
            def _():
                forward(zl, k, number, False)

            @pl.when(k <= 8)
            def _():
                share(zr, rel, number)

            @pl.when((k >= 1) & (k <= 7))
            def _():
                share(zl, k, number)

        @pl.when(k == 0)
        def _():
            prepare()

        @pl.when(k == 2)
        def _():
            pass_on()

        @pl.when(k == LAG)
        def _():
            first_terms()

        @pl.when(k >= LAG)
        def _():
            compute(right_z(k - LAG), (NZ + LAG - k) % NZ)

        @pl.when((k >= LAG + 1) & (k <= LAG + 7))
        def _():
            compute(left_z(k - LAG), k - LAG)

        @pl.when((k >= 2) & (k <= 10))
        def _():
            complement(right_z(k - 2), (NZ + 2 - k) % NZ)

        @pl.when((k >= 3) & (k <= 9))
        def _():
            complement(left_z(k - 2), k - 2)

        return carry

    lax.fori_loop(0, LAG + 9, step, 0)

    picked = adapter_ref[0]

    out = acc[...]
    tok_snd[...] = as_lanes((jnp.sum(out * out, axis=1, keepdims=True),))
    remote(tok_snd, tok_rcv, small_sem.at[2], small_sem.at[3], {"tensor": peer})
    arrived(tok_rcv, small_sem.at[3])
    squares = as_columns(tok_snd[...] + tok_rcv[...])[:, 0:1]
    token_inv = lax.rsqrt(squares / WIDTH + epsilon)
    gained = acc[...] * gain_ref[...]
    pooled = jnp.sum((gained * token_inv).reshape(ROWS, SEQ, HALF), axis=1) * (1.0 / SEQ)
    pooled_ref[...] = pooled
    e3[dp] = pooled.astype(BF16)

    def row_of(rel, yy):
        return e3.at[((z + rel) % NZ) * 2 + yy]

    def e_send_z(rel, hops, half=None):
        part = row_of(rel, y)
        if half is not None:
            part = part.at[:, pl.ds(half * CORE, CORE)]
        remote(
            part, part, e_send.at[0], ez_sem.at[(rel - hops) % NZ], {"dp": (dp + 32 + 2 * hops) % 32}
        )

    def e_send_y(rel):
        part = row_of(rel, y)
        remote(part, part, e_send.at[1], ey_sem.at[rel], {"dp": dp_y})

    def e_send_diagonal(hops):
        part = row_of(8, y)
        remote(
            part, part, e_send.at[0], ey_sem.at[8 - hops], {"dp": (dp_y + 32 + 2 * hops) % 32}
        )

    for hops in (4, -4, 1, -1, 2, -2):
        e_send_z(0, hops)
    e_send_y(0)
    gained_ref[...] = (acc[...] * gain_ref[...]).astype(BF16)
    for rel in (15, 1, 14, 2, 12, 4, 11, 3, 13, 5, 10, 6, 8, 7, 9):
        arrived(row_of(rel, y), ez_sem.at[rel])
        if rel == 12:
            e_send_z(12, 4, 0)
        if rel == 4:
            e_send_z(4, -4, 1)
        if rel % 4 == 0:
            e_send_z(rel, 1)
            e_send_z(rel, -1)
        if rel == 12:
            e_send_z(12, 2)
        if rel == 4:
            e_send_z(4, -2)
        if rel == 8:
            e_send_diagonal(1)
            e_send_diagonal(-1)
        if rel not in (7, 9):
            e_send_y(rel)

    for rel in (0, 15, 1, 14, 2, 12, 4, 11, 3, 13, 5, 10, 6, 8, 7, 9):
        zz = (z + rel) % NZ
        arrived(row_of(rel, 1 - y), ey_sem.at[rel])
        plane = e3[pl.ds(zz * 2, 2)].astype(F32).reshape(2 * ROWS, HALF).astype(BF16)
        e2[pl.ds(pl.multiple_of(zz * 2 * ROWS, 2 * ROWS), 2 * ROWS), :] = plane

    row = lax.broadcasted_iota(jnp.int32, (TOK, TOK), 0)
    column = lax.broadcasted_iota(jnp.int32, (TOK, TOK), 1)
    upper, lower = e2[0:TOK, :], e2[TOK:ALL, :]
    corner = nt(lower, lower)
    s_snd[0:TOK, :] = nt(upper, lower)
    s_snd[TOK:ALL, :] = jnp.where(row >= column, nt(upper, upper), corner)
    s_snd[ALL:, :] = jnp.broadcast_to(
        jnp.sum(jnp.where(row == column, corner, 0.0), axis=0, keepdims=True), (8, TOK)
    )
    remote(s_snd, s_rcv, small_sem.at[4], small_sem.at[5], {"tensor": peer})
    t_snd[...] = nt(gained_ref[...], e2[...]).astype(BF16)
    remote(t_snd, t_rcv, small_sem.at[6], small_sem.at[7], {"tensor": peer})
    arrived(s_rcv, small_sem.at[5])
    block = s_snd[0:TOK, :] + s_rcv[0:TOK, :]
    both = s_snd[TOK:ALL, :] + s_rcv[TOK:ALL, :]
    below = jnp.where(row > column, both, 0.0)
    above = jnp.where(row < column, both, 0.0)
    corner = jnp.broadcast_to(s_snd[ALL : ALL + 1, :] + s_rcv[ALL : ALL + 1, :], (TOK, TOK))
    s_all[0:TOK, 0:TOK] = jnp.where(row >= column, both, 0.0) + jnp.transpose(below)
    s_all[0:TOK, TOK:ALL] = block
    s_all[TOK:ALL, 0:TOK] = jnp.transpose(block)
    s_all[TOK:ALL, TOK:ALL] = above + jnp.transpose(above) + jnp.where(row == column, corner, 0.0)
    row = lax.broadcasted_iota(jnp.int32, (ALL, ALL), 0)
    column = lax.broadcasted_iota(jnp.int32, (ALL, ALL), 1)
    raw = s_all[...]
    diagonal = jnp.where(row == column, raw, 0.0)
    inverse_row = lax.rsqrt(jnp.sum(diagonal, axis=0, keepdims=True) + epsilon)
    inverse_column = lax.rsqrt(jnp.sum(diagonal, axis=1, keepdims=True) + epsilon)
    scores = raw * inverse_column * inverse_row / logit_divisor
    exps = jnp.where(mask_ref[...] > 0.0, jnp.exp(scores), 0.0)
    total_row = jnp.log(jnp.sum(exps, axis=0, keepdims=True))
    own_rows = pl.ds(pl.multiple_of(dp * ROWS, ROWS), ROWS)
    own_raw = s_all[own_rows, :]
    own_mask = mask_ref[own_rows, :]
    own_row = lax.broadcasted_iota(jnp.int32, (ROWS, ALL), 0) + dp * ROWS
    own_column = lax.broadcasted_iota(jnp.int32, (ROWS, ALL), 1)
    inverse = lax.rsqrt(
        jnp.sum(jnp.where(own_row == own_column, own_raw, 0.0), axis=1, keepdims=True) + epsilon
    )
    own_scores = own_raw * inverse * inverse_row / logit_divisor
    mated = own_column == own_row + 1 - 2 * (own_row % 2)
    allowed = own_mask > 0.0
    total = jnp.log(jnp.sum(jnp.where(allowed, jnp.exp(own_scores), 0.0), axis=1, keepdims=True))
    positive = jnp.sum(jnp.where(mated, own_scores, 0.0), axis=1, keepdims=True)
    loss = jnp.broadcast_to(total - positive, (ROWS, TOK))
    loss_ref[...] = jnp.transpose(loss)[0:1, :]
    both = jnp.where(allowed, jnp.exp(own_scores - total) + jnp.exp(own_scores - total_row), 0.0)
    weights = loss_scale * (both - jnp.where(mated, 2.0, 0.0))
    rounded = (weights * inverse_row).astype(BF16)
    grad_emb = nn(rounded, e2[...]) / logit_divisor
    rounded = rounded.astype(F32) / logit_divisor
    unit = pooled_ref[...] * inverse
    along = inverse * jnp.sum(rounded * own_raw, axis=1, keepdims=True)
    factors = rounded - jnp.where(own_row == own_column, along * inverse, 0.0)
    arrived(t_rcv, small_sem.at[7])
    meets = t_snd[...].astype(F32) + t_rcv[...].astype(F32)
    inverse_tokens = per_token(jnp.broadcast_to(inverse, (ROWS, TOK)))[:, 0:1]
    inner = inverse_tokens * jnp.sum(per_token(factors) * meets, axis=1, keepdims=True) * (1.0 / SEQ)
    spread = per_token(inverse * (grad_emb - unit * along) * gain_ref[...] * (1.0 / SEQ))
    pull = inner * token_inv * token_inv * (1.0 / WIDTH)
    go[...] = (token_inv * (spread - acc[...] * pull)).astype(BF16)

    gl_snd[...] = adapter_scale * nt(ups[picked], go[...])
    remote(gl_snd, gl_rcv, small_sem.at[8], small_sem.at[9], {"tensor": peer})

    owner = z < OWNERS

    def far_first(number):
        away = 8 - (number + 1) // 2
        return (number % 2) * away + (1 - number % 2) * (NZ - away)

    def scatter(buffer, values, kind):
        for number in range(OWNERS):
            buffer[number] = values[:, number * 128 : (number + 1) * 128].astype(BF16)

        @pl.when((y == kind) & owner)
        def _():
            rs_rcv[dp] = buffer[jnp.minimum(z, OWNERS - 1)]

        def one(number, carry):
            zz = (z + far_first(number)) % NZ
            there = zz * 2 + kind

            @pl.when((zz < OWNERS) & (there != dp))
            def _():
                remote(
                    buffer.at[zz], rs_rcv.at[dp], rs_sem.at[kind], rs_sem.at[2], {"dp": there}
                )

            return carry

        lax.fori_loop(0, NZ, one, 0)

    scatter(rs_up, adapter_scale * nn(lowt[...], go[...]), 0)

    def part_step(j, carry):
        rows = pl.ds(pl.multiple_of(peer * HALF + j * TILE, TILE), TILE)
        part_snd[j] = nt(go[...], wbuf[rows, :]).astype(BF16)
        remote(part_snd.at[j], part_rcv.at[j], part_sem.at[TILES], part_sem.at[j], {"tensor": peer})
        return carry

    arrived(gl_rcv, small_sem.at[9])
    glt[...] = (gl_snd[...] + gl_rcv[...]).astype(BF16)
    scatter(rs_down, nn(glt[...], x_own[...]), 1)

    lax.fori_loop(0, TILES, part_step, 0)

    def own_step(j, carry):
        rows = pl.ds(pl.multiple_of(tensor * HALF + j * TILE, TILE), TILE)
        at = pl.ds(pl.multiple_of(j * TILE, TILE), TILE)
        own_part[j] = nt(go[...], wbuf[rows, :]) + tn(glt[...], downs[picked, :, at])
        return carry

    lax.fori_loop(0, TILES, own_step, 0)

    @pl.when(owner)
    def _():
        arrived(rs_rcv.at[pl.ds(0, 31)], rs_sem.at[2])
        mine = ag.at[y * OWNERS + jnp.minimum(z, OWNERS - 1)]
        mine[...] = jnp.sum(rs_rcv[...].astype(F32), axis=0).astype(BF16)

        def one(number, carry):
            off = far_first(number)
            there = ((z + off) % NZ) * 2
            remote(mine, mine, ag_sem.at[0], agz_sem.at[NZ - off], {"dp": there + y})

            @pl.when(number >= FAR)
            def _():
                remote(
                    mine, mine, ag_sem.at[0], agz_sem.at[2 * NZ - off], {"dp": there + 1 - y}
                )

            return carry

        remote(mine, mine, ags_sem.at[0], agz_sem.at[NZ], {"dp": dp_y})
        lax.fori_loop(0, NZ - 1, one, 0)

    def gin_step(j, carry):
        at = pl.ds(pl.multiple_of(j * TILE, TILE), TILE)
        arrived(part_rcv.at[j], part_sem.at[j])
        gin_snd[j] = (own_part[j] + part_rcv[j].astype(F32)).astype(BF16)
        remote(gin_snd.at[j], gin_ref.at[:, at], gin_sem.at[TILES], gin_sem.at[j], {"pipe": before})
        return carry

    lax.fori_loop(0, TILES, gin_step, 0)

    def ag_step(number, carry):
        rel = far_first(number)
        zz = (z + rel) % NZ

        @pl.when(zz < OWNERS)
        def _():
            part = ag.at[y * OWNERS + zz]
            arrived(part, agz_sem.at[rel])

            @pl.when(number < FAR)
            def _():
                remote(part, part, ags_sem.at[rel], agz_sem.at[NZ + rel], {"dp": dp_y})

        return carry

    lax.fori_loop(0, NZ - 1, ag_step, 0)

    def ag_last(rel, carry):
        zz = (z + rel) % NZ

        @pl.when(zz < OWNERS)
        def _():
            arrived(ag.at[(1 - y) * OWNERS + zz], agz_sem.at[NZ + rel])

        return carry

    lax.fori_loop(0, NZ, ag_last, 0)

    for number in range(OWNERS):
        at = slice(number * 128, (number + 1) * 128)
        gup_ref[:, at] = ag[number].astype(F32)
        gdown_ref[:, at] = ag[OWNERS + number].astype(F32)

    for number, rows in enumerate((7 * SHARD + 64, 7 * SHARD + 48, NZ * 16, NZ * 48, NZ * 48, 2 * NZ * SHARD)):
        arrived(wbuf.at[pl.ds(0, rows), pl.ds(0, CORE)], w_send.at[number])

    @pl.when(x % 2 == 1)
    def _():
        arrived(wbuf.at[pl.ds(0, SHARD), pl.ds(0, CORE)], w_send.at[6])

    arrived(x3.at[pl.ds(0, 8)], x_sem.at[0])
    arrived(x3.at[pl.ds(0, 8)], x_sem.at[3])
    arrived(low_snd, small_sem.at[0])
    arrived(tok_snd, small_sem.at[2])
    arrived(e3.at[pl.ds(0, 17)], e_send.at[0])
    arrived(e3.at[pl.ds(0, 14)], e_send.at[1])
    arrived(s_snd, small_sem.at[4])
    arrived(t_snd, small_sem.at[6])
    arrived(gl_snd, small_sem.at[8])
    arrived(part_snd, part_sem.at[TILES])
    arrived(gin_snd, gin_sem.at[TILES])
    for kind in range(2):

        @pl.when((y == kind) & owner)
        def _():
            arrived(rs_up.at[pl.ds(0, OWNERS - 1)], rs_sem.at[kind])

        @pl.when((y != kind) | (z >= OWNERS))
        def _():
            arrived(rs_up, rs_sem.at[kind])

    @pl.when(owner)
    def _():
        arrived(rs_rcv.at[pl.ds(0, 2 * (NZ - 1) - FAR)], ag_sem.at[0])
        arrived(ag.at[0], ags_sem.at[0])

    def ag_left(number, carry):
        rel = far_first(number)

        @pl.when((z + rel) % NZ < OWNERS)
        def _():
            arrived(ag.at[0], ags_sem.at[rel])

        return carry

    lax.fori_loop(0, FAR, ag_left, 0)

    def gin_last(j, carry):
        at = pl.ds(pl.multiple_of(j * TILE, TILE), TILE)
        arrived(gin_ref.at[:, at], gin_sem.at[j])
        return carry

    lax.fori_loop(0, TILES, gin_last, 0)


def put_out(gin, gup, gdown, loss, gin_hbm, gup_hbm, gdown_hbm, loss_hbm, sems):
    copies = [
        pltpu.make_async_copy(src, dst, sems.at[number])
        for number, (src, dst) in enumerate(
            ((gin, gin_hbm), (gup, gup_hbm), (gdown, gdown_hbm), (loss, loss_hbm))
        )
    ]
    for copy in copies:
        copy.start()
    for copy in copies:
        copy.wait()


def body(hidden, frozen_weight, final_norm_gain, down_maps, up_maps, tenant, adapter):
    vmem = pl.BlockSpec(memory_space=pltpu.VMEM)
    anywhere = pl.BlockSpec(memory_space=pl.ANY)
    dma = pltpu.SemaphoreType.DMA
    gin, gup, gdown, loss = pl.pallas_call(
        kernel,
        name="whole_step",
        out_shape=(
            pltpu.VMEM((TOK, HALF), BF16),
            pltpu.VMEM((RANK, HALF), F32),
            pltpu.VMEM((RANK, HALF), F32),
            pltpu.VMEM((1, ROWS), F32),
        ),
        in_specs=[
            anywhere,
            anywhere,
            anywhere,
            anywhere,
            anywhere,
            vmem,
            pl.BlockSpec(memory_space=pltpu.SMEM),
        ],
        out_specs=(anywhere, vmem, vmem, vmem),
        scratch_shapes=[
            pltpu.VMEM((1, HALF), F32),
            pltpu.VMEM((WIDTH, HALF), BF16),
            pltpu.VMEM((TOK, HALF), F32),
            pltpu.VMEM((TOK, HALF), BF16),
            pltpu.VMEM((NZ, TOK, PLANE), BF16),
            pltpu.VMEM((2, 4, TOK, PLANE), BF16),
            pltpu.VMEM((8, RANK, HALF), BF16),
            pltpu.VMEM((8, RANK, HALF), BF16),
            pltpu.VMEM((RANK, TOK), F32),
            pltpu.VMEM((RANK, TOK), F32),
            pltpu.VMEM((RANK, TOK), BF16),
            pltpu.VMEM((8, TOK), F32),
            pltpu.VMEM((8, TOK), F32),
            pltpu.VMEM((ROWS, HALF), F32),
            pltpu.VMEM((32, ROWS, HALF), BF16),
            pltpu.VMEM((ALL, HALF), BF16),
            pltpu.VMEM((ALL + 8, TOK), F32),
            pltpu.VMEM((ALL + 8, TOK), F32),
            pltpu.VMEM((ALL, ALL), F32),
            pltpu.VMEM((ALL, ALL), F32),
            pltpu.VMEM((TOK, HALF), BF16),
            pltpu.VMEM((TOK, ALL), BF16),
            pltpu.VMEM((TOK, ALL), BF16),
            pltpu.VMEM((TOK, HALF), BF16),
            pltpu.VMEM((RANK, TOK), F32),
            pltpu.VMEM((RANK, TOK), F32),
            pltpu.VMEM((RANK, TOK), BF16),
            pltpu.VMEM((TILES, TOK, TILE), BF16),
            pltpu.VMEM((TILES, TOK, TILE), BF16),
            pltpu.VMEM((TILES, TOK, TILE), F32),
            pltpu.VMEM((TILES, TOK, TILE), BF16),
            pltpu.VMEM((OWNERS, RANK, 128), BF16),
            pltpu.VMEM((OWNERS, RANK, 128), BF16),
            pltpu.VMEM((32, RANK, 128), BF16),
            pltpu.VMEM((2 * OWNERS, RANK, 128), BF16),
            dma((4,)),
            dma((NZ, 3)),
            dma((NZ,)),
            dma((2, NZ)),
            dma((7,)),
            dma((6,)),
            dma((10,)),
            dma((NZ,)),
            dma((NZ,)),
            dma((2,)),
            dma((TILES + 1,)),
            dma((TILES + 1,)),
            dma((3,)),
            dma((1,)),
            dma((2 * NZ,)),
            dma((NZ,)),
        ],
        compiler_params=pltpu.CompilerParams(
            collective_id=0, has_side_effects=True, vmem_limit_bytes=56 * 1024 * 1024
        ),
    )(hidden[0], frozen_weight, final_norm_gain, down_maps, up_maps, tenant, adapter)
    gin, gup, gdown, loss = pl.pallas_call(
        put_out,
        name="put_out",
        out_shape=(
            jax.ShapeDtypeStruct((TOK, HALF), BF16),
            jax.ShapeDtypeStruct((RANK, HALF), F32),
            jax.ShapeDtypeStruct((RANK, HALF), F32),
            jax.ShapeDtypeStruct((1, ROWS), F32),
        ),
        in_specs=[vmem] * 4,
        out_specs=(anywhere,) * 4,
        scratch_shapes=[dma((4,))],
        compiler_params=pltpu.CompilerParams(vmem_limit_bytes=4 * 1024 * 1024),
    )(gin, gup, gdown, loss)
    return gin[None], gup[None], gdown[None], loss


def solution(mesh):
    return jax.shard_map(
        body,
        mesh=mesh,
        in_specs=(
            P("pipe", "dp", "tensor"),
            P("dp", "tensor"),
            P("tensor"),
            P(None, None, "tensor"),
            P(None, None, "tensor"),
            P("pipe", None),
            P("pipe"),
        ),
        out_specs=(
            P("pipe", "dp", "tensor"),
            P("pipe", None, "tensor"),
            P("pipe", None, "tensor"),
            P("pipe", "dp"),
        ),
        check_vma=False,
    )
```

```python
import jax
import jax.numpy as jnp
from jax import lax
from jax.experimental import pallas as pl
from jax.experimental.pallas import tpu as pltpu
from jax.sharding import PartitionSpec as P

MESH = pl.DeviceIdType.MESH
F32, BF16 = jnp.float32, jnp.bfloat16

WIDTH = 3584
HALF = 1792
CORE = 896
SHARD = 112
PLANE = 224
CUT_A, CUT_B = 48, 96
NZ = 16
SEQ = 16
ROWS = 8
ALL = 256
TOK = 128
RANK = 32
OWNERS = 14
TILE = 256
TILES = 7
LAG = 5
CATCH = 9

logit_divisor = 0.05
loss_scale = 256.0
adapter_scale = 0.5
epsilon = 1e-06


def nt(a, b):
    return lax.dot_general(a, b, (((1,), (1,)), ((), ())), preferred_element_type=F32)


def tn(a, b):
    return lax.dot_general(a, b, (((0,), (0,)), ((), ())), preferred_element_type=F32)


def nn(a, b):
    return jnp.dot(a, b, preferred_element_type=F32)


def per_token(rows):
    width = rows.shape[1]
    return jnp.broadcast_to(rows[:, None, :], (ROWS, SEQ, width)).reshape(TOK, width)


def as_lanes(columns):
    lane = lax.broadcasted_iota(jnp.int32, (TOK, TOK), 1)
    packed = jnp.zeros((TOK, TOK), F32)
    for number, column in enumerate(columns):
        packed = jnp.where(lane == number, jnp.broadcast_to(column, (TOK, TOK)), packed)
    return jnp.transpose(packed)[0:8, :]


def as_columns(lanes):
    return jnp.transpose(lanes)


def kernel(
    x_hbm,
    w_hbm,
    gain_hbm,
    down_hbm,
    up_hbm,
    tenant_ref,
    adapter_ref,
    gin_ref,
    gup_ref,
    gdown_ref,
    loss_ref,
    gain_ref,
    wbuf,
    acc,
    x_own,
    x3,
    x_pass,
    downs,
    ups,
    low_snd,
    low_rcv,
    lowt,
    tok_snd,
    tok_rcv,
    pooled_ref,
    e3,
    e2,
    s_snd,
    s_rcv,
    s_all,
    mask_ref,
    gained_ref,
    t_snd,
    t_rcv,
    go,
    gl_snd,
    gl_rcv,
    glt,
    part_snd,
    part_rcv,
    own_part,
    gin_snd,
    rs_up,
    rs_down,
    rs_rcv,
    ag,
    in_sem,
    z_sem,
    xy_sem,
    d2d_sem,
    w_send,
    x_sem,
    small_sem,
    ez_sem,
    ey_sem,
    e_send,
    part_sem,
    gin_sem,
    rs_sem,
    ag_sem,
    agz_sem,
):
    dp = lax.axis_index("dp")
    pipe = lax.axis_index("pipe")
    tensor = lax.axis_index("tensor")
    z = dp // 2
    y = dp % 2
    x = pipe // 2
    core = pipe % 2
    own_q = (x + y) % 2
    dp_right = (dp + 2) % 32
    dp_left = (dp + 30) % 32
    dp_y = dp + 1 - 2 * y
    x_right = (pipe + 2) % 8
    x_left = (pipe + 6) % 8
    partner = pipe + 1 - 2 * core
    peer = 1 - tensor
    plus = {"dp": dp_y, "tensor": (tensor + y) % 2}
    minus = {"dp": dp_y, "tensor": (tensor + 1 - y) % 2}
    before = (pipe + 7) % 8
    after = (pipe + 1) % 8

    def fetch(src, dst, number):
        return pltpu.make_async_copy(src, dst, in_sem.at[number])

    x_copy = fetch(x_hbm, x_own, 0)
    down_copy = fetch(down_hbm, downs, 1)
    up_copy = fetch(up_hbm, ups, 2)
    x_copy.start()
    down_copy.start()
    up_copy.start()
    gain_copy = fetch(gain_hbm, gain_ref.at[0], 3)
    gain_copy.start()

    barrier = pltpu.get_barrier_semaphore()
    for where in (
        {"dp": dp_right},
        {"dp": dp_left},
        {"dp": dp_y},
        {"pipe": x_right},
        {"pipe": x_left},
        {"pipe": before},
        {"pipe": after},
        {"tensor": peer},
        {"dp": dp_y, "tensor": peer},
    ):
        pl.semaphore_signal(barrier, inc=1, device_id=where, device_id_type=MESH)
    pl.semaphore_wait(barrier, 9)

    def remote(src, dst, send, recv, where):
        copy = pltpu.make_async_remote_copy(
            src_ref=src, dst_ref=dst, send_sem=send, recv_sem=recv, device_id=where, device_id_type=MESH
        )
        copy.start()

    def arrived(ref, sem):
        pltpu.make_async_copy(ref, ref, sem).wait()

    columns = pl.ds(pl.multiple_of(core * CORE, 128), CORE)

    def piece(zz, q, first, count):
        return wbuf.at[pl.ds(pl.multiple_of((zz * 2 + q) * SHARD + first, 16), count), columns]

    chunks = ((CUT_B, SHARD - CUT_B), (0, CUT_A), (CUT_A, CUT_B - CUT_A))

    @pl.when(x % 2 == 0)
    def _():
        for number, (first, count) in enumerate(chunks):
            pltpu.make_async_copy(
                w_hbm.at[pl.ds(first, count), columns], piece(z, own_q, first, count), z_sem.at[0, number]
            ).start()

    @pl.when(x % 2 == 1)
    def _():
        for number, (first, count) in enumerate(chunks):
            remote(
                w_hbm.at[pl.ds(first, count), columns],
                piece(z, y, first, count),
                w_send.at[6],
                z_sem.at[0, number],
                {"dp": dp_y},
            )

    def got(zz, rel, number):
        first, count = chunks[number]
        arrived(piece(zz, own_q, first, count), z_sem.at[rel, number])

    def forward(zz, rel, number, right):
        first, count = chunks[number]
        part = piece(zz, own_q, first, count)
        there = (rel + 15) % NZ if right else (rel + 1) % NZ
        remote(
            part, part, w_send.at[0 if right else 1], z_sem.at[there, number],
            {"dp": dp_right if right else dp_left},
        )

    def share(zz, rel, number):
        first, count = chunks[number]
        part = piece(zz, own_q, first, count)
        where = ({"dp": dp_y}, {"pipe": x_right}, {"pipe": x_left})[number]
        remote(part, part, w_send.at[2 + number], xy_sem.at[rel], where)
        if number == 2:
            part = piece(zz, own_q, 0, SHARD)
            remote(part, part, w_send.at[5], d2d_sem.at[0, rel], {"pipe": partner})

    def complement(zz, rel):
        part = piece(zz, 1 - own_q, 0, SHARD)
        arrived(part, xy_sem.at[rel])
        remote(part, part, w_send.at[5], d2d_sem.at[1, rel], {"pipe": partner})

    other = pl.ds(pl.multiple_of((1 - core) * CORE, 128), CORE)

    def compute(zz, rel):
        for number in range(2):
            q = own_q if number == 0 else 1 - own_q
            rows = pl.ds(pl.multiple_of((zz * 2 + q) * SHARD, 16), SHARD)
            arrived(wbuf.at[rows, other], d2d_sem.at[number, rel])
        lhs = x3[zz]
        rows = pl.ds(pl.multiple_of(zz * PLANE, 16), PLANE)
        for n in range(TILES):
            at = slice(n * TILE, (n + 1) * TILE)
            acc[:, at] += nn(lhs, wbuf[rows, at])

    def right_z(k):
        return (z + NZ - k) % NZ

    def left_z(k):
        return (z + k) % NZ

    def prepare():
        x_copy.wait()
        down_copy.wait()
        up_copy.wait()
        gain_copy.wait()
        for number in range(8):
            x3[tensor * 8 + number] = x_own[:, number * PLANE : (number + 1) * PLANE]
        remote(x3.at[pl.ds(tensor * 8, 4)], x_pass.at[0], x_sem.at[0], x_sem.at[1], plus)
        remote(x3.at[pl.ds(tensor * 8 + 4, 4)], x_pass.at[1], x_sem.at[0], x_sem.at[2], minus)
        picked = adapter_ref[0]
        low_snd[...] = nt(downs[picked], x_own[...])
        remote(low_snd, low_rcv, small_sem.at[0], small_sem.at[1], {"tensor": peer})
        tenants = jnp.broadcast_to(tenant_ref[...], (ALL, ALL)).astype(F32)
        own = jnp.transpose(tenants)
        row = lax.broadcasted_iota(jnp.int32, (ALL, ALL), 0)
        column = lax.broadcasted_iota(jnp.int32, (ALL, ALL), 1)
        mask_ref[...] = jnp.where((tenants == own) & (row != column), 1.0, 0.0)

    def pass_on():
        arrived(x_pass.at[0], x_sem.at[1])
        half = (tensor + 1 - y) % 2
        remote(x_pass.at[0], x3.at[pl.ds(half * 8, 4)], x_sem.at[3], x_sem.at[4], plus)
        arrived(x_pass.at[1], x_sem.at[2])
        half = (tensor + y) % 2
        remote(x_pass.at[1], x3.at[pl.ds(half * 8 + 4, 4)], x_sem.at[3], x_sem.at[5], minus)

    def first_terms():
        arrived(x3.at[pl.ds(peer * 8, 4)], x_sem.at[4])
        arrived(x3.at[pl.ds(peer * 8 + 4, 4)], x_sem.at[5])
        arrived(low_rcv, small_sem.at[1])
        picked = adapter_ref[0]
        lowt[...] = (low_snd[...] + low_rcv[...]).astype(BF16)
        for n in range(TILES):
            at = slice(n * TILE, (n + 1) * TILE)
            acc[:, at] = adapter_scale * tn(lowt[...], ups[picked, :, at])

    def step(k, carry):
        rel = (NZ - k) % NZ
        zr = right_z(k)
        zl = left_z(k)

        for number in range(3):

            @pl.when(k <= 8)
            def _():
                got(zr, rel, number)

            @pl.when(k <= (7 if number < 2 else 6))
            def _():
                forward(zr, rel, number, True)

            @pl.when(k == 0)
            def _():
                forward(z, 0, number, False)

            @pl.when((k >= 1) & (k <= 7))
            def _():
                got(zl, k, number)

            @pl.when((k >= 1) & (k <= (6 if number < 2 else 7)))
            def _():
                forward(zl, k, number, False)

            @pl.when(k <= 8)
            def _():
                share(zr, rel, number)

            @pl.when((k >= 1) & (k <= 7))
            def _():
                share(zl, k, number)

        @pl.when(k == 0)
        def _():
            prepare()

        @pl.when(k == 2)
        def _():
            pass_on()

        @pl.when(k == LAG)
        def _():
            first_terms()

        for lag, begin, end in ((LAG, LAG, CATCH), (LAG - 1, CATCH, LAG + 7)):

            @pl.when((k >= begin) & (k <= end))
            def _():
                compute(right_z(k - lag), (NZ + lag - k) % NZ)

            @pl.when((k >= begin) & (k <= end) & (k >= lag + 1) & (k <= lag + 7))
            def _():
                compute(left_z(k - lag), k - lag)

        @pl.when((k >= 2) & (k <= 10))
        def _():
            complement(right_z(k - 2), (NZ + 2 - k) % NZ)

        @pl.when((k >= 3) & (k <= 9))
        def _():
            complement(left_z(k - 2), k - 2)

        return carry

    lax.fori_loop(0, LAG + 8, step, 0)

    picked = adapter_ref[0]

    out = acc[...]
    tok_snd[...] = as_lanes((jnp.sum(out * out, axis=1, keepdims=True),))
    remote(tok_snd, tok_rcv, small_sem.at[2], small_sem.at[3], {"tensor": peer})
    arrived(tok_rcv, small_sem.at[3])
    squares = as_columns(tok_snd[...] + tok_rcv[...])[:, 0:1]
    token_inv = lax.rsqrt(squares / WIDTH + epsilon)
    gained = acc[...] * gain_ref[...]
    pooled = jnp.sum((gained * token_inv).reshape(ROWS, SEQ, HALF), axis=1) * (1.0 / SEQ)
    pooled_ref[...] = pooled
    e3[dp] = pooled.astype(BF16)

    def row_of(rel, yy):
        return e3.at[((z + rel) % NZ) * 2 + yy]

    def e_send_z(rel, hops, half=None):
        part = row_of(rel, y)
        if half is not None:
            part = part.at[:, pl.ds(half * CORE, CORE)]
        remote(
            part, part, e_send.at[0], ez_sem.at[(rel - hops) % NZ], {"dp": (dp + 32 + 2 * hops) % 32}
        )

    def e_send_y(rel):
        part = row_of(rel, y)
        remote(part, part, e_send.at[1], ey_sem.at[rel], {"dp": dp_y})

    def e_send_diagonal(hops):
        part = row_of(8, y)
        remote(
            part, part, e_send.at[0], ey_sem.at[8 - hops], {"dp": (dp_y + 32 + 2 * hops) % 32}
        )

    for hops in (4, -4, 1, -1, 2, -2):
        e_send_z(0, hops)
    e_send_y(0)
    gained_ref[...] = (acc[...] * gain_ref[...]).astype(BF16)
    for rel in (15, 1, 14, 2, 12, 4, 11, 3, 13, 5, 10, 6, 8, 7, 9):
        arrived(row_of(rel, y), ez_sem.at[rel])
        if rel == 12:
            e_send_z(12, 4, 0)
        if rel == 4:
            e_send_z(4, -4, 1)
        if rel % 4 == 0:
            e_send_z(rel, 1)
            e_send_z(rel, -1)
        if rel == 12:
            e_send_z(12, 2)
        if rel == 4:
            e_send_z(4, -2)
        if rel == 8:
            e_send_diagonal(1)
            e_send_diagonal(-1)
        if rel not in (7, 9):
            e_send_y(rel)

    def e_last(rel, carry):
        arrived(e3.at[((z + rel) % NZ) * 2 + 1 - y], ey_sem.at[rel])
        return carry

    lax.fori_loop(0, NZ, e_last, 0)
    e2[...] = e3[...].astype(F32).reshape(ALL, HALF).astype(BF16)

    row = lax.broadcasted_iota(jnp.int32, (TOK, TOK), 0)
    column = lax.broadcasted_iota(jnp.int32, (TOK, TOK), 1)
    upper, lower = e2[0:TOK, :], e2[TOK:ALL, :]
    corner = nt(lower, lower)
    s_snd[0:TOK, :] = nt(upper, lower)
    s_snd[TOK:ALL, :] = jnp.where(row >= column, nt(upper, upper), corner)
    s_snd[ALL:, :] = jnp.broadcast_to(
        jnp.sum(jnp.where(row == column, corner, 0.0), axis=0, keepdims=True), (8, TOK)
    )
    remote(s_snd, s_rcv, small_sem.at[4], small_sem.at[5], {"tensor": peer})
    t_snd[...] = nt(gained_ref[...], e2[...]).astype(BF16)
    remote(t_snd, t_rcv, small_sem.at[6], small_sem.at[7], {"tensor": peer})
    arrived(s_rcv, small_sem.at[5])
    block = s_snd[0:TOK, :] + s_rcv[0:TOK, :]
    both = s_snd[TOK:ALL, :] + s_rcv[TOK:ALL, :]
    below = jnp.where(row > column, both, 0.0)
    above = jnp.where(row < column, both, 0.0)
    corner = jnp.broadcast_to(s_snd[ALL : ALL + 1, :] + s_rcv[ALL : ALL + 1, :], (TOK, TOK))
    s_all[0:TOK, 0:TOK] = jnp.where(row >= column, both, 0.0) + jnp.transpose(below)
    s_all[0:TOK, TOK:ALL] = block
    s_all[TOK:ALL, 0:TOK] = jnp.transpose(block)
    s_all[TOK:ALL, TOK:ALL] = above + jnp.transpose(above) + jnp.where(row == column, corner, 0.0)
    row = lax.broadcasted_iota(jnp.int32, (ALL, ALL), 0)
    column = lax.broadcasted_iota(jnp.int32, (ALL, ALL), 1)
    raw = s_all[...]
    diagonal = jnp.where(row == column, raw, 0.0)
    inverse_row = lax.rsqrt(jnp.sum(diagonal, axis=0, keepdims=True) + epsilon)
    inverse_column = lax.rsqrt(jnp.sum(diagonal, axis=1, keepdims=True) + epsilon)
    scores = raw * inverse_column * inverse_row / logit_divisor
    exps = jnp.where(mask_ref[...] > 0.0, jnp.exp(scores), 0.0)
    total_row = jnp.log(jnp.sum(exps, axis=0, keepdims=True))
    own_rows = pl.ds(pl.multiple_of(dp * ROWS, ROWS), ROWS)
    own_raw = s_all[own_rows, :]
    own_mask = mask_ref[own_rows, :]
    own_row = lax.broadcasted_iota(jnp.int32, (ROWS, ALL), 0) + dp * ROWS
    own_column = lax.broadcasted_iota(jnp.int32, (ROWS, ALL), 1)
    inverse = lax.rsqrt(
        jnp.sum(jnp.where(own_row == own_column, own_raw, 0.0), axis=1, keepdims=True) + epsilon
    )
    own_scores = own_raw * inverse * inverse_row / logit_divisor
    mated = own_column == own_row + 1 - 2 * (own_row % 2)
    allowed = own_mask > 0.0
    total = jnp.log(jnp.sum(jnp.where(allowed, jnp.exp(own_scores), 0.0), axis=1, keepdims=True))
    positive = jnp.sum(jnp.where(mated, own_scores, 0.0), axis=1, keepdims=True)
    loss = jnp.broadcast_to(total - positive, (ROWS, TOK))
    loss_ref[...] = jnp.transpose(loss)[0:1, :]
    both = jnp.where(allowed, jnp.exp(own_scores - total) + jnp.exp(own_scores - total_row), 0.0)
    weights = loss_scale * (both - jnp.where(mated, 2.0, 0.0))
    rounded = (weights * inverse_row).astype(BF16)
    grad_emb = nn(rounded, e2[...]) / logit_divisor
    rounded = rounded.astype(F32) / logit_divisor
    unit = pooled_ref[...] * inverse
    along = inverse * jnp.sum(rounded * own_raw, axis=1, keepdims=True)
    factors = rounded - jnp.where(own_row == own_column, along * inverse, 0.0)
    arrived(t_rcv, small_sem.at[7])
    meets = t_snd[...].astype(F32) + t_rcv[...].astype(F32)
    inverse_tokens = per_token(jnp.broadcast_to(inverse, (ROWS, TOK)))[:, 0:1]
    inner = inverse_tokens * jnp.sum(per_token(factors) * meets, axis=1, keepdims=True) * (1.0 / SEQ)
    spread = per_token(inverse * (grad_emb - unit * along) * gain_ref[...] * (1.0 / SEQ))
    pull = inner * token_inv * token_inv * (1.0 / WIDTH)
    go[...] = (token_inv * (spread - acc[...] * pull)).astype(BF16)

    gl_snd[...] = adapter_scale * nt(ups[picked], go[...])
    remote(gl_snd, gl_rcv, small_sem.at[8], small_sem.at[9], {"tensor": peer})

    owner = z < OWNERS

    def far_first(number):
        away = 8 - (number + 1) // 2
        return (number % 2) * away + (1 - number % 2) * (NZ - away)

    def scatter(buffer, values, kind):
        for number in range(OWNERS):
            buffer[number] = values[:, number * 128 : (number + 1) * 128].astype(BF16)

        @pl.when((y == kind) & owner)
        def _():
            rs_rcv[dp] = buffer[jnp.minimum(z, OWNERS - 1)]

        def one(number, carry):
            zz = (z + far_first(number)) % NZ
            there = zz * 2 + kind

            @pl.when((zz < OWNERS) & (there != dp))
            def _():
                remote(
                    buffer.at[zz], rs_rcv.at[dp], rs_sem.at[kind], rs_sem.at[2], {"dp": there}
                )

            return carry

        lax.fori_loop(0, NZ, one, 0)

    scatter(rs_up, adapter_scale * nn(lowt[...], go[...]), 0)

    def part_step(j, carry):
        rows = pl.ds(pl.multiple_of(peer * HALF + j * TILE, TILE), TILE)
        part_snd[j] = nt(go[...], wbuf[rows, :]).astype(BF16)
        remote(part_snd.at[j], part_rcv.at[j], part_sem.at[TILES], part_sem.at[j], {"tensor": peer})
        return carry

    arrived(gl_rcv, small_sem.at[9])
    glt[...] = (gl_snd[...] + gl_rcv[...]).astype(BF16)
    scatter(rs_down, nn(glt[...], x_own[...]), 1)

    lax.fori_loop(0, TILES, part_step, 0)

    def own_step(j, carry):
        rows = pl.ds(pl.multiple_of(tensor * HALF + j * TILE, TILE), TILE)
        at = pl.ds(pl.multiple_of(j * TILE, TILE), TILE)
        own_part[j] = nt(go[...], wbuf[rows, :]) + tn(glt[...], downs[picked, :, at])
        return carry

    lax.fori_loop(0, TILES, own_step, 0)

    @pl.when(owner)
    def _():
        arrived(rs_rcv.at[pl.ds(0, 31)], rs_sem.at[2])
        mine = ag.at[y * OWNERS + jnp.minimum(z, OWNERS - 1)]
        mine[...] = jnp.sum(rs_rcv[...].astype(F32), axis=0).astype(BF16)

        def one(number, carry):
            off = far_first(number)
            remote(
                mine, mine, ag_sem.at[0], agz_sem.at[NZ - off], {"dp": ((z + off) % NZ) * 2 + y}
            )
            return carry

        remote(mine, mine, ag_sem.at[1], ag_sem.at[2], {"dp": dp_y})
        lax.fori_loop(0, NZ - 1, one, 0)

    def gin_step(j, carry):
        at = pl.ds(pl.multiple_of(j * TILE, TILE), TILE)
        arrived(part_rcv.at[j], part_sem.at[j])
        gin_snd[j] = (own_part[j] + part_rcv[j].astype(F32)).astype(BF16)
        remote(gin_snd.at[j], gin_ref.at[:, at], gin_sem.at[TILES], gin_sem.at[j], {"pipe": before})
        return carry

    lax.fori_loop(0, TILES, gin_step, 0)

    def ag_step(number, carry):
        rel = far_first(NZ - 2 - number)
        zz = (z + rel) % NZ

        @pl.when(zz < OWNERS)
        def _():
            part = ag.at[y * OWNERS + zz]
            arrived(part, agz_sem.at[rel])
            remote(part, part, ag_sem.at[1], ag_sem.at[2], {"dp": dp_y})

        return carry

    lax.fori_loop(0, NZ - 1, ag_step, 0)
    arrived(ag.at[pl.ds((1 - y) * OWNERS, OWNERS)], ag_sem.at[2])

    for number in range(OWNERS):
        at = slice(number * 128, (number + 1) * 128)
        gup_ref[:, at] = ag[number].astype(F32)
        gdown_ref[:, at] = ag[OWNERS + number].astype(F32)

    for number, rows in enumerate((7 * SHARD + 64, 7 * SHARD + 48, NZ * 16, NZ * 48, NZ * 48, 2 * NZ * SHARD)):
        arrived(wbuf.at[pl.ds(0, rows), pl.ds(0, CORE)], w_send.at[number])

    @pl.when(x % 2 == 1)
    def _():
        arrived(wbuf.at[pl.ds(0, SHARD), pl.ds(0, CORE)], w_send.at[6])

    arrived(x3.at[pl.ds(0, 8)], x_sem.at[0])
    arrived(x3.at[pl.ds(0, 8)], x_sem.at[3])
    arrived(low_snd, small_sem.at[0])
    arrived(tok_snd, small_sem.at[2])
    arrived(e3.at[pl.ds(0, 17)], e_send.at[0])
    arrived(e3.at[pl.ds(0, 14)], e_send.at[1])
    arrived(s_snd, small_sem.at[4])
    arrived(t_snd, small_sem.at[6])
    arrived(gl_snd, small_sem.at[8])
    arrived(part_snd, part_sem.at[TILES])
    arrived(gin_snd, gin_sem.at[TILES])
    for kind in range(2):

        @pl.when((y == kind) & owner)
        def _():
            arrived(rs_up.at[pl.ds(0, OWNERS - 1)], rs_sem.at[kind])

        @pl.when((y != kind) | (z >= OWNERS))
        def _():
            arrived(rs_up, rs_sem.at[kind])

    @pl.when(owner)
    def _():
        arrived(rs_rcv.at[pl.ds(0, NZ - 1)], ag_sem.at[0])

    arrived(rs_up, ag_sem.at[1])

    def gin_last(j, carry):
        at = pl.ds(pl.multiple_of(j * TILE, TILE), TILE)
        arrived(gin_ref.at[:, at], gin_sem.at[j])
        return carry

    lax.fori_loop(0, TILES, gin_last, 0)


def put_out(gin, gup, gdown, loss, gin_hbm, gup_hbm, gdown_hbm, loss_hbm, sems):
    copies = [
        pltpu.make_async_copy(src, dst, sems.at[number])
        for number, (src, dst) in enumerate(
            ((gin, gin_hbm), (gup, gup_hbm), (gdown, gdown_hbm), (loss, loss_hbm))
        )
    ]
    for copy in copies:
        copy.start()
    for copy in copies:
        copy.wait()


def body(hidden, frozen_weight, final_norm_gain, down_maps, up_maps, tenant, adapter):
    vmem = pl.BlockSpec(memory_space=pltpu.VMEM)
    anywhere = pl.BlockSpec(memory_space=pl.ANY)
    dma = pltpu.SemaphoreType.DMA
    gin, gup, gdown, loss = pl.pallas_call(
        kernel,
        name="whole_step",
        out_shape=(
            pltpu.VMEM((TOK, HALF), BF16),
            pltpu.VMEM((RANK, HALF), F32),
            pltpu.VMEM((RANK, HALF), F32),
            pltpu.VMEM((1, ROWS), F32),
        ),
        in_specs=[
            anywhere,
            anywhere,
            anywhere,
            anywhere,
            anywhere,
            vmem,
            pl.BlockSpec(memory_space=pltpu.SMEM),
        ],
        out_specs=(anywhere, vmem, vmem, vmem),
        scratch_shapes=[
            pltpu.VMEM((1, HALF), F32),
            pltpu.VMEM((WIDTH, HALF), BF16),
            pltpu.VMEM((TOK, HALF), F32),
            pltpu.VMEM((TOK, HALF), BF16),
            pltpu.VMEM((NZ, TOK, PLANE), BF16),
            pltpu.VMEM((2, 4, TOK, PLANE), BF16),
            pltpu.VMEM((8, RANK, HALF), BF16),
            pltpu.VMEM((8, RANK, HALF), BF16),
            pltpu.VMEM((RANK, TOK), F32),
            pltpu.VMEM((RANK, TOK), F32),
            pltpu.VMEM((RANK, TOK), BF16),
            pltpu.VMEM((8, TOK), F32),
            pltpu.VMEM((8, TOK), F32),
            pltpu.VMEM((ROWS, HALF), F32),
            pltpu.VMEM((32, ROWS, HALF), BF16),
            pltpu.VMEM((ALL, HALF), BF16),
            pltpu.VMEM((ALL + 8, TOK), F32),
            pltpu.VMEM((ALL + 8, TOK), F32),
            pltpu.VMEM((ALL, ALL), F32),
            pltpu.VMEM((ALL, ALL), F32),
            pltpu.VMEM((TOK, HALF), BF16),
            pltpu.VMEM((TOK, ALL), BF16),
            pltpu.VMEM((TOK, ALL), BF16),
            pltpu.VMEM((TOK, HALF), BF16),
            pltpu.VMEM((RANK, TOK), F32),
            pltpu.VMEM((RANK, TOK), F32),
            pltpu.VMEM((RANK, TOK), BF16),
            pltpu.VMEM((TILES, TOK, TILE), BF16),
            pltpu.VMEM((TILES, TOK, TILE), BF16),
            pltpu.VMEM((TILES, TOK, TILE), F32),
            pltpu.VMEM((TILES, TOK, TILE), BF16),
            pltpu.VMEM((OWNERS, RANK, 128), BF16),
            pltpu.VMEM((OWNERS, RANK, 128), BF16),
            pltpu.VMEM((32, RANK, 128), BF16),
            pltpu.VMEM((2 * OWNERS, RANK, 128), BF16),
            dma((4,)),
            dma((NZ, 3)),
            dma((NZ,)),
            dma((2, NZ)),
            dma((7,)),
            dma((6,)),
            dma((10,)),
            dma((NZ,)),
            dma((NZ,)),
            dma((2,)),
            dma((TILES + 1,)),
            dma((TILES + 1,)),
            dma((3,)),
            dma((3,)),
            dma((NZ,)),
        ],
        compiler_params=pltpu.CompilerParams(
            collective_id=0, has_side_effects=True, vmem_limit_bytes=56 * 1024 * 1024
        ),
    )(hidden[0], frozen_weight, final_norm_gain, down_maps, up_maps, tenant, adapter)
    gin, gup, gdown, loss = pl.pallas_call(
        put_out,
        name="put_out",
        out_shape=(
            jax.ShapeDtypeStruct((TOK, HALF), BF16),
            jax.ShapeDtypeStruct((RANK, HALF), F32),
            jax.ShapeDtypeStruct((RANK, HALF), F32),
            jax.ShapeDtypeStruct((1, ROWS), F32),
        ),
        in_specs=[vmem] * 4,
        out_specs=(anywhere,) * 4,
        scratch_shapes=[dma((4,))],
        compiler_params=pltpu.CompilerParams(vmem_limit_bytes=4 * 1024 * 1024),
    )(gin, gup, gdown, loss)
    return gin[None], gup[None], gdown[None], loss


def solution(mesh):
    return jax.shard_map(
        body,
        mesh=mesh,
        in_specs=(
            P("pipe", "dp", "tensor"),
            P("dp", "tensor"),
            P("tensor"),
            P(None, None, "tensor"),
            P(None, None, "tensor"),
            P("pipe", None),
            P("pipe"),
        ),
        out_specs=(
            P("pipe", "dp", "tensor"),
            P("pipe", None, "tensor"),
            P("pipe", None, "tensor"),
            P("pipe", "dp"),
        ),
        check_vma=False,
    )
```

```python
import jax
import jax.numpy as jnp
from jax import lax
from jax.experimental import pallas as pl
from jax.experimental.pallas import tpu as pltpu
from jax.sharding import PartitionSpec as P

MESH = pl.DeviceIdType.MESH
F32, BF16 = jnp.float32, jnp.bfloat16

WIDTH = 3584
HALF = 1792
CORE = 896
SHARD = 112
PLANE = 224
CUT_A, CUT_B = 48, 96
NZ = 16
SEQ = 16
ROWS = 8
ALL = 256
TOK = 128
RANK = 32
OWNERS = 14
TILE = 256
TILES = 7
LAG = 4

logit_divisor = 0.05
loss_scale = 256.0
adapter_scale = 0.5
epsilon = 1e-06


def nt(a, b):
    return lax.dot_general(a, b, (((1,), (1,)), ((), ())), preferred_element_type=F32)


def tn(a, b):
    return lax.dot_general(a, b, (((0,), (0,)), ((), ())), preferred_element_type=F32)


def nn(a, b):
    return jnp.dot(a, b, preferred_element_type=F32)


def per_token(rows):
    width = rows.shape[1]
    return jnp.broadcast_to(rows[:, None, :], (ROWS, SEQ, width)).reshape(TOK, width)


def as_lanes(columns):
    lane = lax.broadcasted_iota(jnp.int32, (TOK, TOK), 1)
    packed = jnp.zeros((TOK, TOK), F32)
    for number, column in enumerate(columns):
        packed = jnp.where(lane == number, jnp.broadcast_to(column, (TOK, TOK)), packed)
    return jnp.transpose(packed)[0:8, :]


def as_columns(lanes):
    return jnp.transpose(lanes)


def kernel(
    x_hbm,
    w_hbm,
    gain_hbm,
    down_hbm,
    up_hbm,
    tenant_ref,
    adapter_ref,
    gin_ref,
    gup_ref,
    gdown_ref,
    loss_ref,
    gain_ref,
    wbuf,
    acc,
    x_own,
    x3,
    x_pass,
    downs,
    ups,
    low_snd,
    low_rcv,
    lowt,
    tok_snd,
    tok_rcv,
    pooled_ref,
    e3,
    e2,
    s_snd,
    s_rcv,
    s_all,
    mask_ref,
    gained_ref,
    t_snd,
    t_rcv,
    go,
    gl_snd,
    gl_rcv,
    glt,
    part_snd,
    part_rcv,
    own_part,
    gin_snd,
    rs_up,
    rs_down,
    rs_rcv,
    ag,
    in_sem,
    z_sem,
    xy_sem,
    d2d_sem,
    w_send,
    x_sem,
    small_sem,
    ez_sem,
    ey_sem,
    e_send,
    part_sem,
    gin_sem,
    rs_sem,
    ag_sem,
    agz_sem,
):
    dp = lax.axis_index("dp")
    pipe = lax.axis_index("pipe")
    tensor = lax.axis_index("tensor")
    z = dp // 2
    y = dp % 2
    x = pipe // 2
    core = pipe % 2
    own_q = (x + y) % 2
    dp_right = (dp + 2) % 32
    dp_left = (dp + 30) % 32
    dp_y = dp + 1 - 2 * y
    x_right = (pipe + 2) % 8
    x_left = (pipe + 6) % 8
    partner = pipe + 1 - 2 * core
    peer = 1 - tensor
    plus = {"dp": dp_y, "tensor": (tensor + y) % 2}
    minus = {"dp": dp_y, "tensor": (tensor + 1 - y) % 2}
    before = (pipe + 7) % 8
    after = (pipe + 1) % 8

    def fetch(src, dst, number):
        return pltpu.make_async_copy(src, dst, in_sem.at[number])

    x_copy = fetch(x_hbm, x_own, 0)
    down_copy = fetch(down_hbm, downs, 1)
    up_copy = fetch(up_hbm, ups, 2)
    x_copy.start()
    down_copy.start()
    up_copy.start()
    gain_copy = fetch(gain_hbm, gain_ref.at[0], 3)
    gain_copy.start()

    barrier = pltpu.get_barrier_semaphore()
    for where in (
        {"dp": dp_right},
        {"dp": dp_left},
        {"dp": dp_y},
        {"pipe": x_right},
        {"pipe": x_left},
        {"pipe": before},
        {"pipe": after},
        {"tensor": peer},
        {"dp": dp_y, "tensor": peer},
    ):
        pl.semaphore_signal(barrier, inc=1, device_id=where, device_id_type=MESH)
    pl.semaphore_wait(barrier, 9)

    def remote(src, dst, send, recv, where):
        copy = pltpu.make_async_remote_copy(
            src_ref=src, dst_ref=dst, send_sem=send, recv_sem=recv, device_id=where, device_id_type=MESH
        )
        copy.start()

    def arrived(ref, sem):
        pltpu.make_async_copy(ref, ref, sem).wait()

    columns = pl.ds(pl.multiple_of(core * CORE, 128), CORE)

    def piece(zz, q, first, count):
        return wbuf.at[pl.ds(pl.multiple_of((zz * 2 + q) * SHARD + first, 16), count), columns]

    chunks = ((CUT_B, SHARD - CUT_B), (0, CUT_A), (CUT_A, CUT_B - CUT_A))

    @pl.when(x % 2 == 0)
    def _():
        for number, (first, count) in enumerate(chunks):
            pltpu.make_async_copy(
                w_hbm.at[pl.ds(first, count), columns], piece(z, own_q, first, count), z_sem.at[0, number]
            ).start()

    @pl.when(x % 2 == 1)
    def _():
        for number, (first, count) in enumerate(chunks):
            remote(
                w_hbm.at[pl.ds(first, count), columns],
                piece(z, y, first, count),
                w_send.at[6],
                z_sem.at[0, number],
                {"dp": dp_y},
            )

    def got(zz, rel, number):
        first, count = chunks[number]
        arrived(piece(zz, own_q, first, count), z_sem.at[rel, number])

    def forward(zz, rel, number, right):
        first, count = chunks[number]
        part = piece(zz, own_q, first, count)
        there = (rel + 15) % NZ if right else (rel + 1) % NZ
        remote(
            part, part, w_send.at[0 if right else 1], z_sem.at[there, number],
            {"dp": dp_right if right else dp_left},
        )

    def share(zz, rel, number):
        first, count = chunks[number]
        part = piece(zz, own_q, first, count)
        where = ({"dp": dp_y}, {"pipe": x_right}, {"pipe": x_left})[number]
        remote(part, part, w_send.at[2 + number], xy_sem.at[rel], where)
        if number == 2:
            part = piece(zz, own_q, 0, SHARD)
            remote(part, part, w_send.at[5], d2d_sem.at[0, rel], {"pipe": partner})

    def complement(zz, rel):
        part = piece(zz, 1 - own_q, 0, SHARD)
        arrived(part, xy_sem.at[rel])
        remote(part, part, w_send.at[5], d2d_sem.at[1, rel], {"pipe": partner})

    other = pl.ds(pl.multiple_of((1 - core) * CORE, 128), CORE)

    def compute(zz, rel):
        for number in range(2):
            q = own_q if number == 0 else 1 - own_q
            rows = pl.ds(pl.multiple_of((zz * 2 + q) * SHARD, 16), SHARD)
            arrived(wbuf.at[rows, other], d2d_sem.at[number, rel])
        lhs = x3[zz]
        rows = pl.ds(pl.multiple_of(zz * PLANE, 16), PLANE)
        for n in range(TILES):
            at = slice(n * TILE, (n + 1) * TILE)
            acc[:, at] += nn(lhs, wbuf[rows, at])

    def right_z(k):
        return (z + NZ - k) % NZ

    def left_z(k):
        return (z + k) % NZ

    def prepare():
        x_copy.wait()
        down_copy.wait()
        up_copy.wait()
        gain_copy.wait()
        for number in range(8):
            x3[tensor * 8 + number] = x_own[:, number * PLANE : (number + 1) * PLANE]
        remote(x3.at[pl.ds(tensor * 8, 4)], x_pass.at[0], x_sem.at[0], x_sem.at[1], plus)
        remote(x3.at[pl.ds(tensor * 8 + 4, 4)], x_pass.at[1], x_sem.at[0], x_sem.at[2], minus)
        picked = adapter_ref[0]
        low_snd[...] = nt(downs[picked], x_own[...])
        remote(low_snd, low_rcv, small_sem.at[0], small_sem.at[1], {"tensor": peer})
        tenants = jnp.broadcast_to(tenant_ref[...], (ALL, ALL)).astype(F32)
        own = jnp.transpose(tenants)
        row = lax.broadcasted_iota(jnp.int32, (ALL, ALL), 0)
        column = lax.broadcasted_iota(jnp.int32, (ALL, ALL), 1)
        mask_ref[...] = jnp.where((tenants == own) & (row != column), 1.0, 0.0)

    def pass_on():
        arrived(x_pass.at[0], x_sem.at[1])
        half = (tensor + 1 - y) % 2
        remote(x_pass.at[0], x3.at[pl.ds(half * 8, 4)], x_sem.at[3], x_sem.at[4], plus)
        arrived(x_pass.at[1], x_sem.at[2])
        half = (tensor + y) % 2
        remote(x_pass.at[1], x3.at[pl.ds(half * 8 + 4, 4)], x_sem.at[3], x_sem.at[5], minus)

    def first_terms():
        arrived(x3.at[pl.ds(peer * 8, 4)], x_sem.at[4])
        arrived(x3.at[pl.ds(peer * 8 + 4, 4)], x_sem.at[5])
        arrived(low_rcv, small_sem.at[1])
        picked = adapter_ref[0]
        lowt[...] = (low_snd[...] + low_rcv[...]).astype(BF16)
        for n in range(TILES):
            at = slice(n * TILE, (n + 1) * TILE)
            acc[:, at] = adapter_scale * tn(lowt[...], ups[picked, :, at])

    def step(k, carry):
        rel = (NZ - k) % NZ
        zr = right_z(k)
        zl = left_z(k)

        for number in range(3):

            @pl.when(k <= 8)
            def _():
                got(zr, rel, number)

            @pl.when(k <= (7 if number < 2 else 6))
            def _():
                forward(zr, rel, number, True)

            @pl.when(k == 0)
            def _():
                forward(z, 0, number, False)

            @pl.when((k >= 1) & (k <= 7))
            def _():
                got(zl, k, number)

            @pl.when((k >= 1) & (k <= (6 if number < 2 else 7)))
            def _():
                forward(zl, k, number, False)

            @pl.when(k <= 8)
            def _():
                share(zr, rel, number)

            @pl.when((k >= 1) & (k <= 7))
            def _():
                share(zl, k, number)

        @pl.when(k == 0)
        def _():
            prepare()

        @pl.when(k == 2)
        def _():
            pass_on()

        @pl.when(k == LAG)
        def _():
            first_terms()

        @pl.when(k >= LAG)
        def _():
            compute(right_z(k - LAG), (NZ + LAG - k) % NZ)

        @pl.when((k >= LAG + 1) & (k <= LAG + 7))
        def _():
            compute(left_z(k - LAG), k - LAG)

        @pl.when((k >= 2) & (k <= 10))
        def _():
            complement(right_z(k - 2), (NZ + 2 - k) % NZ)

        @pl.when((k >= 3) & (k <= 9))
        def _():
            complement(left_z(k - 2), k - 2)

        return carry

    lax.fori_loop(0, LAG + 9, step, 0)

    picked = adapter_ref[0]

    out = acc[...]
    tok_snd[...] = as_lanes((jnp.sum(out * out, axis=1, keepdims=True),))
    remote(tok_snd, tok_rcv, small_sem.at[2], small_sem.at[3], {"tensor": peer})
    arrived(tok_rcv, small_sem.at[3])
    squares = as_columns(tok_snd[...] + tok_rcv[...])[:, 0:1]
    token_inv = lax.rsqrt(squares / WIDTH + epsilon)
    gained = acc[...] * gain_ref[...]
    pooled = jnp.sum((gained * token_inv).reshape(ROWS, SEQ, HALF), axis=1) * (1.0 / SEQ)
    pooled_ref[...] = pooled
    e3[dp] = pooled.astype(BF16)

    def row_of(rel, yy):
        return e3.at[((z + rel) % NZ) * 2 + yy]

    def e_send_z(rel, hops, half=None):
        part = row_of(rel, y)
        if half is not None:
            part = part.at[:, pl.ds(half * CORE, CORE)]
        remote(
            part, part, e_send.at[0], ez_sem.at[(rel - hops) % NZ], {"dp": (dp + 32 + 2 * hops) % 32}
        )

    def e_send_y(rel):
        part = row_of(rel, y)
        remote(part, part, e_send.at[1], ey_sem.at[rel], {"dp": dp_y})

    def e_send_diagonal(hops):
        part = row_of(8, y)
        remote(
            part, part, e_send.at[0], ey_sem.at[8 - hops], {"dp": (dp_y + 32 + 2 * hops) % 32}
        )

    for hops in (4, -4, 1, -1, 2, -2):
        e_send_z(0, hops)
    e_send_y(0)
    gained_ref[...] = (acc[...] * gain_ref[...]).astype(BF16)
    for rel in (15, 1, 14, 2, 12, 4, 11, 3, 13, 5, 10, 6, 8, 7, 9):
        arrived(row_of(rel, y), ez_sem.at[rel])
        if rel == 12:
            e_send_z(12, 4, 0)
        if rel == 4:
            e_send_z(4, -4, 1)
        if rel % 4 == 0:
            e_send_z(rel, 1)
            e_send_z(rel, -1)
        if rel == 12:
            e_send_z(12, 2)
        if rel == 4:
            e_send_z(4, -2)
        if rel == 8:
            e_send_diagonal(1)
            e_send_diagonal(-1)
        if rel not in (7, 9):
            e_send_y(rel)

    def e_last(rel, carry):
        arrived(e3.at[((z + rel) % NZ) * 2 + 1 - y], ey_sem.at[rel])
        return carry

    lax.fori_loop(0, NZ, e_last, 0)
    e2[...] = e3[...].astype(F32).reshape(ALL, HALF).astype(BF16)

    row = lax.broadcasted_iota(jnp.int32, (TOK, TOK), 0)
    column = lax.broadcasted_iota(jnp.int32, (TOK, TOK), 1)
    upper, lower = e2[0:TOK, :], e2[TOK:ALL, :]
    corner = nt(lower, lower)
    s_snd[0:TOK, :] = nt(upper, lower)
    s_snd[TOK:ALL, :] = jnp.where(row >= column, nt(upper, upper), corner)
    s_snd[ALL:, :] = jnp.broadcast_to(
        jnp.sum(jnp.where(row == column, corner, 0.0), axis=0, keepdims=True), (8, TOK)
    )
    remote(s_snd, s_rcv, small_sem.at[4], small_sem.at[5], {"tensor": peer})
    t_snd[...] = nt(gained_ref[...], e2[...]).astype(BF16)
    remote(t_snd, t_rcv, small_sem.at[6], small_sem.at[7], {"tensor": peer})
    arrived(s_rcv, small_sem.at[5])
    block = s_snd[0:TOK, :] + s_rcv[0:TOK, :]
    both = s_snd[TOK:ALL, :] + s_rcv[TOK:ALL, :]
    below = jnp.where(row > column, both, 0.0)
    above = jnp.where(row < column, both, 0.0)
    corner = jnp.broadcast_to(s_snd[ALL : ALL + 1, :] + s_rcv[ALL : ALL + 1, :], (TOK, TOK))
    s_all[0:TOK, 0:TOK] = jnp.where(row >= column, both, 0.0) + jnp.transpose(below)
    s_all[0:TOK, TOK:ALL] = block
    s_all[TOK:ALL, 0:TOK] = jnp.transpose(block)
    s_all[TOK:ALL, TOK:ALL] = above + jnp.transpose(above) + jnp.where(row == column, corner, 0.0)
    row = lax.broadcasted_iota(jnp.int32, (ALL, ALL), 0)
    column = lax.broadcasted_iota(jnp.int32, (ALL, ALL), 1)
    raw = s_all[...]
    diagonal = jnp.where(row == column, raw, 0.0)
    inverse_row = lax.rsqrt(jnp.sum(diagonal, axis=0, keepdims=True) + epsilon)
    inverse_column = lax.rsqrt(jnp.sum(diagonal, axis=1, keepdims=True) + epsilon)
    scores = raw * inverse_column * inverse_row / logit_divisor
    exps = jnp.where(mask_ref[...] > 0.0, jnp.exp(scores), 0.0)
    total_row = jnp.log(jnp.sum(exps, axis=0, keepdims=True))
    own_rows = pl.ds(pl.multiple_of(dp * ROWS, ROWS), ROWS)
    own_raw = s_all[own_rows, :]
    own_mask = mask_ref[own_rows, :]
    own_row = lax.broadcasted_iota(jnp.int32, (ROWS, ALL), 0) + dp * ROWS
    own_column = lax.broadcasted_iota(jnp.int32, (ROWS, ALL), 1)
    inverse = lax.rsqrt(
        jnp.sum(jnp.where(own_row == own_column, own_raw, 0.0), axis=1, keepdims=True) + epsilon
    )
    own_scores = own_raw * inverse * inverse_row / logit_divisor
    mated = own_column == own_row + 1 - 2 * (own_row % 2)
    allowed = own_mask > 0.0
    total = jnp.log(jnp.sum(jnp.where(allowed, jnp.exp(own_scores), 0.0), axis=1, keepdims=True))
    positive = jnp.sum(jnp.where(mated, own_scores, 0.0), axis=1, keepdims=True)
    loss = jnp.broadcast_to(total - positive, (ROWS, TOK))
    loss_ref[...] = jnp.transpose(loss)[0:1, :]
    both = jnp.where(allowed, jnp.exp(own_scores - total) + jnp.exp(own_scores - total_row), 0.0)
    weights = loss_scale * (both - jnp.where(mated, 2.0, 0.0))
    rounded = (weights * inverse_row).astype(BF16)
    grad_emb = nn(rounded, e2[...]) / logit_divisor
    rounded = rounded.astype(F32) / logit_divisor
    unit = pooled_ref[...] * inverse
    along = inverse * jnp.sum(rounded * own_raw, axis=1, keepdims=True)
    factors = rounded - jnp.where(own_row == own_column, along * inverse, 0.0)
    arrived(t_rcv, small_sem.at[7])
    meets = t_snd[...].astype(F32) + t_rcv[...].astype(F32)
    inverse_tokens = per_token(jnp.broadcast_to(inverse, (ROWS, TOK)))[:, 0:1]
    inner = inverse_tokens * jnp.sum(per_token(factors) * meets, axis=1, keepdims=True) * (1.0 / SEQ)
    spread = per_token(inverse * (grad_emb - unit * along) * gain_ref[...] * (1.0 / SEQ))
    pull = inner * token_inv * token_inv * (1.0 / WIDTH)
    go[...] = (token_inv * (spread - acc[...] * pull)).astype(BF16)

    gl_snd[...] = adapter_scale * nt(ups[picked], go[...])
    remote(gl_snd, gl_rcv, small_sem.at[8], small_sem.at[9], {"tensor": peer})

    owner = z < OWNERS

    def far_first(number):
        away = 8 - (number + 1) // 2
        return (number % 2) * away + (1 - number % 2) * (NZ - away)

    def scatter(buffer, values, kind):
        for number in range(OWNERS):
            buffer[number] = values[:, number * 128 : (number + 1) * 128].astype(BF16)

        @pl.when((y == kind) & owner)
        def _():
            rs_rcv[dp] = buffer[jnp.minimum(z, OWNERS - 1)]

        def one(number, carry):
            zz = (z + far_first(number)) % NZ
            there = zz * 2 + kind

            @pl.when((zz < OWNERS) & (there != dp))
            def _():
                remote(
                    buffer.at[zz], rs_rcv.at[dp], rs_sem.at[kind], rs_sem.at[2], {"dp": there}
                )

            return carry

        lax.fori_loop(0, NZ, one, 0)

    scatter(rs_up, adapter_scale * nn(lowt[...], go[...]), 0)

    def part_step(j, carry):
        rows = pl.ds(pl.multiple_of(peer * HALF + j * TILE, TILE), TILE)
        part_snd[j] = nt(go[...], wbuf[rows, :]).astype(BF16)
        remote(part_snd.at[j], part_rcv.at[j], part_sem.at[TILES], part_sem.at[j], {"tensor": peer})
        return carry

    arrived(gl_rcv, small_sem.at[9])
    glt[...] = (gl_snd[...] + gl_rcv[...]).astype(BF16)
    scatter(rs_down, nn(glt[...], x_own[...]), 1)

    lax.fori_loop(0, TILES, part_step, 0)

    def own_step(j, carry):
        rows = pl.ds(pl.multiple_of(tensor * HALF + j * TILE, TILE), TILE)
        at = pl.ds(pl.multiple_of(j * TILE, TILE), TILE)
        own_part[j] = nt(go[...], wbuf[rows, :]) + tn(glt[...], downs[picked, :, at])
        return carry

    lax.fori_loop(0, TILES, own_step, 0)

    @pl.when(owner)
    def _():
        arrived(rs_rcv.at[pl.ds(0, 31)], rs_sem.at[2])
        mine = ag.at[y * OWNERS + jnp.minimum(z, OWNERS - 1)]
        mine[...] = jnp.sum(rs_rcv[...].astype(F32), axis=0).astype(BF16)

        def one(number, carry):
            off = far_first(number)
            remote(
                mine, mine, ag_sem.at[0], agz_sem.at[NZ - off], {"dp": ((z + off) % NZ) * 2 + y}
            )
            return carry

        remote(mine, mine, ag_sem.at[1], ag_sem.at[2], {"dp": dp_y})
        lax.fori_loop(0, NZ - 1, one, 0)

    def gin_step(j, carry):
        at = pl.ds(pl.multiple_of(j * TILE, TILE), TILE)
        arrived(part_rcv.at[j], part_sem.at[j])
        gin_snd[j] = (own_part[j] + part_rcv[j].astype(F32)).astype(BF16)
        remote(gin_snd.at[j], gin_ref.at[:, at], gin_sem.at[TILES], gin_sem.at[j], {"pipe": before})
        return carry

    lax.fori_loop(0, TILES, gin_step, 0)

    def ag_step(number, carry):
        rel = far_first(NZ - 2 - number)
        zz = (z + rel) % NZ

        @pl.when(zz < OWNERS)
        def _():
            part = ag.at[y * OWNERS + zz]
            arrived(part, agz_sem.at[rel])
            remote(part, part, ag_sem.at[1], ag_sem.at[2], {"dp": dp_y})

        return carry

    lax.fori_loop(0, NZ - 1, ag_step, 0)
    arrived(ag.at[pl.ds((1 - y) * OWNERS, OWNERS)], ag_sem.at[2])

    for number in range(OWNERS):
        at = slice(number * 128, (number + 1) * 128)
        gup_ref[:, at] = ag[number].astype(F32)
        gdown_ref[:, at] = ag[OWNERS + number].astype(F32)

    for number, rows in enumerate((7 * SHARD + 64, 7 * SHARD + 48, NZ * 16, NZ * 48, NZ * 48, 2 * NZ * SHARD)):
        arrived(wbuf.at[pl.ds(0, rows), pl.ds(0, CORE)], w_send.at[number])

    @pl.when(x % 2 == 1)
    def _():
        arrived(wbuf.at[pl.ds(0, SHARD), pl.ds(0, CORE)], w_send.at[6])

    arrived(x3.at[pl.ds(0, 8)], x_sem.at[0])
    arrived(x3.at[pl.ds(0, 8)], x_sem.at[3])
    arrived(low_snd, small_sem.at[0])
    arrived(tok_snd, small_sem.at[2])
    arrived(e3.at[pl.ds(0, 17)], e_send.at[0])
    arrived(e3.at[pl.ds(0, 14)], e_send.at[1])
    arrived(s_snd, small_sem.at[4])
    arrived(t_snd, small_sem.at[6])
    arrived(gl_snd, small_sem.at[8])
    arrived(part_snd, part_sem.at[TILES])
    arrived(gin_snd, gin_sem.at[TILES])
    for kind in range(2):

        @pl.when((y == kind) & owner)
        def _():
            arrived(rs_up.at[pl.ds(0, OWNERS - 1)], rs_sem.at[kind])

        @pl.when((y != kind) | (z >= OWNERS))
        def _():
            arrived(rs_up, rs_sem.at[kind])

    @pl.when(owner)
    def _():
        arrived(rs_rcv.at[pl.ds(0, NZ - 1)], ag_sem.at[0])

    arrived(rs_up, ag_sem.at[1])

    def gin_last(j, carry):
        at = pl.ds(pl.multiple_of(j * TILE, TILE), TILE)
        arrived(gin_ref.at[:, at], gin_sem.at[j])
        return carry

    lax.fori_loop(0, TILES, gin_last, 0)


def put_out(gin, gup, gdown, loss, gin_hbm, gup_hbm, gdown_hbm, loss_hbm, sems):
    copies = [
        pltpu.make_async_copy(src, dst, sems.at[number])
        for number, (src, dst) in enumerate(
            ((gin, gin_hbm), (gup, gup_hbm), (gdown, gdown_hbm), (loss, loss_hbm))
        )
    ]
    for copy in copies:
        copy.start()
    for copy in copies:
        copy.wait()


def body(hidden, frozen_weight, final_norm_gain, down_maps, up_maps, tenant, adapter):
    vmem = pl.BlockSpec(memory_space=pltpu.VMEM)
    anywhere = pl.BlockSpec(memory_space=pl.ANY)
    dma = pltpu.SemaphoreType.DMA
    gin, gup, gdown, loss = pl.pallas_call(
        kernel,
        name="whole_step",
        out_shape=(
            pltpu.VMEM((TOK, HALF), BF16),
            pltpu.VMEM((RANK, HALF), F32),
            pltpu.VMEM((RANK, HALF), F32),
            pltpu.VMEM((1, ROWS), F32),
        ),
        in_specs=[
            anywhere,
            anywhere,
            anywhere,
            anywhere,
            anywhere,
            vmem,
            pl.BlockSpec(memory_space=pltpu.SMEM),
        ],
        out_specs=(anywhere, vmem, vmem, vmem),
        scratch_shapes=[
            pltpu.VMEM((1, HALF), F32),
            pltpu.VMEM((WIDTH, HALF), BF16),
            pltpu.VMEM((TOK, HALF), F32),
            pltpu.VMEM((TOK, HALF), BF16),
            pltpu.VMEM((NZ, TOK, PLANE), BF16),
            pltpu.VMEM((2, 4, TOK, PLANE), BF16),
            pltpu.VMEM((8, RANK, HALF), BF16),
            pltpu.VMEM((8, RANK, HALF), BF16),
            pltpu.VMEM((RANK, TOK), F32),
            pltpu.VMEM((RANK, TOK), F32),
            pltpu.VMEM((RANK, TOK), BF16),
            pltpu.VMEM((8, TOK), F32),
            pltpu.VMEM((8, TOK), F32),
            pltpu.VMEM((ROWS, HALF), F32),
            pltpu.VMEM((32, ROWS, HALF), BF16),
            pltpu.VMEM((ALL, HALF), BF16),
            pltpu.VMEM((ALL + 8, TOK), F32),
            pltpu.VMEM((ALL + 8, TOK), F32),
            pltpu.VMEM((ALL, ALL), F32),
            pltpu.VMEM((ALL, ALL), F32),
            pltpu.VMEM((TOK, HALF), BF16),
            pltpu.VMEM((TOK, ALL), BF16),
            pltpu.VMEM((TOK, ALL), BF16),
            pltpu.VMEM((TOK, HALF), BF16),
            pltpu.VMEM((RANK, TOK), F32),
            pltpu.VMEM((RANK, TOK), F32),
            pltpu.VMEM((RANK, TOK), BF16),
            pltpu.VMEM((TILES, TOK, TILE), BF16),
            pltpu.VMEM((TILES, TOK, TILE), BF16),
            pltpu.VMEM((TILES, TOK, TILE), F32),
            pltpu.VMEM((TILES, TOK, TILE), BF16),
            pltpu.VMEM((OWNERS, RANK, 128), BF16),
            pltpu.VMEM((OWNERS, RANK, 128), BF16),
            pltpu.VMEM((32, RANK, 128), BF16),
            pltpu.VMEM((2 * OWNERS, RANK, 128), BF16),
            dma((4,)),
            dma((NZ, 3)),
            dma((NZ,)),
            dma((2, NZ)),
            dma((7,)),
            dma((6,)),
            dma((10,)),
            dma((NZ,)),
            dma((NZ,)),
            dma((2,)),
            dma((TILES + 1,)),
            dma((TILES + 1,)),
            dma((3,)),
            dma((3,)),
            dma((NZ,)),
        ],
        compiler_params=pltpu.CompilerParams(
            collective_id=0, has_side_effects=True, vmem_limit_bytes=56 * 1024 * 1024
        ),
    )(hidden[0], frozen_weight, final_norm_gain, down_maps, up_maps, tenant, adapter)
    gin, gup, gdown, loss = pl.pallas_call(
        put_out,
        name="put_out",
        out_shape=(
            jax.ShapeDtypeStruct((TOK, HALF), BF16),
            jax.ShapeDtypeStruct((RANK, HALF), F32),
            jax.ShapeDtypeStruct((RANK, HALF), F32),
            jax.ShapeDtypeStruct((1, ROWS), F32),
        ),
        in_specs=[vmem] * 4,
        out_specs=(anywhere,) * 4,
        scratch_shapes=[dma((4,))],
        compiler_params=pltpu.CompilerParams(vmem_limit_bytes=4 * 1024 * 1024),
    )(gin, gup, gdown, loss)
    return gin[None], gup[None], gdown[None], loss


def solution(mesh):
    return jax.shard_map(
        body,
        mesh=mesh,
        in_specs=(
            P("pipe", "dp", "tensor"),
            P("dp", "tensor"),
            P("tensor"),
            P(None, None, "tensor"),
            P(None, None, "tensor"),
            P("pipe", None),
            P("pipe"),
        ),
        out_specs=(
            P("pipe", "dp", "tensor"),
            P("pipe", None, "tensor"),
            P("pipe", None, "tensor"),
            P("pipe", "dp"),
        ),
        check_vma=False,
    )
```
